8 devices in a mesh: dp: 1 (over z), pool: 2 (over y), ep: 4 (over x, core).
Axes of the slice: x: 2, y: 2, z: 1, core: 2. Of those that a mesh axis runs over, the one named last changes fastest.
Arguments:
- hidden: bfloat16 [1024, 1024], P(('dp', 'ep'))
- k_cache: bfloat16 [2, 1024, 512, 2, 128], P(None, ('dp', 'ep'))
- v_cache: bfloat16 [2, 1024, 512, 2, 128], P(None, ('dp', 'ep'))
- lengths: int32 [1024], P(('dp', 'ep'))
- expert_ids: int32 [2, 1024, 2], P(None, ('dp', 'ep'))
- w_query: bfloat16 [2, 1024, 1024], replicated
- w_key: bfloat16 [2, 1024, 256], replicated
- w_value: bfloat16 [2, 1024, 256], replicated
- w_out: bfloat16 [2, 1024, 1024], replicated
- w_router: float32 [2, 1024, 8], replicated
- w_gate: bfloat16 [2, 8, 1024, 3584], P(None, 'ep')
- w_up: bfloat16 [2, 8, 1024, 3584], P(None, 'ep')
- w_down: bfloat16 [2, 8, 3584, 1024], P(None, 'ep')
Outputs:
- output: bfloat16 [1024, 1024], P(('dp', 'ep'))
All inputs are finite; a program needn't handle non-finite values.
Results may differ from the reference program's by a relative error of at most 0.018765.
Values are sent between devices in bfloat16 or wider.
A program may use at most 1.5 GiB of HBM per device.

```python
import math
import jax
import jax.numpy as jnp
from jax import lax

LAYERS = 2
D = 1024
FF = 3584
EXPERTS = 8
TOPK = 2
HEADS = 8
KV_HEADS = 2
HEAD = 128
TOK = 256
SEQ = 512
NATT = 4
CAP = 192

EPSILON = 1e-6
ROPE_BASE = 10000.0


def draw_routing(key):
    total = TOK * TOPK
    layers_ids = []
    for layer in range(LAYERS):
        key_hot, key_dev = jax.random.split(jax.random.fold_in(key, layer))
        order = jax.random.permutation(key_hot, EXPERTS)
        n_hot = layer + 1
        n_cold = EXPERTS - n_hot
        spare = total - n_hot * CAP
        base_count = spare // n_cold
        extra_count = spare % n_cold

        def one_block(block_key):
            key_rank, key_tok = jax.random.split(block_key)
            ranks = jax.random.permutation(key_rank, n_cold)
            cold_counts = base_count + (ranks < extra_count).astype(jnp.int32)
            counts = jnp.zeros((EXPERTS,), jnp.int32).at[order[:n_hot]].set(CAP).at[order[n_hot:]].set(cold_counts)
            bounds = jnp.cumsum(counts)
            flat = jnp.sum((bounds[None, :] <= jnp.arange(total)[:, None]).astype(jnp.int32), axis=1)
            table = flat.reshape(TOPK, TOK).T
            return table[jax.random.permutation(key_tok, TOK)]

        block_ids = jax.vmap(one_block)(jax.random.split(key_dev, NATT))
        layers_ids.append(block_ids.reshape(NATT * TOK, TOPK))
    return jnp.stack(layers_ids)


def draw_lengths(key):
    tok_total = NATT * TOK
    key_exp, key_len, key_full = jax.random.split(key, 3)
    top_exp = int(math.log2(SEQ))
    exponent = jax.random.randint(key_exp, (tok_total,), 0, top_exp + 1)
    span = jnp.left_shift(jnp.ones((tok_total,), jnp.int32), exponent)
    lens = 1 + jax.random.randint(key_len, (tok_total,), 0, span)
    return lens.at[jax.random.randint(key_full, (), 0, tok_total)].set(SEQ)


def setup_inputs(seed: int = 0, part: int = 0) -> dict:
    tok_total = NATT * TOK
    base_key = jax.random.key(seed)
    part_key = jax.random.fold_in(jax.random.key(seed + 1), part)
    key_hid, key_kc, key_vc, key_len, key_ids = jax.random.split(part_key, 5)
    keys_w = jax.random.split(base_key, 8)

    def gauss(key, shape, scale):
        return jax.random.normal(key, shape, jnp.float32) * scale

    return {
        "hidden": gauss(key_hid, (tok_total, D), 1.0).astype(jnp.bfloat16),
        "k_cache": gauss(key_kc, (LAYERS, tok_total, SEQ, KV_HEADS, HEAD), 1.0).astype(jnp.bfloat16),
        "v_cache": gauss(key_vc, (LAYERS, tok_total, SEQ, KV_HEADS, HEAD), 1.0).astype(jnp.bfloat16),
        "lengths": draw_lengths(key_len),
        "expert_ids": draw_routing(key_ids),
        "w_query": gauss(keys_w[0], (LAYERS, D, HEADS * HEAD), 1.5 * D ** -0.5).astype(jnp.bfloat16),
        "w_key": gauss(keys_w[1], (LAYERS, D, KV_HEADS * HEAD), D ** -0.5).astype(jnp.bfloat16),
        "w_value": gauss(keys_w[2], (LAYERS, D, KV_HEADS * HEAD), D ** -0.5).astype(jnp.bfloat16),
        "w_out": gauss(keys_w[3], (LAYERS, HEADS * HEAD, D), 2.0 * (HEADS * HEAD) ** -0.5).astype(jnp.bfloat16),
        "w_router": gauss(keys_w[4], (LAYERS, D, EXPERTS), 1.5 * D ** -0.5),
        "w_gate": gauss(keys_w[5], (LAYERS, EXPERTS, D, FF), D ** -0.5).astype(jnp.bfloat16),
        "w_up": gauss(keys_w[6], (LAYERS, EXPERTS, D, FF), D ** -0.5).astype(jnp.bfloat16),
        "w_down": gauss(keys_w[7], (LAYERS, EXPERTS, FF, D), 2.0 * FF ** -0.5).astype(jnp.bfloat16),
    }


def rms_normed(values):
    return values * lax.rsqrt(jnp.mean(values * values, axis=-1, keepdims=True) + EPSILON)


def rotary(vectors, positions):
    half = vectors.shape[-1] // 2
    freqs = ROPE_BASE ** (-2.0 * jnp.arange(half, dtype=jnp.float32) / vectors.shape[-1])
    angle = positions[:, None, None] * freqs[None, None, :]
    cosine = jnp.cos(angle)
    sine = jnp.sin(angle)
    first = vectors[..., :half]
    second = vectors[..., half:]
    return jnp.concatenate([first * cosine - second * sine, second * cosine + first * sine], axis=-1)


def attend_block(hidden_blk, keys_blk, vals_blk, lens_blk, w_q, w_k, w_v, w_o):
    hidden_f = hidden_blk.astype(jnp.float32)
    normed = rms_normed(hidden_f).astype(jnp.bfloat16)
    positions = lens_blk.astype(jnp.float32)
    query = rotary(jnp.dot(normed, w_q, preferred_element_type=jnp.float32).reshape(TOK, HEADS, HEAD), positions)
    query = query.astype(jnp.bfloat16).reshape(TOK, KV_HEADS, HEADS // KV_HEADS, HEAD).astype(jnp.float32)
    key_new = rotary(jnp.dot(normed, w_k, preferred_element_type=jnp.float32).reshape(TOK, KV_HEADS, HEAD), positions)
    key_new = key_new.astype(jnp.bfloat16).astype(jnp.float32)
    val_new = jnp.dot(normed, w_v, preferred_element_type=jnp.float32).astype(jnp.bfloat16).reshape(TOK, KV_HEADS, HEAD)
    scale = HEAD ** -0.5
    scores = jnp.einsum("tkgd,tskd->tkgs", query, keys_blk.astype(jnp.float32)) * scale
    valid = jnp.arange(SEQ)[None, None, None, :] < lens_blk[:, None, None, None]
    scores = jnp.where(valid, scores, -jnp.inf)
    score_new = jnp.einsum("tkgd,tkd->tkg", query, key_new) * scale
    peak = jnp.maximum(jnp.max(scores, axis=-1), score_new)
    weights = jnp.exp(scores - peak[..., None])
    weight_new = jnp.exp(score_new - peak)
    denominator = jnp.sum(weights, axis=-1) + weight_new
    mixed = jnp.einsum("tkgs,tskd->tkgd", weights.astype(jnp.bfloat16).astype(jnp.float32), vals_blk.astype(jnp.float32))
    mixed = mixed + weight_new.astype(jnp.bfloat16).astype(jnp.float32)[..., None] * val_new.astype(jnp.float32)[:, :, None, :]
    attended = (mixed / denominator[..., None]).astype(jnp.bfloat16).reshape(TOK, HEADS * HEAD)
    return (hidden_f + jnp.dot(attended, w_o, preferred_element_type=jnp.float32)).astype(jnp.bfloat16)


def moe_layer(attn_out, ids_layer, w_r, w_gate, w_up, w_down):
    residual = attn_out.astype(jnp.float32)
    mixed_in = rms_normed(residual).astype(jnp.bfloat16)
    logits = jnp.dot(mixed_in.astype(jnp.float32), w_r)
    gates = jax.nn.softmax(jnp.take_along_axis(logits, ids_layer, axis=1), axis=-1)
    blocks_in = mixed_in.reshape(NATT, TOK, D).astype(jnp.float32)
    id_blocks = ids_layer.reshape(NATT, TOK, TOPK)
    gate_blocks = gates.reshape(NATT, TOK, TOPK)
    slot_ids = jnp.arange(CAP)

    def step(total_acc, layer_pack):
        expert, w_one, w_three, w_two = layer_pack
        hit = id_blocks == expert
        weight = jnp.sum(jnp.where(hit, gate_blocks, 0.0), axis=2)
        chosen = jnp.any(hit, axis=2)
        rank = jnp.cumsum(chosen.astype(jnp.int32), axis=1) - 1
        select = ((rank[:, None, :] == slot_ids[None, :, None]) & chosen[:, None, :]).astype(jnp.float32)
        rows = jnp.einsum("bct,btd->bcd", select, blocks_in).astype(jnp.bfloat16).reshape(NATT * CAP, D)
        inner = jax.nn.silu(jnp.dot(rows, w_one, preferred_element_type=jnp.float32)) * jnp.dot(rows, w_three, preferred_element_type=jnp.float32)
        result = jnp.dot(inner.astype(jnp.bfloat16), w_two, preferred_element_type=jnp.float32).astype(jnp.bfloat16)
        back = jnp.einsum("bct,bcd->btd", select, result.reshape(NATT, CAP, D).astype(jnp.float32))
        return total_acc + weight[:, :, None] * back, None

    total_acc, _ = lax.scan(step, jnp.zeros((NATT, TOK, D), jnp.float32), (jnp.arange(EXPERTS), w_gate, w_up, w_down))
    return (residual + total_acc.reshape(NATT * TOK, D)).astype(jnp.bfloat16)


def reference(hidden, k_cache, v_cache, lengths, expert_ids, w_query, w_key, w_value, w_out, w_router, w_gate, w_up, w_down):
    def layer_step(state, layer_pack):
        cache_k, cache_v, ids_layer, w_q, w_k, w_v, w_o, w_r, w_one, w_three, w_two = layer_pack

        def per_block(block_in):
            return attend_block(block_in[0], block_in[1], block_in[2], block_in[3], w_q, w_k, w_v, w_o)

        attn_out = lax.map(per_block, (state.reshape(NATT, TOK, D), cache_k.reshape(NATT, TOK, SEQ, KV_HEADS, HEAD), cache_v.reshape(NATT, TOK, SEQ, KV_HEADS, HEAD), lengths.reshape(NATT, TOK)))
        return moe_layer(attn_out.reshape(NATT * TOK, D), ids_layer, w_r, w_one, w_three, w_two), None

    final, _ = lax.scan(layer_step, hidden, (k_cache, v_cache, expert_ids, w_query, w_key, w_value, w_out, w_router, w_gate, w_up, w_down))
    return final
```

```python
import functools

import jax
import jax.numpy as jnp
from jax import lax
from jax.experimental import pallas as pl
from jax.experimental.pallas import tpu as pltpu
from jax.sharding import PartitionSpec as P

MESH = pl.DeviceIdType.MESH
EPSILON = 1e-6
ROPE_BASE = 10000.0
VMEM = pltpu.VMEM
ANY = pl.ANY
F32 = jnp.float32
BF16 = jnp.bfloat16

TOKG = 16
TILE = 1024
FT = 512
SIZES = (128, 256, 416, 512)


def vspec():
    return pl.BlockSpec(memory_space=VMEM)


def anyspec():
    return pl.BlockSpec(memory_space=ANY)


def sspec():
    return pl.BlockSpec(memory_space=pltpu.SMEM)


def dot(a, b):
    return jnp.dot(a, b, preferred_element_type=F32)


def rms_bf16(v):
    return (v * lax.rsqrt(jnp.mean(v * v, axis=-1, keepdims=True) + EPSILON)).astype(BF16)


def attn_kernel(layer, n_tok, x_off_static, t0_ref, lens_ref, x_ref, meta_ref, cos_ref, sin_ref, wq_hbm, wk_hbm, wv_hbm, wo_hbm,
                kc, vc, a_ref, u_ref, wq, wk, wv, wo, kbuf, vbuf, sbuf, qs, kn, vn, os_, wsem, ksem, vsem):
    t0 = t0_ref[0]
    heads = wq.shape[1] // 128
    n_groups = n_tok // TOKG
    hpk = heads // 2
    cols = heads * TOKG

    def rows_of(tok):
        return pl.multiple_of(((lens_ref[t0 + tok] + 7) // 8) * 16, 16)

    def start_group(g, slot):
        def one(i, off):
            off = pl.multiple_of(off, 16)
            tok = g * TOKG + i
            n = rows_of(tok)
            pltpu.make_async_copy(kc.at[layer, t0 + tok, pl.ds(0, n), :], kbuf.at[slot, pl.ds(off, n), :], ksem.at[slot]).start()
            pltpu.make_async_copy(vc.at[layer, t0 + tok, pl.ds(0, n), :], vbuf.at[slot, pl.ds(off, n), :], vsem.at[slot]).start()
            return off + n
        return lax.fori_loop(0, TOKG, one, 0)

    w_copies = [pltpu.make_async_copy(src.at[layer], dst, wsem.at[i])
                for i, (src, dst) in enumerate(((wq_hbm, wq), (wk_hbm, wk), (wv_hbm, wv), (wo_hbm, wo)))]
    for c in w_copies[:3]:
        c.start()
    total0 = start_group(0, 0)
    w_copies[3].start()

    if x_off_static:
        x = x_ref[...].astype(F32)
    else:
        x = x_ref[pl.ds(pl.multiple_of(t0, n_tok), n_tok), :].astype(F32)
    h = rms_bf16(x)
    cos = cos_ref[...]
    sin = sin_ref[...]
    for c in w_copies[:3]:
        c.wait()
    q = dot(h, wq[...])
    k = dot(h, wk[...])
    v = dot(h, wv[...])

    def rope(vec):
        return vec * cos + pltpu.roll(vec, 64, 1) * sin

    for j in range(heads):
        qs[:, j * 128:(j + 1) * 128] = rope(q[:, j * 128:(j + 1) * 128]).astype(BF16)
    for j in range(2):
        kn[:, j * 128:(j + 1) * 128] = rope(k[:, j * 128:(j + 1) * 128]).astype(BF16)
    vn[...] = v.astype(BF16)
    scale = 128.0 ** -0.5

    def group(g, total):
        slot = lax.rem(g, 2)
        nxt = lax.cond(g + 1 < n_groups, lambda: start_group(g + 1, 1 - slot), lambda: 0)
        total = pl.multiple_of(total, 16)
        g0 = pl.multiple_of(g * TOKG, TOKG)
        qrow = qs[pl.ds(g0, TOKG), :]
        q2 = jnp.concatenate([qrow[:, j * 128:(j + 1) * 128] for j in range(heads)], axis=0)
        krow = kn[pl.ds(g0, TOKG), :]
        vrow = vn[pl.ds(g0, TOKG), :]
        k2 = jnp.concatenate([krow[:, (j // hpk) * 128:(j // hpk + 1) * 128] for j in range(heads)], axis=0)
        v2 = jnp.concatenate([vrow[:, (j // hpk) * 128:(j // hpk + 1) * 128] for j in range(heads)], axis=0)
        s_new = jnp.sum(q2.astype(F32) * k2.astype(F32), axis=1, keepdims=True) * scale
        meta = meta_ref[pl.ds(g0, TOKG), :]
        start = jnp.concatenate([meta[:, 0:1]] * heads, axis=0)
        end = jnp.concatenate([meta[:, 1:2]] * heads, axis=0)
        kv = (lax.broadcasted_iota(jnp.int32, (cols, 1), 0) >= (hpk * TOKG)).astype(jnp.int32)
        n_tiles = (total + TILE - 1) // TILE
        vbuf[slot, pl.ds(total, TILE), :] = jnp.zeros((TILE, 128), BF16)
        pltpu.make_async_copy(kbuf.at[slot, pl.ds(0, total), :], kbuf.at[slot, pl.ds(0, total), :], ksem.at[slot]).wait()

        def first(i, macc):
            base = pl.multiple_of(i * TILE, TILE)
            kt = kbuf[slot, pl.ds(base, TILE), :]
            s = lax.dot_general(q2, kt, (((1,), (1,)), ((), ())), preferred_element_type=F32)
            r = lax.broadcasted_iota(jnp.int32, (cols, TILE), 1) + base
            valid = (r >= start) & (r < end) & ((r & 1) == kv)
            s = jnp.where(valid, s * scale, -jnp.inf)
            sbuf[:, pl.ds(base, TILE)] = s
            for j in range(TILE // 128):
                macc = jnp.maximum(macc, s[:, j * 128:(j + 1) * 128])
            return macc

        macc = lax.fori_loop(0, n_tiles, first, jnp.full((cols, 128), -jnp.inf, F32))
        peak = jnp.maximum(jnp.max(macc, axis=1, keepdims=True), s_new)
        w_new = jnp.exp(s_new - peak)
        pltpu.make_async_copy(vbuf.at[slot, pl.ds(0, total), :], vbuf.at[slot, pl.ds(0, total), :], vsem.at[slot]).wait()

        def second(i, carry):
            lacc, acc = carry
            base = pl.multiple_of(i * TILE, TILE)
            p = jnp.exp(sbuf[:, pl.ds(base, TILE)] - peak)
            for j in range(TILE // 128):
                lacc = lacc + p[:, j * 128:(j + 1) * 128]
            acc = acc + dot(p.astype(BF16), vbuf[slot, pl.ds(base, TILE), :])
            return lacc, acc

        lacc, acc = lax.fori_loop(0, n_tiles, second, (jnp.zeros((cols, 128), F32), jnp.zeros((cols, 128), F32)))
        den = jnp.sum(lacc, axis=1, keepdims=True) + w_new
        o = ((acc + w_new.astype(BF16).astype(F32) * v2.astype(F32)) / den).astype(BF16)
        for j in range(heads):
            os_[pl.ds(g0, TOKG), j * 128:(j + 1) * 128] = o[j * TOKG:(j + 1) * TOKG, :]
        return nxt

    lax.fori_loop(0, n_groups, group, total0)
    w_copies[3].wait()
    a = (x + dot(os_[...], wo[...])).astype(BF16)
    a_ref[...] = a
    u_ref[...] = rms_bf16(a.astype(F32))


def attention(layer, n_tok, t0, lens, x, meta, cos, sin, wq, wk, wv, wo, kc, vc):
    model, qdim = wq.shape[1], wq.shape[2]
    kvdim = wk.shape[2]
    max_rows = TOKG * kc.shape[2]
    cols = (qdim // 128) * TOKG
    return pl.pallas_call(
        functools.partial(attn_kernel, layer, n_tok, x.shape[0] == n_tok),
        out_shape=(jax.ShapeDtypeStruct((n_tok, model), BF16), jax.ShapeDtypeStruct((n_tok, model), BF16)),
        in_specs=[sspec(), sspec(), vspec(), vspec(), vspec(), vspec()] + [anyspec()] * 6,
        out_specs=(vspec(), vspec()),
        scratch_shapes=[
            VMEM((model, qdim), BF16), VMEM((model, kvdim), BF16), VMEM((model, kvdim), BF16), VMEM((qdim, model), BF16),
            VMEM((2, max_rows + TILE, 128), BF16), VMEM((2, max_rows + TILE, 128), BF16), VMEM((cols, max_rows), F32),
            VMEM((n_tok, qdim), BF16), VMEM((n_tok, kvdim), BF16), VMEM((n_tok, kvdim), BF16), VMEM((n_tok, qdim), BF16),
            pltpu.SemaphoreType.DMA((4,)), pltpu.SemaphoreType.DMA((2,)), pltpu.SemaphoreType.DMA((2,)),
        ],
        compiler_params=pltpu.CompilerParams(vmem_limit_bytes=48 * 1024 * 1024),
        name=f"attention{layer}",
    )(t0, lens, x, meta, cos, sin, wq, wk, wv, wo, kc, vc)


def peers():
    me = lax.axis_index("ep")
    core = me % 2
    x = me // 2
    return me, x * 2 + (1 - core), (1 - x) * 2 + core, (1 - x) * 2 + (1 - core)


def barrier(devices):
    sem = pltpu.get_barrier_semaphore()
    for d in devices:
        pl.semaphore_signal(sem, inc=1, device_id=d, device_id_type=MESH)
    pl.semaphore_wait(sem, len(devices))


def rcopy(src, dst, ssem, rsem, dev):
    return pltpu.make_async_remote_copy(src_ref=src, dst_ref=dst, send_sem=ssem, recv_sem=rsem, device_id=dev, device_id_type=MESH)


NCH = 4


def dispatch_kernel(with_ids, u_ref, *refs):
    if with_ids:
        ids_ref, uall, idsall, s_p, r_p, s_x, r_x, s_f, r_f, s_i, r_i = refs
    else:
        uall, s_p, r_p, s_x, r_x, s_f, r_f = refs
    n = u_ref.shape[0]
    ch = n // NCH
    me, part, xp, diag = peers()
    devs = [{"ep": part}, {"ep": xp}] + ([{"ep": diag}] if with_ids else [])
    barrier(devs)

    def rows(ep, c=None):
        if c is None:
            return pl.ds(pl.multiple_of(ep * n, n), n)
        return pl.ds(pl.multiple_of(ep * n + c * ch, ch), ch)

    xs = []
    for c in range(NCH):
        cp = rcopy(u_ref.at[pl.ds(c * ch, ch)], uall.at[rows(me, c)], s_x.at[c], r_x.at[c], {"ep": xp})
        cp.start()
        xs.append(cp)
    pc = rcopy(u_ref, uall.at[rows(me)], s_p, r_p, {"ep": part})
    pc.start()
    ics = []
    if with_ids:
        for i, d in enumerate(devs):
            cp = rcopy(ids_ref, idsall.at[me], s_i.at[i], r_i.at[i], d)
            cp.start()
            ics.append(cp)
        idsall[me] = ids_ref[...]
    uall[rows(me), :] = u_ref[...]
    fs = []
    for c in range(NCH):
        xs[c].wait_recv()
        cp = rcopy(uall.at[rows(xp, c)], uall.at[rows(xp, c)], s_f.at[c], r_f.at[c], {"ep": part})
        cp.start()
        fs.append(cp)
    pc.wait()
    for cp in ics:
        cp.wait()
    for c in range(NCH):
        xs[c].wait_send()
        fs[c].wait()


def dispatch(layer, u, ids):
    n, model = u.shape
    with_ids = ids is not None
    dma = pltpu.SemaphoreType.DMA
    out_shape = [jax.ShapeDtypeStruct((4 * n, model), BF16)]
    scratch = [dma, dma, dma((NCH,)), dma((NCH,)), dma((NCH,)), dma((NCH,))]
    args = [u]
    if with_ids:
        out_shape.append(jax.ShapeDtypeStruct((4,) + ids.shape, jnp.int32))
        scratch += [dma((3,)), dma((3,))]
        args.append(ids)
    out = pl.pallas_call(
        functools.partial(dispatch_kernel, with_ids),
        out_shape=out_shape,
        in_specs=[vspec()] * len(args),
        out_specs=[vspec()] * len(out_shape),
        scratch_shapes=scratch,
        compiler_params=pltpu.CompilerParams(collective_id=2 * layer, has_side_effects=True),
        name=f"dispatch{layer}",
    )(*args)
    return out if with_ids else (out[0], None)


def expert_kernel(layer, e0_ref, u_ref, ids_ref, wr_ref, wg_hbm, wu_hbm, wd_hbm, out_ref,
                  wg, wu, wd, xe, yacc, gcol, rcol, sg, su, sd):
    n = u_ref.shape[0]
    ff = wg_hbm.shape[3]
    steps = ff // FT
    n_loc = wg_hbm.shape[1]

    def copies(e, f, slot):
        return (pltpu.make_async_copy(wg_hbm.at[layer, e, :, pl.ds(pl.multiple_of(f * FT, FT), FT)], wg.at[slot], sg.at[slot]),
                pltpu.make_async_copy(wu_hbm.at[layer, e, :, pl.ds(pl.multiple_of(f * FT, FT), FT)], wu.at[slot], su.at[slot]),
                pltpu.make_async_copy(wd_hbm.at[layer, e, pl.ds(pl.multiple_of(f * FT, FT), FT), :], wd.at[slot], sd.at[slot]))

    for e in range(n_loc):
        def issue(f, _, e=e):
            for c in copies(e, f, e * steps + f):
                c.start()
            return 0
        lax.fori_loop(0, steps, issue, 0)

    e0 = e0_ref[0]
    blk = n // 4
    ids_row = [jnp.concatenate([ids_ref[b, 2 * layer + k:2 * layer + k + 1, :] for b in range(4)], axis=1) for k in range(2)]
    row8 = lax.broadcasted_iota(jnp.int32, (8, n), 0)
    hit = (ids_row[0] == row8 + e0) | (ids_row[1] == row8 + e0)
    hit_f = (hit & (row8 < n_loc)).astype(F32)
    tri = (lax.broadcasted_iota(jnp.int32, (n, n), 0) < lax.broadcasted_iota(jnp.int32, (n, n), 1)).astype(F32).astype(BF16)
    rank = dot(hit_f.astype(BF16), tri)
    rank = jnp.where(hit_f > 0, rank, -1.0)
    idf = jnp.where(row8 == 2, jnp.broadcast_to(ids_row[0].astype(F32), (8, n)),
                    jnp.where(row8 == 3, jnp.broadcast_to(ids_row[1].astype(F32), (8, n)), rank))
    tcol = jnp.transpose(idf)
    rcol[...] = tcol
    logits = dot(u_ref[...], wr_ref[...])
    logits = logits + pltpu.roll(logits, 120, 1) + pltpu.roll(logits, 112, 1)
    lane = lax.broadcasted_iota(jnp.int32, (n, 128), 1).astype(F32)
    id0 = tcol[:, 2:3]
    id1 = tcol[:, 3:4]
    l0 = jnp.sum(jnp.where(lane == id0, logits, 0.0), axis=1, keepdims=True)
    l1 = jnp.sum(jnp.where(lane == id1, logits, 0.0), axis=1, keepdims=True)
    top = jnp.maximum(l0, l1)
    x0 = jnp.exp(l0 - top)
    x1 = jnp.exp(l1 - top)
    den = x0 + x1
    g0 = x0 / den
    g1 = x1 / den
    e0f = e0.astype(F32)
    lane8 = lax.broadcasted_iota(jnp.int32, (n, 8), 1).astype(F32) + e0f
    gcol[...] = jnp.where(id0 == lane8, g0, 0.0) + jnp.where(id1 == lane8, g1, 0.0)

    for e in range(n_loc):
        count = jnp.sum(hit_f[e:e + 1, :]).astype(jnp.int32)
        rank_row = rank[e:e + 1, :]
        lo = 0
        for m in SIZES:
            @pl.when((count <= m) & ((count > lo) | (lo == 0)))
            def _(m=m, e=e):
                sel = (rank_row == lax.broadcasted_iota(jnp.int32, (m, n), 0).astype(F32)).astype(F32).astype(BF16)
                xe[pl.ds(0, m), :] = dot(sel, u_ref[...]).astype(BF16)
                yacc[pl.ds(0, m), :] = jnp.zeros((m, yacc.shape[1]), F32)

                def step(f, _):
                    slot = e * steps + f
                    c1, c3, c2 = copies(e, f, slot)
                    c1.wait()
                    gate = dot(xe[pl.ds(0, m), :], wg[slot])
                    c3.wait()
                    up = dot(xe[pl.ds(0, m), :], wu[slot])
                    inner = (gate * jax.nn.sigmoid(gate) * up).astype(BF16)
                    c2.wait()
                    yacc[pl.ds(0, m), :] += dot(inner, wd[slot])
                    return 0

                lax.fori_loop(0, steps, step, 0)
                y = yacc[pl.ds(0, m), :].astype(BF16)
                sel_t = (rcol[:, e:e + 1] == lax.broadcasted_iota(jnp.int32, (n, m), 1).astype(F32)).astype(F32).astype(BF16)
                back = dot(sel_t, y) * gcol[:, e:e + 1]
                if e == 0:
                    out_ref[...] = back
                else:
                    out_ref[...] += back
            lo = m


def experts(layer, e0, u_all, ids_all, wr, wg, wu, wd):
    n, model = u_all.shape
    ff = wg.shape[3]
    slots = (ff // FT) * wg.shape[1]
    dma = pltpu.SemaphoreType.DMA
    return pl.pallas_call(
        functools.partial(expert_kernel, layer),
        out_shape=jax.ShapeDtypeStruct((n, model), F32),
        in_specs=[sspec(), vspec(), vspec(), vspec(), anyspec(), anyspec(), anyspec()],
        out_specs=vspec(),
        scratch_shapes=[VMEM((slots, model, FT), BF16), VMEM((slots, model, FT), BF16), VMEM((slots, FT, model), BF16),
                        VMEM((n, model), BF16), VMEM((n, model), F32), VMEM((n, 8), F32), VMEM((n, 8), F32),
                        dma((slots,)), dma((slots,)), dma((slots,))],
        compiler_params=pltpu.CompilerParams(vmem_limit_bytes=62 * 1024 * 1024),
        name=f"experts{layer}",
    )(e0, u_all, ids_all, wr, wg, wu, wd)


def combine_kernel(last, p_ref, a_ref, out_ref, own, mid, far, sums, *sems):
    if last:
        s_o, r_o, s_m, r_m, s_f, r_f, s_y, r_y = sems
    else:
        s_o, r_o, s_m, r_m, s_f, r_f = sems
    n = a_ref.shape[0]
    ch = n // NCH
    me, part, xp, diag = peers()
    devs = [{"ep": part}, {"ep": xp}]
    if last:
        pool = lax.axis_index("pool")
        devs.append({"pool": 1 - pool})
    barrier(devs)

    def rows(ep, c):
        return pl.ds(pl.multiple_of(ep * n + c * ch, ch), ch)

    mids, owns, fars, ys = [], [], [], []
    for c in range(NCH):
        cp = rcopy(p_ref.at[rows(diag, c)], mid.at[pl.ds(c * ch, ch)], s_m.at[c], r_m.at[c], devs[0])
        cp.start()
        mids.append(cp)
    own_cp = rcopy(p_ref.at[pl.ds(pl.multiple_of(part * n, n), n)], own, s_o, r_o, devs[0])
    own_cp.start()
    for c in range(NCH):
        mids[c].wait_recv()
        sums[pl.ds(c * ch, ch), :] = p_ref[rows(xp, c), :] + mid[pl.ds(c * ch, ch), :]
        cp = rcopy(sums.at[pl.ds(c * ch, ch)], far.at[pl.ds(c * ch, ch)], s_f.at[c], r_f.at[c], devs[1])
        cp.start()
        fars.append(cp)
    own_cp.wait()
    for c in range(NCH):
        r = pl.ds(c * ch, ch)
        fars[c].wait_recv()
        total = p_ref[rows(me, c), :] + own[r, :] + far[r, :]
        res = (a_ref[r, :].astype(F32) + total).astype(BF16)
        if last:
            o = pl.ds(pl.multiple_of(pool * n + c * ch, ch), ch)
            out_ref[o, :] = res
            cp = rcopy(out_ref.at[o], out_ref.at[o], s_y.at[c], r_y.at[c], devs[2])
            cp.start()
            ys.append(cp)
        else:
            out_ref[r, :] = res
    for c in range(NCH):
        mids[c].wait_send()
        fars[c].wait_send()
    for cp in ys:
        cp.wait()


def combine(layer, last, p, a):
    n, model = a.shape
    ch = NCH
    dma = pltpu.SemaphoreType.DMA
    sems = [dma, dma, dma((ch,)), dma((ch,)), dma((ch,)), dma((ch,))]
    if last:
        sems += [dma((ch,)), dma((ch,))]
    return pl.pallas_call(
        functools.partial(combine_kernel, last),
        out_shape=jax.ShapeDtypeStruct((2 * n if last else n, model), BF16),
        in_specs=[vspec(), vspec()],
        out_specs=vspec(),
        scratch_shapes=[VMEM((n, model), F32) for _ in range(4)] + sems,
        compiler_params=pltpu.CompilerParams(collective_id=2 * layer + 1, has_side_effects=True),
        name=f"combine{layer}",
    )(p, a)


def solution(mesh):
    def body(hidden, k_cache, v_cache, lengths, expert_ids, w_query, w_key, w_value, w_out, w_router, w_gate, w_up, w_down):
        n_layers, _, seq, kvh, hd = k_cache.shape
        n_tok = hidden.shape[0] // 2
        pool = lax.axis_index("pool")
        ep = lax.axis_index("ep")
        t0 = (pool * n_tok).astype(jnp.int32)
        lens = lax.dynamic_slice_in_dim(lengths, t0, n_tok, 0)
        rows = ((lens + 7) // 8) * 16
        by_group = rows.reshape(n_tok // TOKG, TOKG)
        before = (jnp.arange(TOKG)[:, None] < jnp.arange(TOKG)[None, :]).astype(jnp.int32)
        start = jnp.sum(by_group[:, :, None] * before[None], axis=1).reshape(n_tok)
        meta = jnp.stack([start, start + 2 * lens], axis=1).astype(jnp.int32)
        half = hd // 2
        freqs = ROPE_BASE ** (-2.0 * jnp.arange(half, dtype=F32) / hd)
        angle = lens.astype(F32)[:, None] * freqs[None, :]
        cosine, sine = jnp.cos(angle), jnp.sin(angle)
        cos = jnp.concatenate([cosine, cosine], axis=1)
        sin = jnp.concatenate([-sine, sine], axis=1)
        ids = lax.dynamic_slice_in_dim(expert_ids, t0, n_tok, 1).transpose(0, 2, 1).reshape(n_layers * 2, n_tok)
        ids = jnp.pad(ids, ((0, 8 - n_layers * 2), (0, 0)))
        w1 = lax.reduce_precision(w_router, 8, 7)
        rest = w_router - w1
        w2 = lax.reduce_precision(rest, 8, 7)
        w3 = rest - w2
        wr = jnp.concatenate([w1, w2, w3], axis=2)
        wr = jnp.pad(wr, ((0, 0), (0, 0), (0, 128 - wr.shape[2]))).astype(BF16)
        kc = k_cache.reshape(n_layers, -1, seq * kvh, hd)
        vc = v_cache.reshape(n_layers, -1, seq * kvh, hd)
        t0v = t0.reshape(1)
        e0v = (ep * w_gate.shape[1]).astype(jnp.int32).reshape(1)
        state = hidden
        ids_all = None
        for layer in range(n_layers):
            a, u = attention(layer, n_tok, t0v, lengths, state, meta, cos, sin, w_query, w_key, w_value, w_out, kc, vc)
            if layer == 0:
                u_all, ids_all = dispatch(layer, u, ids)
            else:
                u_all, _ = dispatch(layer, u, None)
            part = experts(layer, e0v, u_all, ids_all, wr[layer], w_gate, w_up, w_down)
            state = combine(layer, layer == n_layers - 1, part, a)
        return state

    rows_spec = ("dp", "ep")
    in_specs = (P(rows_spec, None), P(None, rows_spec), P(None, rows_spec), P(rows_spec), P(None, rows_spec, None), P(), P(), P(), P(), P(), P(None, "ep"), P(None, "ep"), P(None, "ep"))
    return jax.shard_map(body, mesh=mesh, in_specs=in_specs, out_specs=P(rows_spec, None), check_vma=False)
```

```python
import functools

import numpy as np

import jax
import jax.numpy as jnp
from jax import lax
from jax.experimental import pallas as pl
from jax.experimental.pallas import tpu as pltpu
from jax.sharding import PartitionSpec as P

MESH = pl.DeviceIdType.MESH
EPSILON = 1e-6
ROPE_BASE = 10000.0
VMEM = pltpu.VMEM
F32 = jnp.float32
BF16 = jnp.bfloat16

TOKG = 16
TILE = 1024
FT = 512
LIM_D = 30 * 1024 * 1024
LIM_E = 27 * 1024 * 1024
LIM_C = 16 * 1024 * 1024
SIZES = (128, 256, 416, 512)


def vspec():
    return pl.BlockSpec(memory_space=VMEM)


def anyspec():
    return pl.BlockSpec(memory_space=pltpu.HBM)


def sspec():
    return pl.BlockSpec(memory_space=pltpu.SMEM)


def dot(a, b):
    return jnp.dot(a, b, preferred_element_type=F32)


def rms_bf16(v):
    return (v * lax.rsqrt(jnp.mean(v * v, axis=-1, keepdims=True) + EPSILON)).astype(BF16)


def rope_table(seq, hd):
    half = hd // 2
    freqs = np.power(np.float32(ROPE_BASE), (np.float32(-2.0) * np.arange(half, dtype=np.float32) / np.float32(hd)))
    angle = np.arange(seq + 1, dtype=np.float32)[:, None] * freqs.astype(np.float32)[None, :]
    wide = angle.astype(np.float64)
    return np.concatenate([np.cos(wide), np.sin(wide)], axis=1).astype(np.float32)


def rope(vec, cos, sin):
    return vec * cos + pltpu.roll(vec, 64, 1) * sin


def project(h, cos, sin, wq, wk, wv, qs, kn, vn, rows):
    q = dot(h, wq[...])
    k = dot(h, wk[...])
    v = dot(h, wv[...])
    for j in range(q.shape[1] // 128):
        qs[rows, j * 128:(j + 1) * 128] = rope(q[:, j * 128:(j + 1) * 128], cos, sin).astype(BF16)
    for j in range(k.shape[1] // 128):
        kn[rows, j * 128:(j + 1) * 128] = rope(k[:, j * 128:(j + 1) * 128], cos, sin).astype(BF16)
    vn[rows, :] = v.astype(BF16)


def attn_kernel(layer, n_tok, first_layer, lens_ref, *refs):
    if first_layer:
        (x_ref, tab_ref, wq_hbm, wk_hbm, wv_hbm, kc, vc, os_, cos_ref, sin_ref,
         wq, wk, wv, qs, kn, vn, wsem, kbuf, vbuf, sbuf, mst, men, ksem, vsem) = refs
    else:
        qs, kn, vn, kc, vc, os_, kbuf, vbuf, sbuf, mst, men, ksem, vsem = refs
    t0 = lax.axis_index("pool") * n_tok
    heads = qs.shape[1] // 128
    n_groups = n_tok // TOKG
    hpk = heads // 2
    cols = heads * TOKG

    def start_group(g, slot):
        def one(i, off):
            off = pl.multiple_of(off, 16)
            tok = t0 + g * TOKG + i
            ln = lens_ref[tok]
            n = pl.multiple_of(((ln + 7) // 8) * 16, 16)
            pltpu.make_async_copy(kc.at[layer, tok, pl.ds(0, n), :], kbuf.at[slot, pl.ds(off, n), :], ksem.at[slot]).start()
            pltpu.make_async_copy(vc.at[layer, tok, pl.ds(0, n), :], vbuf.at[slot, pl.ds(off, n), :], vsem.at[slot]).start()
            mst[slot, pl.ds(i, 1), :] = jnp.full((1, 128), off, jnp.int32)
            men[slot, pl.ds(i, 1), :] = jnp.full((1, 128), off + 2 * ln, jnp.int32)
            return off + n
        return lax.fori_loop(0, TOKG, one, 0)

    if first_layer:
        w_copies = [pltpu.make_async_copy(src.at[layer], dst, wsem.at[i])
                    for i, (src, dst) in enumerate(((wq_hbm, wq), (wk_hbm, wk), (wv_hbm, wv)))]
        for c in w_copies:
            c.start()
    total0 = start_group(0, 0)
    if first_layer:
        h = rms_bf16(x_ref[pl.ds(pl.multiple_of(t0, n_tok), n_tok), :].astype(F32))

        def pick(i, _):
            cos_ref[pl.ds(i, 1), :] = tab_ref[pl.ds(lens_ref[t0 + i], 1), :]
            return 0
        lax.fori_loop(0, n_tok, pick, 0)
        both = cos_ref[...]
        swapped = pltpu.roll(both, 64, 1)
        low = lax.broadcasted_iota(jnp.int32, both.shape, 1) < 64
        cos = jnp.where(low, both, swapped)
        sin = jnp.where(low, -swapped, both)
        cos_ref[...] = cos
        sin_ref[...] = sin
        for c in w_copies:
            c.wait()
        project(h, cos, sin, wq, wk, wv, qs, kn, vn, pl.ds(0, n_tok))
    scale = 128.0 ** -0.5

    def group(g, total):
        slot = lax.rem(g, 2)
        nxt = lax.cond(g + 1 < n_groups, lambda: start_group(g + 1, 1 - slot), lambda: 0)
        total = pl.multiple_of(total, 16)
        g0 = pl.multiple_of(g * TOKG, TOKG)
        qrow = qs[pl.ds(g0, TOKG), :]
        q2 = jnp.concatenate([qrow[:, j * 128:(j + 1) * 128] for j in range(heads)], axis=0)
        krow = kn[pl.ds(g0, TOKG), :]
        vrow = vn[pl.ds(g0, TOKG), :]
        k2 = jnp.concatenate([krow[:, (j // hpk) * 128:(j // hpk + 1) * 128] for j in range(heads)], axis=0)
        v2 = jnp.concatenate([vrow[:, (j // hpk) * 128:(j // hpk + 1) * 128] for j in range(heads)], axis=0)
        s_new = jnp.sum(q2.astype(F32) * k2.astype(F32), axis=1, keepdims=True) * scale
        start = jnp.concatenate([mst[slot]] * heads, axis=0)
        end = jnp.concatenate([men[slot]] * heads, axis=0)
        lane = lax.broadcasted_iota(jnp.int32, (cols, 128), 1)
        kv = (lax.broadcasted_iota(jnp.int32, (cols, 128), 0) >= (hpk * TOKG)).astype(jnp.int32)
        mine = (lane & 1) == kv
        start = jnp.where(mine, start - lane, 1 << 30)
        end = end - lane
        n_tiles = (total + TILE - 1) // TILE
        vbuf[slot, pl.ds(total, TILE), :] = jnp.zeros((TILE, 128), BF16)
        pltpu.make_async_copy(kbuf.at[slot, pl.ds(0, total), :], kbuf.at[slot, pl.ds(0, total), :], ksem.at[slot]).wait()

        def first(i, macc):
            base = pl.multiple_of(i * TILE, TILE)
            for j in range(TILE // 256):
                at = pl.multiple_of(base + j * 256, 256)
                kt = kbuf[slot, pl.ds(at, 256), :]
                s = lax.dot_general(q2, kt, (((1,), (1,)), ((), ())), preferred_element_type=F32)
                for p in range(2):
                    off = at + p * 128
                    sp = jnp.where((start <= off) & (end > off), s[:, p * 128:(p + 1) * 128] * scale, -jnp.inf)
                    sbuf[:, pl.ds(pl.multiple_of(off, 128), 128)] = sp
                    macc = jnp.maximum(macc, sp)
            return macc

        macc = lax.fori_loop(0, n_tiles, first, jnp.full((cols, 128), -jnp.inf, F32))
        peak = jnp.maximum(jnp.max(macc, axis=1, keepdims=True), s_new)
        w_new = jnp.exp(s_new - peak)
        peakb = jnp.broadcast_to(peak, (cols, 128))
        pltpu.make_async_copy(vbuf.at[slot, pl.ds(0, total), :], vbuf.at[slot, pl.ds(0, total), :], vsem.at[slot]).wait()

        def second(i, carry):
            lacc, acc = carry
            base = pl.multiple_of(i * TILE, TILE)
            parts = []
            for j in range(TILE // 128):
                p = jnp.exp(sbuf[:, pl.ds(pl.multiple_of(base + j * 128, 128), 128)] - peakb)
                lacc = lacc + p
                parts.append(p.astype(BF16))
            acc = acc + dot(jnp.concatenate(parts, axis=1), vbuf[slot, pl.ds(base, TILE), :])
            return lacc, acc

        lacc, acc = lax.fori_loop(0, n_tiles, second, (jnp.zeros((cols, 128), F32), jnp.zeros((cols, 128), F32)))
        den = jnp.sum(lacc, axis=1, keepdims=True) + w_new
        o = ((acc + w_new.astype(BF16).astype(F32) * v2.astype(F32)) / den).astype(BF16)
        for j in range(heads):
            os_[pl.ds(g0, TOKG), j * 128:(j + 1) * 128] = o[j * TOKG:(j + 1) * TOKG, :]
        return nxt

    lax.fori_loop(0, n_groups, group, total0)


def attention(layer, n_tok, lens, kc, vc, proj=None, qkv=None):
    dma = pltpu.SemaphoreType.DMA
    first_layer = proj is not None
    out_shape = []
    if first_layer:
        x, tab, wq, wk, wv = proj
        model, qdim, kvdim = wq.shape[1], wq.shape[2], wk.shape[2]
        args = [lens, x, tab, wq, wk, wv, kc, vc]
        specs = [sspec(), vspec(), vspec()] + [anyspec()] * 5
        out_shape = [jax.ShapeDtypeStruct((n_tok, qdim), BF16)] + [jax.ShapeDtypeStruct((n_tok, 128), F32)] * 2
        scratch = [VMEM((model, qdim), BF16), VMEM((model, kvdim), BF16), VMEM((model, kvdim), BF16),
                   VMEM((n_tok, qdim), BF16), VMEM((n_tok, kvdim), BF16), VMEM((n_tok, kvdim), BF16), dma((3,))]
    else:
        qdim = qkv[0].shape[1]
        args = [lens, *qkv, kc, vc]
        specs = [sspec()] + [vspec()] * 3 + [anyspec()] * 2
        out_shape = [jax.ShapeDtypeStruct((n_tok, qdim), BF16)]
        scratch = []
    max_rows = TOKG * kc.shape[2]
    cols = (qdim // 128) * TOKG
    scratch += [VMEM((2, max_rows + TILE, 128), BF16), VMEM((2, max_rows + TILE, 128), BF16), VMEM((cols, max_rows), F32),
                VMEM((2, TOKG, 128), jnp.int32), VMEM((2, TOKG, 128), jnp.int32), dma((2,)), dma((2,))]
    return pl.pallas_call(
        functools.partial(attn_kernel, layer, n_tok, first_layer),
        out_shape=out_shape,
        in_specs=specs,
        out_specs=[vspec()] * len(out_shape),
        scratch_shapes=scratch,
        compiler_params=pltpu.CompilerParams(vmem_limit_bytes=(52 if first_layer else 40) * 1024 * 1024),
        name=f"attention{layer}",
    )(*args)


NCH = 4


def peers():
    me = lax.axis_index("ep")
    core = me % 2
    x = me // 2
    return me, x * 2 + (1 - core), (1 - x) * 2 + core, (1 - x) * 2 + (1 - core)


def barrier(devices):
    sem = pltpu.get_barrier_semaphore()
    for d in devices:
        pl.semaphore_signal(sem, inc=1, device_id=d, device_id_type=MESH)
    pl.semaphore_wait(sem, len(devices))


def rcopy(src, dst, ssem, rsem, dev):
    return pltpu.make_async_remote_copy(src_ref=src, dst_ref=dst, send_sem=ssem, recv_sem=rsem, device_id=dev, device_id_type=MESH)


def weight_copies(layer, e, f, slot, hbm, buf, sems):
    wg_hbm, wu_hbm, wd_hbm = hbm
    cols = pl.ds(f * FT, FT) if isinstance(f, int) else pl.ds(pl.multiple_of(f * FT, FT), FT)
    return (pltpu.make_async_copy(wg_hbm.at[layer, e, :, cols], buf[0].at[slot], sems.at[slot, 0]),
            pltpu.make_async_copy(wu_hbm.at[layer, e, :, cols], buf[1].at[slot], sems.at[slot, 1]),
            pltpu.make_async_copy(wd_hbm.at[layer, e, cols, :], buf[2].at[slot], sems.at[slot, 2]))


def dispatch_kernel(layer, steps, n_loc, os_ref, x_ref, ids_ref, wr_ref, wo_hbm, wg_hbm, wu_hbm, wd_hbm, *refs):
    first_layer = layer == 0
    if first_layer:
        a_ref, uall, rrow, mcol, idsall, pg, pu, pd, wo, idsbuf, *sems = refs
        osem, psem, s_p, r_p, s_x, r_x, s_f, r_f, s_i, r_i = sems
    else:
        a_ref, uall, rrow, mcol, pg, pu, pd, wo, *sems = refs
        osem, psem, s_p, r_p, s_x, r_x, s_f, r_f = sems
        idsall = ids_ref
    n = os_ref.shape[0]
    ch = n // NCH
    pool = lax.axis_index("pool")
    me, part, xp, diag = peers()
    wo_cp = pltpu.make_async_copy(wo_hbm.at[layer], wo, osem)
    wo_cp.start()
    pre = []
    for f in range(steps):
        pre += weight_copies(layer, 0, f, f, (wg_hbm, wu_hbm, wd_hbm), (pg, pu, pd), psem)
    for c in pre:
        c.start()
    devs = [{"ep": part}, {"ep": xp}] + ([{"ep": diag}] if first_layer else [])
    barrier(devs)

    def rows(ep, c):
        return pl.ds(pl.multiple_of(ep * n + c * ch, ch), ch)

    ics = []
    if first_layer:
        t0 = pl.multiple_of(pool * n, n)
        idsbuf[...] = jnp.zeros(idsbuf.shape, jnp.int32)
        for l in range(ids_ref.shape[0]):
            idsbuf[2 * l:2 * l + 2, :] = ids_ref[l, :, pl.ds(t0, n)]
        idsall[me] = idsbuf[...]
        for i, d in enumerate(devs):
            cp = rcopy(idsbuf, idsall.at[me], s_i.at[i], r_i.at[i], d)
            cp.start()
            ics.append(cp)
    wo_cp.wait()
    xs, ps = [], []
    half = n // 2
    for hf in range(2):
        r = pl.ds(hf * half, half)
        if first_layer:
            xr = x_ref[pl.ds(pl.multiple_of(pool * n + hf * half, half), half), :]
        else:
            xr = x_ref[r, :]
        a = (xr.astype(F32) + dot(os_ref[r, :], wo[...])).astype(BF16)
        a_ref[r, :] = a
        uall[pl.ds(pl.multiple_of(me * n + hf * half, half), half), :] = rms_bf16(a.astype(F32))
        for c in range(hf * NCH // 2, (hf + 1) * NCH // 2):
            cp = rcopy(uall.at[rows(me, c)], uall.at[rows(me, c)], s_x.at[c], r_x.at[c], {"ep": xp})
            cp.start()
            xs.append(cp)
            cp = rcopy(uall.at[rows(me, c)], uall.at[rows(me, c)], s_p.at[c], r_p.at[c], {"ep": part})
            cp.start()
            ps.append(cp)
    for cp in ics:
        cp.wait()

    tokens = 4 * n
    e0 = me * n_loc
    ids_row = [jnp.concatenate([idsall[b, 2 * layer + k:2 * layer + k + 1, :] for b in range(4)], axis=1) for k in range(2)]
    row8 = lax.broadcasted_iota(jnp.int32, (8, tokens), 0)
    hit = ((ids_row[0] == row8 + e0) | (ids_row[1] == row8 + e0)) & (row8 < n_loc)
    hit_f = hit.astype(F32)
    tri = (lax.broadcasted_iota(jnp.int32, (tokens, tokens), 0) < lax.broadcasted_iota(jnp.int32, (tokens, tokens), 1)).astype(F32).astype(BF16)
    rank = jnp.where(hit_f > 0, dot(hit_f.astype(BF16), tri), -1.0)
    rrow[...] = rank
    idf = jnp.where(row8 == 2, jnp.broadcast_to(ids_row[0].astype(F32), (8, tokens)),
                    jnp.where(row8 == 3, jnp.broadcast_to(ids_row[1].astype(F32), (8, tokens)), rank))
    mcol[...] = jnp.transpose(idf)

    w = wr_ref[layer]
    w1 = w.astype(BF16).astype(F32)
    w2 = (w - w1).astype(BF16).astype(F32)
    w3 = w - w1 - w2
    wr = jnp.concatenate([w1, w2, w3, jnp.zeros((104, w.shape[1]), F32)], axis=0).astype(BF16)
    e0f = e0.astype(F32)

    def gates(ep):
        r = pl.ds(pl.multiple_of(ep * n, n), n)
        lg = lax.dot_general(uall[r, :], wr, (((1,), (1,)), ((), ())), preferred_element_type=F32)
        lg = lg + pltpu.roll(lg, 120, 1) + pltpu.roll(lg, 112, 1)
        lane = lax.broadcasted_iota(jnp.int32, (n, 128), 1).astype(F32)
        col = mcol[r, :]
        id0, id1 = col[:, 2:3], col[:, 3:4]
        l0 = jnp.sum(jnp.where(lane == id0, lg, 0.0), axis=1, keepdims=True)
        l1 = jnp.sum(jnp.where(lane == id1, lg, 0.0), axis=1, keepdims=True)
        top = jnp.maximum(l0, l1)
        x0 = jnp.exp(l0 - top)
        x1 = jnp.exp(l1 - top)
        den = x0 + x1
        lane8 = lax.broadcasted_iota(jnp.int32, (n, 8), 1)
        expert = (lane8 - 2).astype(F32) + e0f
        g = jnp.where(id0 == expert, x0 / den, 0.0) + jnp.where(id1 == expert, x1 / den, 0.0)
        mcol[r, :] = jnp.where(lane8 < 2, col, g)

    gates(me)
    fs = []

    def forward(c):
        xs[c].wait_recv()
        cp = rcopy(uall.at[rows(xp, c)], uall.at[rows(xp, c)], s_f.at[c], r_f.at[c], {"ep": part})
        cp.start()
        fs.append(cp)

    for c in range(NCH - 1):
        forward(c)
    for cp in ps:
        cp.wait()
    gates(part)
    forward(NCH - 1)
    gates(xp)
    for cp in fs:
        cp.wait()
    gates(diag)
    for cp in xs:
        cp.wait_send()
    for c in pre:
        c.wait()


def dispatch(layer, os_, x, ids, wr, wo, wg, wu, wd):
    n, qdim = os_.shape
    model = wo.shape[2]
    n_loc, ff = wg.shape[1], wg.shape[3]
    steps = ff // FT
    dma = pltpu.SemaphoreType.DMA
    out_shape = [jax.ShapeDtypeStruct((n, model), BF16), jax.ShapeDtypeStruct((4 * n, model), BF16),
                 jax.ShapeDtypeStruct((8, 4 * n), F32), jax.ShapeDtypeStruct((4 * n, 8), F32)]
    scratch = [VMEM((qdim, model), BF16)]
    sems = [dma, dma((steps, 3))] + [dma((NCH,))] * 6
    if layer == 0:
        out_shape.append(jax.ShapeDtypeStruct((4, 8, n), jnp.int32))
        scratch.append(VMEM((8, n), jnp.int32))
        sems += [dma((3,)), dma((3,))]
    n_small = len(out_shape)
    out_shape += [VMEM((steps, model, FT), BF16), VMEM((steps, model, FT), BF16), VMEM((steps, FT, model), BF16)]
    return pl.pallas_call(
        functools.partial(dispatch_kernel, layer, steps, n_loc),
        out_shape=out_shape,
        in_specs=[vspec()] * 4 + [anyspec()] * 4,
        out_specs=[vspec()] * n_small + [vspec()] * 3,
        scratch_shapes=scratch + sems,
        compiler_params=pltpu.CompilerParams(collective_id=2 * layer, has_side_effects=True, vmem_limit_bytes=LIM_D),
        name=f"dispatch{layer}",
    )(os_, x, ids, wr, wo, wg, wu, wd)


def expert_kernel(layer, u_ref, rrow_ref, mcol_ref, pg, pu, pd, wg_hbm, wu_hbm, wd_hbm, y_ref, wg, wu, wd, xe, yacc, sems):
    n = u_ref.shape[0]
    steps = pg.shape[0]
    n_loc = wg_hbm.shape[1]
    hbm = (wg_hbm, wu_hbm, wd_hbm)
    own = (wg, wu, wd)

    for e in range(1, n_loc):
        def issue(f, _, e=e):
            for c in weight_copies(layer, e, f, (e - 1) * steps + f, hbm, own, sems):
                c.start()
            return 0
        lax.fori_loop(0, steps, issue, 0)

    for e in range(n_loc):
        rank_row = rrow_ref[e:e + 1, :]
        count = jnp.sum((rank_row >= 0).astype(F32)).astype(jnp.int32)
        lo = 0
        for m in SIZES:
            @pl.when((count <= m) & ((count > lo) | (lo == 0)))
            def _(m=m, e=e):
                sel = (rank_row == lax.broadcasted_iota(jnp.int32, (m, n), 0).astype(F32)).astype(F32).astype(BF16)
                xe[pl.ds(0, m), :] = dot(sel, u_ref[...]).astype(BF16)
                yacc[pl.ds(0, m), :] = jnp.zeros((m, yacc.shape[1]), F32)

                def step(f, _):
                    if e == 0:
                        w1, w3, w2 = pg, pu, pd
                        slot = f
                    else:
                        w1, w3, w2 = own
                        slot = (e - 1) * steps + f
                        for c in weight_copies(layer, e, f, slot, hbm, own, sems):
                            c.wait()
                    gate = dot(xe[pl.ds(0, m), :], w1[slot])
                    up = dot(xe[pl.ds(0, m), :], w3[slot])
                    inner = (gate * jax.nn.sigmoid(gate) * up).astype(BF16)
                    yacc[pl.ds(0, m), :] += dot(inner, w2[slot])
                    return 0

                lax.fori_loop(0, steps, step, 0)
                y_ref[pl.ds(e * n, m), :] = yacc[pl.ds(0, m), :].astype(BF16)
                if m < n:
                    y_ref[pl.ds(e * n + m, n - m), :] = jnp.zeros((n - m, y_ref.shape[1]), BF16)
            lo = m


def experts(layer, u_all, rrow, mcol, pre, wg, wu, wd):
    n, model = u_all.shape
    steps = pre[0].shape[0]
    n_loc = wg.shape[1]
    slots = steps * (n_loc - 1)
    return pl.pallas_call(
        functools.partial(expert_kernel, layer),
        out_shape=jax.ShapeDtypeStruct((n_loc * n, model), BF16),
        in_specs=[vspec()] * 6 + [anyspec()] * 3,
        out_specs=vspec(),
        scratch_shapes=[VMEM((slots, model, FT), BF16), VMEM((slots, model, FT), BF16), VMEM((slots, FT, model), BF16),
                        VMEM((n, model), BF16), VMEM((n, model), F32), pltpu.SemaphoreType.DMA((slots, 3))],
        compiler_params=pltpu.CompilerParams(vmem_limit_bytes=LIM_E),
        name=f"experts{layer}",
    )(u_all, rrow, mcol, *pre, wg, wu, wd)


def combine_kernel(last, layer, y_ref, mcol_ref, a_ref, *refs):
    if last:
        out_ref, p_d, p_x, p_p, p_me, own, mid, far, *sems = refs
        s_o, r_o, s_m, r_m, s_f, r_f, s_y, r_y = sems
    else:
        (cos_ref, sin_ref, wq_hbm, wk_hbm, wv_hbm, out_ref, qs, kn, vn,
         p_d, p_x, p_p, p_me, own, mid, far, wq, wk, wv, *sems) = refs
        s_o, r_o, s_m, r_m, s_f, r_f, wsem = sems
    n = a_ref.shape[0]
    ch = n // NCH
    nn = mcol_ref.shape[0]
    me, part, xp, diag = peers()
    devs = [{"ep": part}, {"ep": xp}]
    if last:
        pool = lax.axis_index("pool")
        devs.append({"pool": 1 - pool})
    else:
        w_copies = [pltpu.make_async_copy(src.at[layer + 1], dst, wsem.at[i])
                    for i, (src, dst) in enumerate(((wq_hbm, wq), (wk_hbm, wk), (wv_hbm, wv)))]
        for c in w_copies:
            c.start()

    def partial(ep):
        col = mcol_ref[pl.ds(pl.multiple_of(ep * n, n), n), :]
        slot = lax.broadcasted_iota(jnp.int32, (n, nn), 1).astype(F32)
        total = None
        for e in range(y_ref.shape[0] // nn):
            sel = (col[:, e:e + 1] == slot).astype(F32).astype(BF16)
            t = dot(sel, y_ref[e * nn:(e + 1) * nn, :]) * col[:, 2 + e:3 + e]
            total = t if total is None else total + t
        return total

    p_d[...] = partial(diag)
    barrier(devs)
    mids, fars, ys = [], [], []
    for c in range(NCH):
        r = pl.ds(c * ch, ch)
        cp = rcopy(p_d.at[r], mid.at[r], s_m.at[c], r_m.at[c], devs[0])
        cp.start()
        mids.append(cp)
    p_x[...] = partial(xp)
    for c in range(NCH):
        r = pl.ds(c * ch, ch)
        mids[c].wait_recv()
        p_x[r, :] = p_x[r, :] + mid[r, :]
        cp = rcopy(p_x.at[r], far.at[r], s_f.at[c], r_f.at[c], devs[1])
        cp.start()
        fars.append(cp)
    p_p[...] = partial(part)
    own_cp = rcopy(p_p, own, s_o, r_o, devs[0])
    own_cp.start()
    p_me[...] = partial(me)
    own_cp.wait()
    p_me[...] = a_ref[...].astype(F32) + (p_me[...] + own[...])
    if not last:
        for c in w_copies:
            c.wait()
    for c in range(NCH):
        r = pl.ds(c * ch, ch)
        fars[c].wait_recv()
        res = (p_me[r, :] + far[r, :]).astype(BF16)
        if last:
            o = pl.ds(pl.multiple_of(pool * n + c * ch, ch), ch)
            out_ref[o, :] = res
            cp = rcopy(out_ref.at[o], out_ref.at[o], s_y.at[c], r_y.at[c], devs[2])
            cp.start()
            ys.append(cp)
        else:
            out_ref[r, :] = res
            if c % 2 == 1:
                r2 = pl.ds((c - 1) * ch, 2 * ch)
                h = rms_bf16(out_ref[r2, :].astype(F32))
                project(h, cos_ref[r2, :], sin_ref[r2, :], wq, wk, wv, qs, kn, vn, r2)
    for c in range(NCH):
        mids[c].wait_send()
        fars[c].wait_send()
    for cp in ys:
        cp.wait()


def combine(layer, last, y, mcol, a, nxt=None):
    n, model = a.shape
    dma = pltpu.SemaphoreType.DMA
    sems = [dma, dma, dma((NCH,)), dma((NCH,)), dma((NCH,)), dma((NCH,))]
    args = [y, mcol, a]
    specs = [vspec()] * 3
    scratch = [VMEM((n, model), F32) for _ in range(7)]
    if last:
        sems += [dma((NCH,)), dma((NCH,))]
        out_shape = jax.ShapeDtypeStruct((2 * n, model), BF16)
        out_specs = vspec()
    else:
        cos, sin, wq, wk, wv = nxt
        args += [cos, sin, wq, wk, wv]
        specs += [vspec()] * 2 + [anyspec()] * 3
        sems += [dma((3,))]
        scratch += [VMEM(w.shape[1:], BF16) for w in (wq, wk, wv)]
        out_shape = [jax.ShapeDtypeStruct((n, model), BF16)] + [jax.ShapeDtypeStruct((n, w.shape[2]), BF16) for w in (wq, wk, wv)]
        out_specs = [vspec()] * 4
    return pl.pallas_call(
        functools.partial(combine_kernel, last, layer),
        out_shape=out_shape,
        in_specs=specs,
        out_specs=out_specs,
        scratch_shapes=scratch + sems,
        compiler_params=pltpu.CompilerParams(collective_id=2 * layer + 1, has_side_effects=True, vmem_limit_bytes=LIM_C),
        name=f"combine{layer}",
    )(*args)


def solution(mesh):
    def body(hidden, k_cache, v_cache, lengths, expert_ids, w_query, w_key, w_value, w_out, w_router, w_gate, w_up, w_down):
        n_layers, _, seq, kvh, hd = k_cache.shape
        n_tok = hidden.shape[0] // 2
        kc = k_cache.reshape(n_layers, -1, seq * kvh, hd)
        vc = v_cache.reshape(n_layers, -1, seq * kvh, hd)
        ids = expert_ids.transpose(0, 2, 1)
        wr = w_router.transpose(0, 2, 1)
        tab = jnp.asarray(rope_table(seq, hd))
        state = hidden
        qkv = None
        for layer in range(n_layers):
            last = layer == n_layers - 1
            if layer == 0:
                att, cos, sin = attention(layer, n_tok, lengths, kc, vc, proj=(hidden, tab, w_query, w_key, w_value))
            else:
                (att,) = attention(layer, n_tok, lengths, kc, vc, qkv=qkv)
            outs = dispatch(layer, att, state, ids, wr, w_out, w_gate, w_up, w_down)
            a, u_all, rrow, mcol = outs[:4]
            if layer == 0:
                ids = outs[4]
            y = experts(layer, u_all, rrow, mcol, outs[-3:], w_gate, w_up, w_down)
            if last:
                return combine(layer, True, y, mcol, a)
            state, *qkv = combine(layer, False, y, mcol, a, nxt=(cos, sin, w_query, w_key, w_value))

    rows_spec = ("dp", "ep")
    in_specs = (P(rows_spec, None), P(None, rows_spec), P(None, rows_spec), P(rows_spec), P(None, rows_spec, None), P(), P(), P(), P(), P(), P(None, "ep"), P(None, "ep"), P(None, "ep"))
    return jax.shard_map(body, mesh=mesh, in_specs=in_specs, out_specs=P(rows_spec, None), check_vma=False)
```

```python
import functools

import numpy as np

import jax
import jax.numpy as jnp
from jax import lax
from jax.experimental import pallas as pl
from jax.experimental.pallas import tpu as pltpu
from jax.sharding import PartitionSpec as P

MESH = pl.DeviceIdType.MESH
EPSILON = 1e-6
ROPE_BASE = 10000.0
VMEM = pltpu.VMEM
F32 = jnp.float32
BF16 = jnp.bfloat16

TOKG = 16
TILE = 1024
FT = 512
NSLOT = 4
CCH = 8
LIM_A = 50 * 1024 * 1024
LIM_B = 50 * 1024 * 1024
LIM_D = 8 * 1024 * 1024
LIM_E = 27 * 1024 * 1024
LIM_C = 16 * 1024 * 1024
SIZES = (128, 256, 416, 512)


def vspec():
    return pl.BlockSpec(memory_space=VMEM)


def anyspec():
    return pl.BlockSpec(memory_space=pltpu.HBM)


def sspec():
    return pl.BlockSpec(memory_space=pltpu.SMEM)


def dot(a, b):
    return jnp.dot(a, b, preferred_element_type=F32)


def rms_bf16(v):
    return (v * lax.rsqrt(jnp.mean(v * v, axis=-1, keepdims=True) + EPSILON)).astype(BF16)


def rope_table(seq, hd):
    half = hd // 2
    freqs = np.power(np.float32(ROPE_BASE), (np.float32(-2.0) * np.arange(half, dtype=np.float32) / np.float32(hd)))
    angle = np.arange(seq + 1, dtype=np.float32)[:, None] * freqs.astype(np.float32)[None, :]
    wide = angle.astype(np.float64)
    return np.concatenate([np.cos(wide), np.sin(wide)], axis=1).astype(np.float32)


def rope(vec, cos, sin):
    return vec * cos + pltpu.roll(vec, 64, 1) * sin


def project(h, cos, sin, wq, wk, wv, qs, kn, vn, rows):
    q = dot(h, wq[...])
    k = dot(h, wk[...])
    v = dot(h, wv[...])
    for j in range(q.shape[1] // 128):
        qs[rows, j * 128:(j + 1) * 128] = rope(q[:, j * 128:(j + 1) * 128], cos, sin).astype(BF16)
    for j in range(k.shape[1] // 128):
        kn[rows, j * 128:(j + 1) * 128] = rope(k[:, j * 128:(j + 1) * 128], cos, sin).astype(BF16)
    vn[rows, :] = v.astype(BF16)


def attn_kernel(layer, n_tok, first_layer, lens_ref, *refs):
    if first_layer:
        (x_hbm, tab_hbm, wq_hbm, wk_hbm, wv_hbm, wo_hbm, kc, vc, os_, wo, cos_ref, sin_ref,
         x_ref, tab_ref, wq, wk, wv, qs, kn, vn, wsem, kbuf, vbuf, sbuf, mst, men, ksem, vsem, osem) = refs
    else:
        qs, kn, vn, wo_hbm, kc, vc, os_, wo, kbuf, vbuf, sbuf, mst, men, ksem, vsem, osem = refs
    t0 = lax.axis_index("pool") * n_tok
    heads = qs.shape[1] // 128
    n_groups = n_tok // TOKG
    hpk = heads // 2
    cols = heads * TOKG

    def start_group(g, slot):
        def one(i, off):
            off = pl.multiple_of(off, 16)
            tok = t0 + g * TOKG + i
            ln = lens_ref[tok]
            n = pl.multiple_of(lax.shift_left(lax.shift_right_logical(ln + 7, 3), 4), 16)
            pltpu.make_async_copy(kc.at[layer, tok, pl.ds(0, n), :], kbuf.at[slot, pl.ds(off, n), :], ksem.at[slot]).start()
            pltpu.make_async_copy(vc.at[layer, tok, pl.ds(0, n), :], vbuf.at[slot, pl.ds(off, n), :], vsem.at[slot]).start()
            mst[slot, pl.ds(i, 1), :] = jnp.full((1, 128), off, jnp.int32)
            men[slot, pl.ds(i, 1), :] = jnp.full((1, 128), off + 2 * ln, jnp.int32)
            return off + n
        return lax.fori_loop(0, TOKG, one, 0)

    if first_layer:
        w_copies = [pltpu.make_async_copy(src.at[layer], dst, wsem.at[i])
                    for i, (src, dst) in enumerate(((wq_hbm, wq), (wk_hbm, wk), (wv_hbm, wv)))]
        x_cp = pltpu.make_async_copy(x_hbm.at[pl.ds(pl.multiple_of(t0, n_tok), n_tok), :], x_ref, wsem.at[3])
        tab_cp = pltpu.make_async_copy(tab_hbm, tab_ref, wsem.at[4])
        x_cp.start()
        tab_cp.start()
        for c in w_copies:
            c.start()
    totals0 = tuple(start_group(g, g) for g in range(NSLOT - 1))
    wo_cp = pltpu.make_async_copy(wo_hbm.at[layer], wo, osem)
    wo_cp.start()
    if first_layer:
        x_cp.wait()
        tab_cp.wait()
        h = rms_bf16(x_ref[...].astype(F32))

        def pick(i, _):
            cos_ref[pl.ds(i, 1), :] = tab_ref[pl.ds(lens_ref[t0 + i], 1), :]
            return 0
        lax.fori_loop(0, n_tok, pick, 0)
        both = cos_ref[...]
        swapped = pltpu.roll(both, 64, 1)
        low = lax.broadcasted_iota(jnp.int32, both.shape, 1) < 64
        cos = jnp.where(low, both, swapped)
        sin = jnp.where(low, -swapped, both)
        cos_ref[...] = cos
        sin_ref[...] = sin
        for c in w_copies:
            c.wait()
        project(h, cos, sin, wq, wk, wv, qs, kn, vn, pl.ds(0, n_tok))
    scale = 128.0 ** -0.5 * 1.4426950408889634

    def group(g, totals):
        slot = g & (NSLOT - 1)
        ahead = g + NSLOT - 1
        nxt = lax.cond(ahead < n_groups, lambda: start_group(ahead, ahead & (NSLOT - 1)), lambda: 0)
        total = pl.multiple_of(totals[0], 16)
        g0 = pl.multiple_of(g * TOKG, TOKG)
        qrow = qs[pl.ds(g0, TOKG), :]
        q2 = jnp.concatenate([qrow[:, j * 128:(j + 1) * 128] for j in range(heads)], axis=0)
        krow = kn[pl.ds(g0, TOKG), :]
        vrow = vn[pl.ds(g0, TOKG), :]
        k2 = jnp.concatenate([krow[:, (j // hpk) * 128:(j // hpk + 1) * 128] for j in range(heads)], axis=0)
        v2 = jnp.concatenate([vrow[:, (j // hpk) * 128:(j // hpk + 1) * 128] for j in range(heads)], axis=0)
        s_new = jnp.sum(q2.astype(F32) * k2.astype(F32), axis=1, keepdims=True)
        start = jnp.concatenate([mst[slot]] * heads, axis=0)
        end = jnp.concatenate([men[slot]] * heads, axis=0)
        lane = lax.broadcasted_iota(jnp.int32, (cols, 128), 1)
        kv = (lax.broadcasted_iota(jnp.int32, (cols, 128), 0) >= (hpk * TOKG)).astype(jnp.int32)
        mine = (lane & 1) == kv
        start = jnp.where(mine, start - lane, 1 << 30)
        end = end - lane
        n_tiles = lax.shift_right_logical(total + TILE - 1, TILE.bit_length() - 1)
        vbuf[slot, pl.ds(total, TILE), :] = jnp.zeros((TILE, 128), BF16)
        pltpu.make_async_copy(kbuf.at[slot, pl.ds(0, total), :], kbuf.at[slot, pl.ds(0, total), :], ksem.at[slot]).wait()

        def first(i, macc):
            base = pl.multiple_of(i * TILE, TILE)
            for j in range(TILE // 256):
                at = pl.multiple_of(base + j * 256, 256)
                kt = kbuf[slot, pl.ds(at, 256), :]
                s = lax.dot_general(q2, kt, (((1,), (1,)), ((), ())), preferred_element_type=F32)
                for p in range(2):
                    off = at + p * 128
                    sp = jnp.where((start <= off) & (end > off), s[:, p * 128:(p + 1) * 128], -jnp.inf)
                    sbuf[:, pl.ds(pl.multiple_of(off, 128), 128)] = sp
                    macc = jnp.maximum(macc, sp)
            return macc

        macc = lax.fori_loop(0, n_tiles, first, jnp.full((cols, 128), -jnp.inf, F32))
        peak = jnp.maximum(jnp.max(macc, axis=1, keepdims=True), s_new)
        w_new = jnp.exp2((s_new - peak) * scale)
        peakb = jnp.broadcast_to(peak, (cols, 128))
        pltpu.make_async_copy(vbuf.at[slot, pl.ds(0, total), :], vbuf.at[slot, pl.ds(0, total), :], vsem.at[slot]).wait()

        def second(i, carry):
            lacc, acc = carry
            base = pl.multiple_of(i * TILE, TILE)
            parts = []
            for j in range(TILE // 128):
                p = jnp.exp2((sbuf[:, pl.ds(pl.multiple_of(base + j * 128, 128), 128)] - peakb) * scale)
                lacc = lacc + p
                parts.append(p.astype(BF16))
            acc = acc + dot(jnp.concatenate(parts, axis=1), vbuf[slot, pl.ds(base, TILE), :])
            return lacc, acc

        lacc, acc = lax.fori_loop(0, n_tiles, second, (jnp.zeros((cols, 128), F32), jnp.zeros((cols, 128), F32)))
        den = jnp.sum(lacc, axis=1, keepdims=True) + w_new
        o = ((acc + w_new.astype(BF16).astype(F32) * v2.astype(F32)) / den).astype(BF16)
        for j in range(heads):
            os_[pl.ds(g0, TOKG), j * 128:(j + 1) * 128] = o[j * TOKG:(j + 1) * TOKG, :]
        return totals[1:] + (nxt,)

    lax.fori_loop(0, n_groups, group, totals0)
    wo_cp.wait()


def attention(layer, n_tok, lens, w_out, kc, vc, proj=None, qkv=None):
    dma = pltpu.SemaphoreType.DMA
    first_layer = proj is not None
    out_shape = []
    if first_layer:
        x, tab, wq, wk, wv = proj
        model, qdim, kvdim = wq.shape[1], wq.shape[2], wk.shape[2]
        args = [lens, x, tab, wq, wk, wv, w_out, kc, vc]
        specs = [sspec()] + [anyspec()] * 8
        out_shape = [VMEM((n_tok, qdim), BF16), VMEM(w_out.shape[1:], BF16)] + [jax.ShapeDtypeStruct((n_tok, 128), F32)] * 2
        scratch = [VMEM((n_tok, model), BF16), VMEM(tab.shape, F32), VMEM((model, qdim), BF16), VMEM((model, kvdim), BF16), VMEM((model, kvdim), BF16),
                   VMEM((n_tok, qdim), BF16), VMEM((n_tok, kvdim), BF16), VMEM((n_tok, kvdim), BF16), dma((5,))]
    else:
        qdim = qkv[0].shape[1]
        args = [lens, *qkv, w_out, kc, vc]
        specs = [sspec()] + [vspec()] * 3 + [anyspec()] * 3
        out_shape = [VMEM((n_tok, qdim), BF16), VMEM(w_out.shape[1:], BF16)]
        scratch = []
    max_rows = TOKG * kc.shape[2]
    cols = (qdim // 128) * TOKG
    scratch += [VMEM((NSLOT, max_rows + TILE, 128), BF16), VMEM((NSLOT, max_rows + TILE, 128), BF16), VMEM((cols, max_rows), F32),
                VMEM((NSLOT, TOKG, 128), jnp.int32), VMEM((NSLOT, TOKG, 128), jnp.int32), dma((NSLOT,)), dma((NSLOT,)), dma]
    return pl.pallas_call(
        functools.partial(attn_kernel, layer, n_tok, first_layer),
        out_shape=out_shape,
        in_specs=specs,
        out_specs=[vspec()] * len(out_shape),
        scratch_shapes=scratch,
        compiler_params=pltpu.CompilerParams(vmem_limit_bytes=LIM_A if first_layer else LIM_B),
        name=f"attention{layer}",
    )(*args)


NCH = 4


def peers():
    me = lax.axis_index("ep")
    core = me % 2
    x = me // 2
    return me, x * 2 + (1 - core), (1 - x) * 2 + core, (1 - x) * 2 + (1 - core)


def barrier(devices):
    sem = pltpu.get_barrier_semaphore()
    for d in devices:
        pl.semaphore_signal(sem, inc=1, device_id=d, device_id_type=MESH)
    return lambda: pl.semaphore_wait(sem, len(devices))


def rcopy(src, dst, ssem, rsem, dev):
    return pltpu.make_async_remote_copy(src_ref=src, dst_ref=dst, send_sem=ssem, recv_sem=rsem, device_id=dev, device_id_type=MESH)


def weight_copies(layer, e, f, slot, hbm, buf, sems):
    wg_hbm, wu_hbm, wd_hbm = hbm
    cols = pl.ds(f * FT, FT) if isinstance(f, int) else pl.ds(pl.multiple_of(f * FT, FT), FT)
    return (pltpu.make_async_copy(wg_hbm.at[layer, e, :, cols], buf[0].at[slot], sems.at[slot, 0]),
            pltpu.make_async_copy(wu_hbm.at[layer, e, :, cols], buf[1].at[slot], sems.at[slot, 1]),
            pltpu.make_async_copy(wd_hbm.at[layer, e, cols, :], buf[2].at[slot], sems.at[slot, 2]))


def dispatch_kernel(layer, steps, n_loc, os_ref, x_ref, ids_ref, wr_ref, wo, wg_hbm, wu_hbm, wd_hbm, *refs):
    first_layer = layer == 0
    if first_layer:
        a_ref, uall, rrow, mcol, idsall, pg, pu, pd, idsbuf, *sems = refs
        psem, s_p, r_p, s_x, r_x, s_f, r_f, s_i, r_i = sems
    else:
        a_ref, uall, rrow, mcol, pg, pu, pd, *sems = refs
        psem, s_p, r_p, s_x, r_x, s_f, r_f = sems
        idsall = ids_ref
    n = os_ref.shape[0]
    ch = n // NCH
    pool = lax.axis_index("pool")
    me, part, xp, diag = peers()
    devs = [{"ep": part}, {"ep": xp}] + ([{"ep": diag}] if first_layer else [])
    arrive = barrier(devs)

    def rows(ep, c):
        return pl.ds(pl.multiple_of(ep * n + c * ch, ch), ch)

    ics = []
    if first_layer:
        t0 = pl.multiple_of(pool * n, n)
        idsbuf[...] = jnp.zeros(idsbuf.shape, jnp.int32)
        for l in range(ids_ref.shape[0]):
            idsbuf[2 * l:2 * l + 2, :] = ids_ref[l, :, pl.ds(t0, n)]
        idsall[me] = idsbuf[...]
        arrive()
        for i, d in enumerate(devs):
            cp = rcopy(idsbuf, idsall.at[me], s_i.at[i], r_i.at[i], d)
            cp.start()
            ics.append(cp)
    xs, ps = [], []
    half = n // 2
    for hf in range(2):
        r = pl.ds(hf * half, half)
        if first_layer:
            xr = x_ref[pl.ds(pl.multiple_of(pool * n + hf * half, half), half), :]
        else:
            xr = x_ref[r, :]
        a = (xr.astype(F32) + dot(os_ref[r, :], wo[...])).astype(BF16)
        a_ref[r, :] = a
        uall[pl.ds(pl.multiple_of(me * n + hf * half, half), half), :] = rms_bf16(a.astype(F32))
        if hf == 0 and not first_layer:
            arrive()
        for c in range(hf * NCH // 2, (hf + 1) * NCH // 2):
            cp = rcopy(uall.at[rows(me, c)], uall.at[rows(me, c)], s_x.at[c], r_x.at[c], {"ep": xp})
            cp.start()
            xs.append(cp)
            cp = rcopy(uall.at[rows(me, c)], uall.at[rows(me, c)], s_p.at[c], r_p.at[c], {"ep": part})
            cp.start()
            ps.append(cp)
    hbm = (wg_hbm, wu_hbm, wd_hbm)

    def prefetch(f, _):
        for cp in weight_copies(layer, 0, f, f, hbm, (pg, pu, pd), psem):
            cp.start()
        return 0

    lax.fori_loop(0, steps, prefetch, 0)
    for cp in ics:
        cp.wait()

    tokens = 4 * n
    e0 = me * n_loc
    ids_row = [jnp.concatenate([idsall[b, 2 * layer + k:2 * layer + k + 1, :] for b in range(4)], axis=1) for k in range(2)]
    row8 = lax.broadcasted_iota(jnp.int32, (8, tokens), 0)
    hit = ((ids_row[0] == row8 + e0) | (ids_row[1] == row8 + e0)) & (row8 < n_loc)
    hit_f = hit.astype(F32)
    tri = (lax.broadcasted_iota(jnp.int32, (tokens, tokens), 0) < lax.broadcasted_iota(jnp.int32, (tokens, tokens), 1)).astype(F32).astype(BF16)
    rank = jnp.where(hit_f > 0, dot(hit_f.astype(BF16), tri), -1.0)
    rrow[...] = rank
    idf = jnp.where(row8 == 2, jnp.broadcast_to(ids_row[0].astype(F32), (8, tokens)),
                    jnp.where(row8 == 3, jnp.broadcast_to(ids_row[1].astype(F32), (8, tokens)), rank))
    mcol[...] = jnp.transpose(idf)

    w = wr_ref[layer]
    w1 = w.astype(BF16).astype(F32)
    w2 = (w - w1).astype(BF16).astype(F32)
    w3 = w - w1 - w2
    wr = jnp.concatenate([w1, w2, w3, jnp.zeros((104, w.shape[1]), F32)], axis=0).astype(BF16)
    e0f = e0.astype(F32)

    def gates(ep):
        r = pl.ds(pl.multiple_of(ep * n, n), n)
        lg = lax.dot_general(uall[r, :], wr, (((1,), (1,)), ((), ())), preferred_element_type=F32)
        lg = lg + pltpu.roll(lg, 120, 1) + pltpu.roll(lg, 112, 1)
        lane = lax.broadcasted_iota(jnp.int32, (n, 128), 1).astype(F32)
        col = mcol[r, :]
        id0, id1 = col[:, 2:3], col[:, 3:4]
        l0 = jnp.sum(jnp.where(lane == id0, lg, 0.0), axis=1, keepdims=True)
        l1 = jnp.sum(jnp.where(lane == id1, lg, 0.0), axis=1, keepdims=True)
        top = jnp.maximum(l0, l1)
        x0 = jnp.exp(l0 - top)
        x1 = jnp.exp(l1 - top)
        den = x0 + x1
        lane8 = lax.broadcasted_iota(jnp.int32, (n, 8), 1)
        expert = (lane8 - 2).astype(F32) + e0f
        g = jnp.where(id0 == expert, x0 / den, 0.0) + jnp.where(id1 == expert, x1 / den, 0.0)
        mcol[r, :] = jnp.where(lane8 < 2, col, g)

    gates(me)
    fs = []

    def forward(c):
        xs[c].wait_recv()
        cp = rcopy(uall.at[rows(xp, c)], uall.at[rows(xp, c)], s_f.at[c], r_f.at[c], {"ep": part})
        cp.start()
        fs.append(cp)

    for c in range(NCH - 1):
        forward(c)
    for cp in ps:
        cp.wait()
    gates(part)
    forward(NCH - 1)
    gates(xp)
    for cp in fs:
        cp.wait()
    gates(diag)
    for cp in xs:
        cp.wait_send()
    for f in range(steps):
        for cp in weight_copies(layer, 0, f, f, hbm, (pg, pu, pd), psem):
            cp.wait()


def dispatch(layer, os_, x, ids, wr, wo, wg, wu, wd):
    n, qdim = os_.shape
    model = wo.shape[1]
    n_loc, ff = wg.shape[1], wg.shape[3]
    steps = ff // FT
    dma = pltpu.SemaphoreType.DMA
    out_shape = [jax.ShapeDtypeStruct((n, model), BF16), jax.ShapeDtypeStruct((4 * n, model), BF16),
                 jax.ShapeDtypeStruct((8, 4 * n), F32), jax.ShapeDtypeStruct((4 * n, 8), F32)]
    scratch = []
    sems = [dma((steps, 3))] + [dma((NCH,))] * 6
    if layer == 0:
        out_shape.append(jax.ShapeDtypeStruct((4, 8, n), jnp.int32))
        scratch.append(VMEM((8, n), jnp.int32))
        sems += [dma((3,)), dma((3,))]
    n_small = len(out_shape)
    out_shape += [VMEM((steps, model, FT), BF16), VMEM((steps, model, FT), BF16), VMEM((steps, FT, model), BF16)]
    return pl.pallas_call(
        functools.partial(dispatch_kernel, layer, steps, n_loc),
        out_shape=out_shape,
        in_specs=[vspec()] * 5 + [anyspec()] * 3,
        out_specs=[vspec()] * n_small + [vspec()] * 3,
        scratch_shapes=scratch + sems,
        compiler_params=pltpu.CompilerParams(collective_id=2 * layer, has_side_effects=True, vmem_limit_bytes=LIM_D),
        name=f"dispatch{layer}",
    )(os_, x, ids, wr, wo, wg, wu, wd)


def expert_kernel(layer, u_ref, rrow_ref, mcol_ref, pg, pu, pd, wg_hbm, wu_hbm, wd_hbm, y_ref, wg, wu, wd, xe, yacc, sems):
    n = u_ref.shape[0]
    steps = pg.shape[0]
    n_loc = wg_hbm.shape[1]
    hbm = (wg_hbm, wu_hbm, wd_hbm)
    own = (wg, wu, wd)

    for e in range(1, n_loc):
        def issue(f, _, e=e):
            for c in weight_copies(layer, e, f, (e - 1) * steps + f, hbm, own, sems):
                c.start()
            return 0
        lax.fori_loop(0, steps, issue, 0)

    for e in range(n_loc):
        rank_row = rrow_ref[e:e + 1, :]
        count = jnp.sum((rank_row >= 0).astype(F32)).astype(jnp.int32)
        lo = 0
        for m in SIZES:
            @pl.when((count <= m) & ((count > lo) | (lo == 0)))
            def _(m=m, e=e):
                sel = (rank_row == lax.broadcasted_iota(jnp.int32, (m, n), 0).astype(F32)).astype(F32).astype(BF16)
                xe[pl.ds(0, m), :] = dot(sel, u_ref[...]).astype(BF16)
                yacc[pl.ds(0, m), :] = jnp.zeros((m, yacc.shape[1]), F32)

                def step(f, _):
                    if e == 0:
                        w1, w3, w2 = pg, pu, pd
                        slot = f
                    else:
                        w1, w3, w2 = own
                        slot = (e - 1) * steps + f
                        for c in weight_copies(layer, e, f, slot, hbm, own, sems):
                            c.wait()
                    gate = dot(xe[pl.ds(0, m), :], w1[slot])
                    up = dot(xe[pl.ds(0, m), :], w3[slot])
                    inner = (gate * jax.nn.sigmoid(gate) * up).astype(BF16)
                    yacc[pl.ds(0, m), :] += dot(inner, w2[slot])
                    return 0

                lax.fori_loop(0, steps, step, 0)
                y_ref[pl.ds(e * n, m), :] = yacc[pl.ds(0, m), :].astype(BF16)
                if m < n:
                    y_ref[pl.ds(e * n + m, n - m), :] = jnp.zeros((n - m, y_ref.shape[1]), BF16)
            lo = m


def experts(layer, u_all, rrow, mcol, pre, wg, wu, wd):
    n, model = u_all.shape
    steps = pre[0].shape[0]
    n_loc = wg.shape[1]
    slots = steps * (n_loc - 1)
    return pl.pallas_call(
        functools.partial(expert_kernel, layer),
        out_shape=jax.ShapeDtypeStruct((n_loc * n, model), BF16),
        in_specs=[vspec()] * 6 + [anyspec()] * 3,
        out_specs=vspec(),
        scratch_shapes=[VMEM((slots, model, FT), BF16), VMEM((slots, model, FT), BF16), VMEM((slots, FT, model), BF16),
                        VMEM((n, model), BF16), VMEM((n, model), F32), pltpu.SemaphoreType.DMA((slots, 3))],
        compiler_params=pltpu.CompilerParams(vmem_limit_bytes=LIM_E),
        name=f"experts{layer}",
    )(u_all, rrow, mcol, *pre, wg, wu, wd)


def combine_kernel(last, layer, y_ref, mcol_ref, a_ref, *refs):
    if last:
        out_ref, p_d, p_x, p_p, p_me, own, mid, far, *sems = refs
        s_o, r_o, s_m, r_m, s_f, r_f, s_y, r_y = sems
    else:
        (cos_ref, sin_ref, wq_hbm, wk_hbm, wv_hbm, out_ref, qs, kn, vn,
         p_d, p_x, p_p, p_me, own, mid, far, wq, wk, wv, *sems) = refs
        s_o, r_o, s_m, r_m, s_f, r_f, wsem = sems
    n = a_ref.shape[0]
    ch = n // CCH
    nn = mcol_ref.shape[0]
    me, part, xp, diag = peers()
    devs = [{"ep": part}, {"ep": xp}]
    if last:
        pool = lax.axis_index("pool")
        devs.append({"pool": 1 - pool})
    else:
        w_copies = [pltpu.make_async_copy(src.at[layer + 1], dst, wsem.at[i])
                    for i, (src, dst) in enumerate(((wq_hbm, wq), (wk_hbm, wk), (wv_hbm, wv)))]
        for c in w_copies:
            c.start()

    def partial(ep):
        col = mcol_ref[pl.ds(pl.multiple_of(ep * n, n), n), :]
        slot = lax.broadcasted_iota(jnp.int32, (n, nn), 1).astype(F32)
        total = None
        for e in range(y_ref.shape[0] // nn):
            sel = (col[:, e:e + 1] == slot).astype(F32).astype(BF16)
            t = dot(sel, y_ref[e * nn:(e + 1) * nn, :]) * col[:, 2 + e:3 + e]
            total = t if total is None else total + t
        return total

    arrive = barrier(devs)
    p_d[...] = partial(diag)
    arrive()
    mids, fars, ys = [], [], []
    for c in range(CCH):
        r = pl.ds(c * ch, ch)
        cp = rcopy(p_d.at[r], mid.at[r], s_m.at[c], r_m.at[c], devs[0])
        cp.start()
        mids.append(cp)
    p_x[...] = partial(xp)
    for c in range(CCH):
        r = pl.ds(c * ch, ch)
        mids[c].wait_recv()
        p_x[r, :] = p_x[r, :] + mid[r, :]
        cp = rcopy(p_x.at[r], far.at[r], s_f.at[c], r_f.at[c], devs[1])
        cp.start()
        fars.append(cp)
    p_p[...] = partial(part)
    own_cp = rcopy(p_p, own, s_o, r_o, devs[0])
    own_cp.start()
    p_me[...] = partial(me)
    own_cp.wait()
    p_me[...] = a_ref[...].astype(F32) + (p_me[...] + own[...])
    if not last:
        for c in w_copies:
            c.wait()
    for c in range(CCH):
        r = pl.ds(c * ch, ch)
        fars[c].wait_recv()
        res = (p_me[r, :] + far[r, :]).astype(BF16)
        if last:
            o = pl.ds(pl.multiple_of(pool * n + c * ch, ch), ch)
            out_ref[o, :] = res
            cp = rcopy(out_ref.at[o], out_ref.at[o], s_y.at[c], r_y.at[c], devs[2])
            cp.start()
            ys.append(cp)
        else:
            out_ref[r, :] = res
            if c % (CCH // 2) == CCH // 2 - 1:
                r2 = pl.ds(c * ch + ch - n // 2, n // 2)
                h = rms_bf16(out_ref[r2, :].astype(F32))
                project(h, cos_ref[r2, :], sin_ref[r2, :], wq, wk, wv, qs, kn, vn, r2)
    for c in range(CCH):
        mids[c].wait_send()
        fars[c].wait_send()
    for cp in ys:
        cp.wait()


def combine(layer, last, y, mcol, a, nxt=None):
    n, model = a.shape
    dma = pltpu.SemaphoreType.DMA
    sems = [dma, dma, dma((CCH,)), dma((CCH,)), dma((CCH,)), dma((CCH,))]
    args = [y, mcol, a]
    specs = [vspec()] * 3
    scratch = [VMEM((n, model), F32) for _ in range(7)]
    if last:
        sems += [dma((CCH,)), dma((CCH,))]
        out_shape = jax.ShapeDtypeStruct((2 * n, model), BF16)
        out_specs = vspec()
    else:
        cos, sin, wq, wk, wv = nxt
        args += [cos, sin, wq, wk, wv]
        specs += [vspec()] * 2 + [anyspec()] * 3
        sems += [dma((3,))]
        scratch += [VMEM(w.shape[1:], BF16) for w in (wq, wk, wv)]
        out_shape = [jax.ShapeDtypeStruct((n, model), BF16)] + [jax.ShapeDtypeStruct((n, w.shape[2]), BF16) for w in (wq, wk, wv)]
        out_specs = [vspec()] * 4
    return pl.pallas_call(
        functools.partial(combine_kernel, last, layer),
        out_shape=out_shape,
        in_specs=specs,
        out_specs=out_specs,
        scratch_shapes=scratch + sems,
        compiler_params=pltpu.CompilerParams(collective_id=2 * layer + 1, has_side_effects=True, vmem_limit_bytes=LIM_C),
        name=f"combine{layer}",
    )(*args)


def solution(mesh):
    def body(hidden, k_cache, v_cache, lengths, expert_ids, w_query, w_key, w_value, w_out, w_router, w_gate, w_up, w_down):
        n_layers, _, seq, kvh, hd = k_cache.shape
        n_tok = hidden.shape[0] // 2
        kc = k_cache.reshape(n_layers, -1, seq * kvh, hd)
        vc = v_cache.reshape(n_layers, -1, seq * kvh, hd)
        ids = expert_ids.transpose(0, 2, 1)
        wr = w_router.transpose(0, 2, 1)
        tab = jnp.asarray(rope_table(seq, hd))
        w_query, w_key, w_value, w_out, w_gate, w_up, w_down, kc, vc, tab, hidden_h = (
            pltpu.with_memory_space_constraint(v, pltpu.HBM) for v in (w_query, w_key, w_value, w_out, w_gate, w_up, w_down, kc, vc, tab, hidden))
        state = hidden
        qkv = None
        for layer in range(n_layers):
            last = layer == n_layers - 1
            if layer == 0:
                att, wo, cos, sin = attention(layer, n_tok, lengths, w_out, kc, vc, proj=(hidden_h, tab, w_query, w_key, w_value))
            else:
                att, wo = attention(layer, n_tok, lengths, w_out, kc, vc, qkv=qkv)
            outs = dispatch(layer, att, state, ids, wr, wo, w_gate, w_up, w_down)
            a, u_all, rrow, mcol = outs[:4]
            if layer == 0:
                ids = outs[4]
            y = experts(layer, u_all, rrow, mcol, outs[-3:], w_gate, w_up, w_down)
            if last:
                return combine(layer, True, y, mcol, a)
            state, *qkv = combine(layer, False, y, mcol, a, nxt=(cos, sin, w_query, w_key, w_value))

    rows_spec = ("dp", "ep")
    in_specs = (P(rows_spec, None), P(None, rows_spec), P(None, rows_spec), P(rows_spec), P(None, rows_spec, None), P(), P(), P(), P(), P(), P(None, "ep"), P(None, "ep"), P(None, "ep"))
    return jax.shard_map(body, mesh=mesh, in_specs=in_specs, out_specs=P(rows_spec, None), check_vma=False)
```

```python
import functools

import numpy as np

import jax
import jax.numpy as jnp
from jax import lax
from jax.experimental import pallas as pl
from jax.experimental.pallas import tpu as pltpu
from jax.sharding import PartitionSpec as P

MESH = pl.DeviceIdType.MESH
EPSILON = 1e-6
ROPE_BASE = 10000.0
VMEM = pltpu.VMEM
F32 = jnp.float32
BF16 = jnp.bfloat16

TOKG = 16
TILE = 1024
FT = 512
NSLOT = 3
CCH = 8
LIM_A = 50 * 1024 * 1024
LIM_B = 50 * 1024 * 1024
LIM_D = 8 * 1024 * 1024
LIM_E = 27 * 1024 * 1024
LIM_C = 16 * 1024 * 1024
SIZES = (192, 400, 512)


def vspec():
    return pl.BlockSpec(memory_space=VMEM)


def anyspec():
    return pl.BlockSpec(memory_space=pltpu.HBM)


def sspec():
    return pl.BlockSpec(memory_space=pltpu.SMEM)


def dot(a, b):
    return jnp.dot(a, b, preferred_element_type=F32)


def rms_bf16(v):
    return (v * lax.rsqrt(jnp.mean(v * v, axis=-1, keepdims=True) + EPSILON)).astype(BF16)


def rope_table(seq, hd):
    half = hd // 2
    freqs = np.power(np.float32(ROPE_BASE), (np.float32(-2.0) * np.arange(half, dtype=np.float32) / np.float32(hd)))
    angle = np.arange(seq + 1, dtype=np.float32)[:, None] * freqs.astype(np.float32)[None, :]
    wide = angle.astype(np.float64)
    return np.concatenate([np.cos(wide), np.sin(wide)], axis=1).astype(np.float32)


def rope(vec, cos, sin):
    return vec * cos + pltpu.roll(vec, 64, 1) * sin


def project(h, cos, sin, wq, wk, wv, qs, kn, vn, rows):
    q = dot(h, wq[...])
    k = dot(h, wk[...])
    v = dot(h, wv[...])
    for j in range(q.shape[1] // 128):
        qs[rows, j * 128:(j + 1) * 128] = rope(q[:, j * 128:(j + 1) * 128], cos, sin).astype(BF16)
    for j in range(k.shape[1] // 128):
        kn[rows, j * 128:(j + 1) * 128] = rope(k[:, j * 128:(j + 1) * 128], cos, sin).astype(BF16)
    vn[rows, :] = v.astype(BF16)


def attn_kernel(layer, n_tok, first_layer, lens_ref, *refs):
    if first_layer:
        (x_hbm, tab_hbm, wq_hbm, wk_hbm, wv_hbm, wo_hbm, kc, vc, os_, wo, cos_ref, sin_ref,
         x_ref, tab_ref, wq, wk, wv, qs, kn, vn, wsem, kbuf, vbuf, sbuf, mst, men, pk, wn, ksem, vsem, osem) = refs
    else:
        qs, kn, vn, wo_hbm, kc, vc, os_, wo, kbuf, vbuf, sbuf, mst, men, pk, wn, ksem, vsem, osem = refs
    t0 = lax.axis_index("pool") * n_tok
    heads = qs.shape[1] // 128
    n_groups = n_tok // TOKG
    hpk = heads // 2
    cols = heads * TOKG

    def padded(ln):
        return pl.multiple_of(lax.shift_left(lax.shift_right_logical(ln + 7, 3), 4), 16)

    def start_keys(g):
        slot = lax.rem(g, NSLOT)
        off = 0
        for i in range(TOKG):
            tok = t0 + g * TOKG + i
            ln = lens_ref[tok]
            n = padded(ln)
            off = pl.multiple_of(off, 16)
            pltpu.make_async_copy(kc.at[layer, tok, pl.ds(0, n), :], kbuf.at[slot, pl.ds(off, n), :], ksem.at[slot]).start()
            mst[slot, i:i + 1, :] = jnp.full((1, 128), off, jnp.int32)
            men[slot, i:i + 1, :] = jnp.full((1, 128), off + 2 * ln, jnp.int32)
            off = off + n
        return jnp.asarray(off, jnp.int32)

    def start_vals(g):
        slot = lax.rem(g, NSLOT)
        off = 0
        for i in range(TOKG):
            tok = t0 + g * TOKG + i
            n = padded(lens_ref[tok])
            off = pl.multiple_of(off, 16)
            pltpu.make_async_copy(vc.at[layer, tok, pl.ds(0, n), :], vbuf.at[slot, pl.ds(off, n), :], vsem.at[slot]).start()
            off = off + n

    if first_layer:
        w_copies = [pltpu.make_async_copy(src.at[layer], dst, wsem.at[i])
                    for i, (src, dst) in enumerate(((wq_hbm, wq), (wk_hbm, wk), (wv_hbm, wv)))]
        x_cp = pltpu.make_async_copy(x_hbm.at[pl.ds(pl.multiple_of(t0, n_tok), n_tok), :], x_ref, wsem.at[3])
        tab_cp = pltpu.make_async_copy(tab_hbm, tab_ref, wsem.at[4])
        x_cp.start()
        tab_cp.start()
        for c in w_copies:
            c.start()
    total0 = start_keys(jnp.int32(0))
    start_vals(jnp.int32(0))
    total1 = start_keys(jnp.int32(1))
    wo_cp = pltpu.make_async_copy(wo_hbm.at[layer], wo, osem)
    wo_cp.start()
    if first_layer:
        x_cp.wait()
        tab_cp.wait()
        h = rms_bf16(x_ref[...].astype(F32))

        def pick(i, _):
            cos_ref[pl.ds(i, 1), :] = tab_ref[pl.ds(lens_ref[t0 + i], 1), :]
            return 0
        lax.fori_loop(0, n_tok, pick, 0)
        both = cos_ref[...]
        swapped = pltpu.roll(both, 64, 1)
        low = lax.broadcasted_iota(jnp.int32, both.shape, 1) < 64
        cos = jnp.where(low, both, swapped)
        sin = jnp.where(low, -swapped, both)
        cos_ref[...] = cos
        sin_ref[...] = sin
        for c in w_copies:
            c.wait()
        project(h, cos, sin, wq, wk, wv, qs, kn, vn, pl.ds(0, n_tok))
    scale = 128.0 ** -0.5 * 1.4426950408889634

    lane = lax.broadcasted_iota(jnp.int32, (cols, 128), 1)
    kv = (lax.broadcasted_iota(jnp.int32, (cols, 128), 0) >= (hpk * TOKG)).astype(jnp.int32)
    mine = (lane & 1) == kv

    def heads_of(ref, g):
        row = ref[pl.ds(pl.multiple_of(g * TOKG, TOKG), TOKG), :]
        per = heads // (ref.shape[1] // 128)
        return jnp.concatenate([row[:, (j // per) * 128:(j // per + 1) * 128] for j in range(heads)], axis=0)

    def tiles_of(total):
        return lax.shift_right_logical(total + TILE - 1, TILE.bit_length() - 1)

    def step(g, totals):
        prev_total, total, next_total = totals
        prev_total = pl.multiple_of(prev_total, 16)
        total = pl.multiple_of(total, 16)
        slot = lax.rem(g, NSLOT)
        prev = lax.rem(g + NSLOT - 1, NSLOT)
        sl, sp = g & 1, 1 - (g & 1)
        last = lax.cond(g + 2 < n_groups, lambda: start_keys(g + 2), lambda: jnp.int32(0))

        @pl.when(g + 1 < n_groups)
        def _():
            start_vals(g + 1)

        gc = jnp.minimum(g, n_groups - 1)
        q2 = heads_of(qs, gc)
        s_new = jnp.sum(q2.astype(F32) * heads_of(kn, gc).astype(F32), axis=1, keepdims=True)
        start = jnp.where(mine, jnp.concatenate([mst[slot]] * heads, axis=0) - lane, 1 << 30)
        end = jnp.concatenate([men[slot]] * heads, axis=0) - lane
        n1 = jnp.where(g < n_groups, tiles_of(total), 0)
        n2 = jnp.where(g > 0, tiles_of(prev_total), 0)
        both = jnp.minimum(n1, n2)

        @pl.when(g < n_groups)
        def _():
            pltpu.make_async_copy(kbuf.at[slot, pl.ds(0, total), :], kbuf.at[slot, pl.ds(0, total), :], ksem.at[slot]).wait()

        @pl.when(g > 0)
        def _():
            vbuf[prev, pl.ds(prev_total, TILE), :] = jnp.zeros((TILE, 128), BF16)
            pltpu.make_async_copy(vbuf.at[prev, pl.ds(0, prev_total), :], vbuf.at[prev, pl.ds(0, prev_total), :], vsem.at[prev]).wait()

        def first(i, macc):
            base = pl.multiple_of(i * TILE, TILE)
            for j in range(TILE // 256):
                at = pl.multiple_of(base + j * 256, 256)
                s = lax.dot_general(q2, kbuf[slot, pl.ds(at, 256), :], (((1,), (1,)), ((), ())), preferred_element_type=F32)
                for p in range(2):
                    off = at + p * 128
                    part = jnp.where((start <= off) & (end > off), s[:, p * 128:(p + 1) * 128], -jnp.inf)
                    sbuf[sl, :, pl.ds(pl.multiple_of(off, 128), 128)] = part
                    macc = jnp.maximum(macc, part)
            return macc

        def second(i, carry):
            lacc, acc = carry
            base = pl.multiple_of(i * TILE, TILE)
            top = pk[...]
            parts = []
            for j in range(TILE // 128):
                p = jnp.exp2((sbuf[sp, :, pl.ds(pl.multiple_of(base + j * 128, 128), 128)] - top) * scale)
                lacc = lacc + p
                parts.append(p.astype(BF16))
            acc = acc + dot(jnp.concatenate(parts, axis=1), vbuf[prev, pl.ds(base, TILE), :])
            return lacc, acc

        def joint(i, carry):
            macc, lacc, acc = carry
            return (first(i, macc),) + second(i, (lacc, acc))

        zero = jnp.zeros((cols, 128), F32)
        macc, lacc, acc = lax.fori_loop(0, both, joint, (jnp.full((cols, 128), -jnp.inf, F32), zero, zero))
        lacc, acc = lax.fori_loop(both, n2, second, (lacc, acc))
        macc = lax.fori_loop(both, n1, first, macc)

        @pl.when(g > 0)
        def _():
            w_new = wn[...]
            den = jnp.sum(lacc, axis=1, keepdims=True) + w_new
            o = ((acc + w_new.astype(BF16).astype(F32) * heads_of(vn, g - 1).astype(F32)) / den).astype(BF16)
            g0 = pl.multiple_of((g - 1) * TOKG, TOKG)
            for j in range(heads):
                os_[pl.ds(g0, TOKG), j * 128:(j + 1) * 128] = o[j * TOKG:(j + 1) * TOKG, :]

        peak = jnp.maximum(jnp.max(macc, axis=1, keepdims=True), s_new)
        pk[...] = jnp.broadcast_to(peak, (cols, 128))
        wn[...] = jnp.broadcast_to(jnp.exp2((s_new - peak) * scale), (cols, 128))
        return total, next_total, last

    lax.fori_loop(0, n_groups + 1, step, (jnp.int32(0), total0, total1))
    wo_cp.wait()


def attention(layer, n_tok, lens, w_out, kc, vc, proj=None, qkv=None):
    dma = pltpu.SemaphoreType.DMA
    first_layer = proj is not None
    out_shape = []
    if first_layer:
        x, tab, wq, wk, wv = proj
        model, qdim, kvdim = wq.shape[1], wq.shape[2], wk.shape[2]
        args = [lens, x, tab, wq, wk, wv, w_out, kc, vc]
        specs = [sspec()] + [anyspec()] * 8
        out_shape = [VMEM((n_tok, qdim), BF16), VMEM(w_out.shape[1:], BF16)] + [jax.ShapeDtypeStruct((n_tok, 128), F32)] * 2
        scratch = [VMEM((n_tok, model), BF16), VMEM(tab.shape, F32), VMEM((model, qdim), BF16), VMEM((model, kvdim), BF16), VMEM((model, kvdim), BF16),
                   VMEM((n_tok, qdim), BF16), VMEM((n_tok, kvdim), BF16), VMEM((n_tok, kvdim), BF16), dma((5,))]
    else:
        qdim = qkv[0].shape[1]
        args = [lens, *qkv, w_out, kc, vc]
        specs = [sspec()] + [vspec()] * 3 + [anyspec()] * 3
        out_shape = [VMEM((n_tok, qdim), BF16), VMEM(w_out.shape[1:], BF16)]
        scratch = []
    max_rows = TOKG * kc.shape[2]
    cols = (qdim // 128) * TOKG
    scratch += [VMEM((NSLOT, max_rows + TILE, 128), BF16), VMEM((NSLOT, max_rows + TILE, 128), BF16), VMEM((2, cols, max_rows), F32),
                VMEM((NSLOT, TOKG, 128), jnp.int32), VMEM((NSLOT, TOKG, 128), jnp.int32), VMEM((cols, 128), F32), VMEM((cols, 128), F32), dma((NSLOT,)), dma((NSLOT,)), dma]
    return pl.pallas_call(
        functools.partial(attn_kernel, layer, n_tok, first_layer),
        out_shape=out_shape,
        in_specs=specs,
        out_specs=[vspec()] * len(out_shape),
        scratch_shapes=scratch,
        compiler_params=pltpu.CompilerParams(vmem_limit_bytes=LIM_A if first_layer else LIM_B),
        name=f"attention{layer}",
    )(*args)


NCH = 4


def peers():
    me = lax.axis_index("ep")
    core = me % 2
    x = me // 2
    return me, x * 2 + (1 - core), (1 - x) * 2 + core, (1 - x) * 2 + (1 - core)


def barrier(devices):
    sem = pltpu.get_barrier_semaphore()
    for d in devices:
        pl.semaphore_signal(sem, inc=1, device_id=d, device_id_type=MESH)
    return lambda: pl.semaphore_wait(sem, len(devices))


def rcopy(src, dst, ssem, rsem, dev):
    return pltpu.make_async_remote_copy(src_ref=src, dst_ref=dst, send_sem=ssem, recv_sem=rsem, device_id=dev, device_id_type=MESH)


def weight_copies(layer, e, f, slot, hbm, buf, sems):
    wg_hbm, wu_hbm, wd_hbm = hbm
    cols = pl.ds(f * FT, FT) if isinstance(f, int) else pl.ds(pl.multiple_of(f * FT, FT), FT)
    return (pltpu.make_async_copy(wg_hbm.at[layer, e, :, cols], buf[0].at[slot], sems.at[slot, 0]),
            pltpu.make_async_copy(wu_hbm.at[layer, e, :, cols], buf[1].at[slot], sems.at[slot, 1]),
            pltpu.make_async_copy(wd_hbm.at[layer, e, cols, :], buf[2].at[slot], sems.at[slot, 2]))


def dispatch_kernel(layer, steps, n_loc, os_ref, x_ref, ids_ref, wr_ref, wo, wg_hbm, wu_hbm, wd_hbm, *refs):
    first_layer = layer == 0
    if first_layer:
        a_ref, uall, rrow, mcol, idsall, pg, pu, pd, idsbuf, *sems = refs
        psem, s_p, r_p, s_x, r_x, s_f, r_f, s_i, r_i = sems
    else:
        a_ref, uall, rrow, mcol, pg, pu, pd, *sems = refs
        psem, s_p, r_p, s_x, r_x, s_f, r_f = sems
        idsall = ids_ref
    n = os_ref.shape[0]
    ch = n // NCH
    pool = lax.axis_index("pool")
    me, part, xp, diag = peers()
    devs = [{"ep": part}, {"ep": xp}] + ([{"ep": diag}] if first_layer else [])
    arrive = barrier(devs)

    def rows(ep, c):
        return pl.ds(pl.multiple_of(ep * n + c * ch, ch), ch)

    ics = []
    if first_layer:
        t0 = pl.multiple_of(pool * n, n)
        idsbuf[...] = jnp.zeros(idsbuf.shape, jnp.int32)
        for l in range(ids_ref.shape[0]):
            idsbuf[2 * l:2 * l + 2, :] = ids_ref[l, :, pl.ds(t0, n)]
        idsall[me] = idsbuf[...]
        arrive()
        for i, d in enumerate(devs):
            cp = rcopy(idsbuf, idsall.at[me], s_i.at[i], r_i.at[i], d)
            cp.start()
            ics.append(cp)
    xs, ps = [], []
    half = n // 2
    for hf in range(2):
        r = pl.ds(hf * half, half)
        if first_layer:
            xr = x_ref[pl.ds(pl.multiple_of(pool * n + hf * half, half), half), :]
        else:
            xr = x_ref[r, :]
        a = (xr.astype(F32) + dot(os_ref[r, :], wo[...])).astype(BF16)
        a_ref[r, :] = a
        uall[pl.ds(pl.multiple_of(me * n + hf * half, half), half), :] = rms_bf16(a.astype(F32))
        if hf == 0 and not first_layer:
            arrive()
        for c in range(hf * NCH // 2, (hf + 1) * NCH // 2):
            cp = rcopy(uall.at[rows(me, c)], uall.at[rows(me, c)], s_x.at[c], r_x.at[c], {"ep": xp})
            cp.start()
            xs.append(cp)
            cp = rcopy(uall.at[rows(me, c)], uall.at[rows(me, c)], s_p.at[c], r_p.at[c], {"ep": part})
            cp.start()
            ps.append(cp)
    hbm = (wg_hbm, wu_hbm, wd_hbm)

    def prefetch(f, _):
        for cp in weight_copies(layer, 0, f, f, hbm, (pg, pu, pd), psem):
            cp.start()
        return 0

    lax.fori_loop(0, steps, prefetch, 0)
    for cp in ics:
        cp.wait()

    tokens = 4 * n
    e0 = me * n_loc
    ids_row = [jnp.concatenate([idsall[b, 2 * layer + k:2 * layer + k + 1, :] for b in range(4)], axis=1) for k in range(2)]
    row8 = lax.broadcasted_iota(jnp.int32, (8, tokens), 0)
    hit = ((ids_row[0] == row8 + e0) | (ids_row[1] == row8 + e0)) & (row8 < n_loc)
    hit_f = hit.astype(F32)
    tri = (lax.broadcasted_iota(jnp.int32, (tokens, tokens), 0) < lax.broadcasted_iota(jnp.int32, (tokens, tokens), 1)).astype(F32).astype(BF16)
    rank = jnp.where(hit_f > 0, dot(hit_f.astype(BF16), tri), -1.0)
    rrow[...] = rank
    idf = jnp.where(row8 == 2, jnp.broadcast_to(ids_row[0].astype(F32), (8, tokens)),
                    jnp.where(row8 == 3, jnp.broadcast_to(ids_row[1].astype(F32), (8, tokens)), rank))
    mcol[...] = jnp.transpose(idf)

    w = wr_ref[layer]
    w1 = w.astype(BF16).astype(F32)
    w2 = (w - w1).astype(BF16).astype(F32)
    w3 = w - w1 - w2
    wr = jnp.concatenate([w1, w2, w3, jnp.zeros((104, w.shape[1]), F32)], axis=0).astype(BF16)
    e0f = e0.astype(F32)

    def gates(ep):
        r = pl.ds(pl.multiple_of(ep * n, n), n)
        lg = lax.dot_general(uall[r, :], wr, (((1,), (1,)), ((), ())), preferred_element_type=F32)
        lg = lg + pltpu.roll(lg, 120, 1) + pltpu.roll(lg, 112, 1)
        lane = lax.broadcasted_iota(jnp.int32, (n, 128), 1).astype(F32)
        col = mcol[r, :]
        id0, id1 = col[:, 2:3], col[:, 3:4]
        l0 = jnp.sum(jnp.where(lane == id0, lg, 0.0), axis=1, keepdims=True)
        l1 = jnp.sum(jnp.where(lane == id1, lg, 0.0), axis=1, keepdims=True)
        top = jnp.maximum(l0, l1)
        x0 = jnp.exp(l0 - top)
        x1 = jnp.exp(l1 - top)
        den = x0 + x1
        lane8 = lax.broadcasted_iota(jnp.int32, (n, 8), 1)
        expert = (lane8 - 2).astype(F32) + e0f
        g = jnp.where(id0 == expert, x0 / den, 0.0) + jnp.where(id1 == expert, x1 / den, 0.0)
        mcol[r, :] = jnp.where(lane8 < 2, col, g)

    gates(me)
    fs = []

    def forward(c):
        xs[c].wait_recv()
        cp = rcopy(uall.at[rows(xp, c)], uall.at[rows(xp, c)], s_f.at[c], r_f.at[c], {"ep": part})
        cp.start()
        fs.append(cp)

    for c in range(NCH - 1):
        forward(c)
    for cp in ps:
        cp.wait()
    gates(part)
    forward(NCH - 1)
    gates(xp)
    for cp in fs:
        cp.wait()
    gates(diag)
    for cp in xs:
        cp.wait_send()
    for f in range(steps):
        for cp in weight_copies(layer, 0, f, f, hbm, (pg, pu, pd), psem):
            cp.wait()


def dispatch(layer, os_, x, ids, wr, wo, wg, wu, wd):
    n, qdim = os_.shape
    model = wo.shape[1]
    n_loc, ff = wg.shape[1], wg.shape[3]
    steps = ff // FT
    dma = pltpu.SemaphoreType.DMA
    out_shape = [jax.ShapeDtypeStruct((n, model), BF16), jax.ShapeDtypeStruct((4 * n, model), BF16),
                 jax.ShapeDtypeStruct((8, 4 * n), F32), jax.ShapeDtypeStruct((4 * n, 8), F32)]
    scratch = []
    sems = [dma((steps, 3))] + [dma((NCH,))] * 6
    if layer == 0:
        out_shape.append(jax.ShapeDtypeStruct((4, 8, n), jnp.int32))
        scratch.append(VMEM((8, n), jnp.int32))
        sems += [dma((3,)), dma((3,))]
    n_small = len(out_shape)
    out_shape += [VMEM((steps, model, FT), BF16), VMEM((steps, model, FT), BF16), VMEM((steps, FT, model), BF16)]
    return pl.pallas_call(
        functools.partial(dispatch_kernel, layer, steps, n_loc),
        out_shape=out_shape,
        in_specs=[vspec()] * 5 + [anyspec()] * 3,
        out_specs=[vspec()] * n_small + [vspec()] * 3,
        scratch_shapes=scratch + sems,
        compiler_params=pltpu.CompilerParams(collective_id=2 * layer, has_side_effects=True, vmem_limit_bytes=LIM_D),
        name=f"dispatch{layer}",
    )(os_, x, ids, wr, wo, wg, wu, wd)


def expert_kernel(layer, u_ref, rrow_ref, mcol_ref, pg, pu, pd, wg_hbm, wu_hbm, wd_hbm, y_ref, wg, wu, wd, xe, yacc, sems):
    n = u_ref.shape[0]
    steps = pg.shape[0]
    n_loc = wg_hbm.shape[1]
    hbm = (wg_hbm, wu_hbm, wd_hbm)
    own = (wg, wu, wd)

    for e in range(1, n_loc):
        def issue(f, _, e=e):
            for c in weight_copies(layer, e, f, (e - 1) * steps + f, hbm, own, sems):
                c.start()
            return 0
        lax.fori_loop(0, steps, issue, 0)

    for e in range(n_loc):
        rank_row = rrow_ref[e:e + 1, :]
        count = jnp.sum((rank_row >= 0).astype(F32)).astype(jnp.int32)
        lo = 0
        for m in SIZES:
            @pl.when((count <= m) & ((count > lo) | (lo == 0)))
            def _(m=m, e=e):
                sel = (rank_row == lax.broadcasted_iota(jnp.int32, (m, n), 0).astype(F32)).astype(F32).astype(BF16)
                xe[pl.ds(0, m), :] = dot(sel, u_ref[...]).astype(BF16)
                yacc[pl.ds(0, m), :] = jnp.zeros((m, yacc.shape[1]), F32)

                def step(f, _):
                    if e == 0:
                        w1, w3, w2 = pg, pu, pd
                        slot = f
                    else:
                        w1, w3, w2 = own
                        slot = (e - 1) * steps + f
                        for c in weight_copies(layer, e, f, slot, hbm, own, sems):
                            c.wait()
                    gate = dot(xe[pl.ds(0, m), :], w1[slot])
                    up = dot(xe[pl.ds(0, m), :], w3[slot])
                    inner = (gate * jax.nn.sigmoid(gate) * up).astype(BF16)
                    yacc[pl.ds(0, m), :] += dot(inner, w2[slot])
                    return 0

                lax.fori_loop(0, steps, step, 0)
                y_ref[pl.ds(e * n, m), :] = yacc[pl.ds(0, m), :].astype(BF16)
                if m < n:
                    y_ref[pl.ds(e * n + m, n - m), :] = jnp.zeros((n - m, y_ref.shape[1]), BF16)
            lo = m


def experts(layer, u_all, rrow, mcol, pre, wg, wu, wd):
    n, model = u_all.shape
    steps = pre[0].shape[0]
    n_loc = wg.shape[1]
    slots = steps * (n_loc - 1)
    return pl.pallas_call(
        functools.partial(expert_kernel, layer),
        out_shape=jax.ShapeDtypeStruct((n_loc * n, model), BF16),
        in_specs=[vspec()] * 6 + [anyspec()] * 3,
        out_specs=vspec(),
        scratch_shapes=[VMEM((slots, model, FT), BF16), VMEM((slots, model, FT), BF16), VMEM((slots, FT, model), BF16),
                        VMEM((n, model), BF16), VMEM((n, model), F32), pltpu.SemaphoreType.DMA((slots, 3))],
        compiler_params=pltpu.CompilerParams(vmem_limit_bytes=LIM_E),
        name=f"experts{layer}",
    )(u_all, rrow, mcol, *pre, wg, wu, wd)


def combine_kernel(last, layer, y_ref, mcol_ref, a_ref, *refs):
    if last:
        out_ref, p_d, p_x, p_p, p_me, own, mid, far, *sems = refs
        s_o, r_o, s_m, r_m, s_f, r_f, s_y, r_y = sems
    else:
        (cos_ref, sin_ref, wq_hbm, wk_hbm, wv_hbm, out_ref, qs, kn, vn,
         p_d, p_x, p_p, p_me, own, mid, far, wq, wk, wv, *sems) = refs
        s_o, r_o, s_m, r_m, s_f, r_f, wsem = sems
    n = a_ref.shape[0]
    ch = n // CCH
    nn = mcol_ref.shape[0]
    me, part, xp, diag = peers()
    devs = [{"ep": part}, {"ep": xp}]
    if last:
        pool = lax.axis_index("pool")
        devs.append({"pool": 1 - pool})
    else:
        w_copies = [pltpu.make_async_copy(src.at[layer + 1], dst, wsem.at[i])
                    for i, (src, dst) in enumerate(((wq_hbm, wq), (wk_hbm, wk), (wv_hbm, wv)))]
        for c in w_copies:
            c.start()

    def partial(ep):
        col = mcol_ref[pl.ds(pl.multiple_of(ep * n, n), n), :]
        slot = lax.broadcasted_iota(jnp.int32, (n, nn), 1).astype(F32)
        total = None
        for e in range(y_ref.shape[0] // nn):
            sel = (col[:, e:e + 1] == slot).astype(F32).astype(BF16)
            t = dot(sel, y_ref[e * nn:(e + 1) * nn, :]) * col[:, 2 + e:3 + e]
            total = t if total is None else total + t
        return total

    arrive = barrier(devs)
    p_d[...] = partial(diag)
    arrive()
    mids, fars, ys = [], [], []
    for c in range(CCH):
        r = pl.ds(c * ch, ch)
        cp = rcopy(p_d.at[r], mid.at[r], s_m.at[c], r_m.at[c], devs[0])
        cp.start()
        mids.append(cp)
    p_x[...] = partial(xp)

    def send(c):
        r = pl.ds(c * ch, ch)
        mids[c].wait_recv()
        p_x[r, :] = p_x[r, :] + mid[r, :]
        if c >= 2:
            fars[c - 2].wait_send()
        cp = rcopy(p_x.at[r], far.at[r], s_f.at[c], r_f.at[c], devs[1])
        cp.start()
        fars.append(cp)

    def receive(c):
        r = pl.ds(c * ch, ch)
        fars[c].wait_recv()
        res = (p_me[r, :] + far[r, :]).astype(BF16)
        if last:
            o = pl.ds(pl.multiple_of(pool * n + c * ch, ch), ch)
            out_ref[o, :] = res
            cp = rcopy(out_ref.at[o], out_ref.at[o], s_y.at[c], r_y.at[c], devs[2])
            cp.start()
            ys.append(cp)
        else:
            out_ref[r, :] = res
            if c % (CCH // 2) == CCH // 2 - 1:
                r2 = pl.ds(c * ch + ch - n // 2, n // 2)
                h = rms_bf16(out_ref[r2, :].astype(F32))
                project(h, cos_ref[r2, :], sin_ref[r2, :], wq, wk, wv, qs, kn, vn, r2)

    send(0)
    send(1)
    p_p[...] = partial(part)
    own_cp = rcopy(p_p, own, s_o, r_o, devs[0])
    own_cp.start()
    p_me[...] = partial(me)
    own_cp.wait()
    p_me[...] = a_ref[...].astype(F32) + (p_me[...] + own[...])
    if not last:
        for c in w_copies:
            c.wait()
    for c in range(2, CCH):
        send(c)
        receive(c - 2)
    receive(CCH - 2)
    receive(CCH - 1)
    for c in range(CCH):
        mids[c].wait_send()
    for c in range(CCH - 2, CCH):
        fars[c].wait_send()
    for cp in ys:
        cp.wait()


def combine(layer, last, y, mcol, a, nxt=None):
    n, model = a.shape
    dma = pltpu.SemaphoreType.DMA
    sems = [dma, dma, dma((CCH,)), dma((CCH,)), dma((CCH,)), dma((CCH,))]
    args = [y, mcol, a]
    specs = [vspec()] * 3
    scratch = [VMEM((n, model), F32) for _ in range(7)]
    if last:
        sems += [dma((CCH,)), dma((CCH,))]
        out_shape = jax.ShapeDtypeStruct((2 * n, model), BF16)
        out_specs = vspec()
    else:
        cos, sin, wq, wk, wv = nxt
        args += [cos, sin, wq, wk, wv]
        specs += [vspec()] * 2 + [anyspec()] * 3
        sems += [dma((3,))]
        scratch += [VMEM(w.shape[1:], BF16) for w in (wq, wk, wv)]
        out_shape = [jax.ShapeDtypeStruct((n, model), BF16)] + [jax.ShapeDtypeStruct((n, w.shape[2]), BF16) for w in (wq, wk, wv)]
        out_specs = [vspec()] * 4
    return pl.pallas_call(
        functools.partial(combine_kernel, last, layer),
        out_shape=out_shape,
        in_specs=specs,
        out_specs=out_specs,
        scratch_shapes=scratch + sems,
        compiler_params=pltpu.CompilerParams(collective_id=2 * layer + 1, has_side_effects=True, vmem_limit_bytes=LIM_C),
        name=f"combine{layer}",
    )(*args)


def solution(mesh):
    def body(hidden, k_cache, v_cache, lengths, expert_ids, w_query, w_key, w_value, w_out, w_router, w_gate, w_up, w_down):
        n_layers, _, seq, kvh, hd = k_cache.shape
        n_tok = hidden.shape[0] // 2
        kc = k_cache.reshape(n_layers, -1, seq * kvh, hd)
        vc = v_cache.reshape(n_layers, -1, seq * kvh, hd)
        ids = expert_ids.transpose(0, 2, 1)
        wr = w_router.transpose(0, 2, 1)
        tab = jnp.asarray(rope_table(seq, hd))
        w_query, w_key, w_value, w_out, w_gate, w_up, w_down, kc, vc, tab, hidden_h, lens_h = (
            pltpu.with_memory_space_constraint(v, pltpu.HBM) for v in (w_query, w_key, w_value, w_out, w_gate, w_up, w_down, kc, vc, tab, hidden, lengths))
        state = hidden
        qkv = None
        for layer in range(n_layers):
            last = layer == n_layers - 1
            if layer == 0:
                att, wo, cos, sin = attention(layer, n_tok, lens_h, w_out, kc, vc, proj=(hidden_h, tab, w_query, w_key, w_value))
            else:
                att, wo = attention(layer, n_tok, lens_h, w_out, kc, vc, qkv=qkv)
            outs = dispatch(layer, att, state, ids, wr, wo, w_gate, w_up, w_down)
            a, u_all, rrow, mcol = outs[:4]
            if layer == 0:
                ids = outs[4]
            y = experts(layer, u_all, rrow, mcol, outs[-3:], w_gate, w_up, w_down)
            if last:
                return combine(layer, True, y, mcol, a)
            state, *qkv = combine(layer, False, y, mcol, a, nxt=(cos, sin, w_query, w_key, w_value))

    rows_spec = ("dp", "ep")
    in_specs = (P(rows_spec, None), P(None, rows_spec), P(None, rows_spec), P(rows_spec), P(None, rows_spec, None), P(), P(), P(), P(), P(), P(None, "ep"), P(None, "ep"), P(None, "ep"))
    return jax.shard_map(body, mesh=mesh, in_specs=in_specs, out_specs=P(rows_spec, None), check_vma=False)
```

```python
import functools

import numpy as np

import jax
import jax.numpy as jnp
from jax import lax
from jax.experimental import pallas as pl
from jax.experimental.pallas import tpu as pltpu
from jax.sharding import PartitionSpec as P

MESH = pl.DeviceIdType.MESH
EPSILON = 1e-6
ROPE_BASE = 10000.0
VMEM = pltpu.VMEM
F32 = jnp.float32
BF16 = jnp.bfloat16

TOKG = 16
TILE = 1024
FT = 512
NSLOT = 3
CCH = 8
LIM_A = 50 * 1024 * 1024
LIM_B = 50 * 1024 * 1024
LIM_D = 8 * 1024 * 1024
LIM_E = 27 * 1024 * 1024
LIM_C = 16 * 1024 * 1024
SIZES = (128, 400, 512)


def vspec():
    return pl.BlockSpec(memory_space=VMEM)


def anyspec():
    return pl.BlockSpec(memory_space=pltpu.HBM)


def sspec():
    return pl.BlockSpec(memory_space=pltpu.SMEM)


def dot(a, b):
    return jnp.dot(a, b, preferred_element_type=F32)


def rms_bf16(v):
    return (v * lax.rsqrt(jnp.mean(v * v, axis=-1, keepdims=True) + EPSILON)).astype(BF16)


def rope_table(seq, hd):
    half = hd // 2
    freqs = np.power(np.float32(ROPE_BASE), (np.float32(-2.0) * np.arange(half, dtype=np.float32) / np.float32(hd)))
    angle = np.arange(seq + 1, dtype=np.float32)[:, None] * freqs.astype(np.float32)[None, :]
    wide = angle.astype(np.float64)
    return np.concatenate([np.cos(wide), np.sin(wide)], axis=1).astype(np.float32)


def rope(vec, cos, sin):
    return vec * cos + pltpu.roll(vec, 64, 1) * sin


def project(h, cos, sin, wq, wk, wv, qs, kn, vn, rows):
    q = dot(h, wq[...])
    k = dot(h, wk[...])
    v = dot(h, wv[...])
    for j in range(q.shape[1] // 128):
        qs[rows, j * 128:(j + 1) * 128] = rope(q[:, j * 128:(j + 1) * 128], cos, sin).astype(BF16)
    for j in range(k.shape[1] // 128):
        kn[rows, j * 128:(j + 1) * 128] = rope(k[:, j * 128:(j + 1) * 128], cos, sin).astype(BF16)
    vn[rows, :] = v.astype(BF16)


def attn_kernel(layer, n_tok, first_layer, lens_hbm, *refs):
    if first_layer:
        (x_hbm, tab_hbm, wq_hbm, wk_hbm, wv_hbm, wo_hbm, kc, vc, os_, wo, cos_ref, sin_ref,
         x_ref, tab_ref, wq, wk, wv, qs, kn, vn, wsem, kbuf, vbuf, sbuf, mst, men, pk, wn, lens_ref, lsem, ksem, vsem, osem) = refs
    else:
        qs, kn, vn, wo_hbm, kc, vc, os_, wo, kbuf, vbuf, sbuf, mst, men, pk, wn, lens_ref, lsem, ksem, vsem, osem = refs
    t0 = lax.axis_index("pool") * n_tok
    lens_cp = pltpu.make_async_copy(lens_hbm, lens_ref, lsem)
    lens_cp.start()
    heads = qs.shape[1] // 128
    n_groups = n_tok // TOKG
    hpk = heads // 2
    cols = heads * TOKG

    def padded(ln):
        return pl.multiple_of(lax.shift_left(lax.shift_right_logical(ln + 7, 3), 4), 16)

    def start_keys(g):
        slot = lax.rem(g, NSLOT)
        off = 0
        for i in range(TOKG):
            tok = t0 + g * TOKG + i
            ln = lens_ref[tok]
            n = padded(ln)
            off = pl.multiple_of(off, 16)
            pltpu.make_async_copy(kc.at[layer, tok, pl.ds(0, n), :], kbuf.at[slot, pl.ds(off, n), :], ksem.at[slot]).start()
            mst[slot, i:i + 1, :] = jnp.full((1, 128), off, jnp.int32)
            men[slot, i:i + 1, :] = jnp.full((1, 128), off + 2 * ln, jnp.int32)
            off = off + n
        return jnp.asarray(off, jnp.int32)

    def start_vals(g):
        slot = lax.rem(g, NSLOT)
        off = 0
        for i in range(TOKG):
            tok = t0 + g * TOKG + i
            n = padded(lens_ref[tok])
            off = pl.multiple_of(off, 16)
            pltpu.make_async_copy(vc.at[layer, tok, pl.ds(0, n), :], vbuf.at[slot, pl.ds(off, n), :], vsem.at[slot]).start()
            off = off + n

    if first_layer:
        w_copies = [pltpu.make_async_copy(src.at[layer], dst, wsem.at[i])
                    for i, (src, dst) in enumerate(((wq_hbm, wq), (wk_hbm, wk), (wv_hbm, wv)))]
        x_cp = pltpu.make_async_copy(x_hbm.at[pl.ds(pl.multiple_of(t0, n_tok), n_tok), :], x_ref, wsem.at[3])
        tab_cp = pltpu.make_async_copy(tab_hbm, tab_ref, wsem.at[4])
        x_cp.start()
        tab_cp.start()
        for c in w_copies:
            c.start()
    lens_cp.wait()
    total0 = start_keys(jnp.int32(0))
    start_vals(jnp.int32(0))
    total1 = start_keys(jnp.int32(1))
    wo_cp = pltpu.make_async_copy(wo_hbm.at[layer], wo, osem)
    wo_cp.start()
    if first_layer:
        x_cp.wait()
        tab_cp.wait()
        h = rms_bf16(x_ref[...].astype(F32))

        def pick(i, _):
            cos_ref[pl.ds(i, 1), :] = tab_ref[pl.ds(lens_ref[t0 + i], 1), :]
            return 0
        lax.fori_loop(0, n_tok, pick, 0)
        both = cos_ref[...]
        swapped = pltpu.roll(both, 64, 1)
        low = lax.broadcasted_iota(jnp.int32, both.shape, 1) < 64
        cos = jnp.where(low, both, swapped)
        sin = jnp.where(low, -swapped, both)
        cos_ref[...] = cos
        sin_ref[...] = sin
        for c in w_copies:
            c.wait()
        project(h, cos, sin, wq, wk, wv, qs, kn, vn, pl.ds(0, n_tok))
    scale = 128.0 ** -0.5 * 1.4426950408889634

    lane = lax.broadcasted_iota(jnp.int32, (cols, 128), 1)
    kv = (lax.broadcasted_iota(jnp.int32, (cols, 128), 0) >= (hpk * TOKG)).astype(jnp.int32)
    mine = (lane & 1) == kv

    def heads_of(ref, g):
        row = ref[pl.ds(pl.multiple_of(g * TOKG, TOKG), TOKG), :]
        per = heads // (ref.shape[1] // 128)
        return jnp.concatenate([row[:, (j // per) * 128:(j // per + 1) * 128] for j in range(heads)], axis=0)

    def tiles_of(total):
        return lax.shift_right_logical(total + TILE - 1, TILE.bit_length() - 1)

    def step(g, totals):
        prev_total, total, next_total = totals
        prev_total = pl.multiple_of(prev_total, 16)
        total = pl.multiple_of(total, 16)
        slot = lax.rem(g, NSLOT)
        prev = lax.rem(g + NSLOT - 1, NSLOT)
        sl, sp = g & 1, 1 - (g & 1)
        last = lax.cond(g + 2 < n_groups, lambda: start_keys(g + 2), lambda: jnp.int32(0))

        @pl.when(g + 1 < n_groups)
        def _():
            start_vals(g + 1)

        gc = jnp.minimum(g, n_groups - 1)
        q2 = heads_of(qs, gc)
        s_new = jnp.sum(q2.astype(F32) * heads_of(kn, gc).astype(F32), axis=1, keepdims=True)
        start = jnp.where(mine, jnp.concatenate([mst[slot]] * heads, axis=0) - lane, 1 << 30)
        end = jnp.concatenate([men[slot]] * heads, axis=0) - lane
        n1 = jnp.where(g < n_groups, tiles_of(total), 0)
        n2 = jnp.where(g > 0, tiles_of(prev_total), 0)
        both = jnp.minimum(n1, n2)

        @pl.when(g < n_groups)
        def _():
            pltpu.make_async_copy(kbuf.at[slot, pl.ds(0, total), :], kbuf.at[slot, pl.ds(0, total), :], ksem.at[slot]).wait()

        @pl.when(g > 0)
        def _():
            vbuf[prev, pl.ds(prev_total, TILE), :] = jnp.zeros((TILE, 128), BF16)
            pltpu.make_async_copy(vbuf.at[prev, pl.ds(0, prev_total), :], vbuf.at[prev, pl.ds(0, prev_total), :], vsem.at[prev]).wait()

        def first(i, macc):
            base = pl.multiple_of(i * TILE, TILE)
            for j in range(TILE // 256):
                at = pl.multiple_of(base + j * 256, 256)
                s = lax.dot_general(q2, kbuf[slot, pl.ds(at, 256), :], (((1,), (1,)), ((), ())), preferred_element_type=F32)
                for p in range(2):
                    off = at + p * 128
                    part = jnp.where((start <= off) & (end > off), s[:, p * 128:(p + 1) * 128], -jnp.inf)
                    sbuf[sl, :, pl.ds(pl.multiple_of(off, 128), 128)] = part
                    macc = jnp.maximum(macc, part)
            return macc

        def second(i, carry):
            lacc, acc = carry
            base = pl.multiple_of(i * TILE, TILE)
            top = pk[...]
            parts = []
            for j in range(TILE // 128):
                p = jnp.exp2((sbuf[sp, :, pl.ds(pl.multiple_of(base + j * 128, 128), 128)] - top) * scale)
                lacc = lacc + p
                parts.append(p.astype(BF16))
            acc = acc + dot(jnp.concatenate(parts, axis=1), vbuf[prev, pl.ds(base, TILE), :])
            return lacc, acc

        def joint(i, carry):
            macc, lacc, acc = carry
            return (first(i, macc),) + second(i, (lacc, acc))

        zero = jnp.zeros((cols, 128), F32)
        macc, lacc, acc = lax.fori_loop(0, both, joint, (jnp.full((cols, 128), -jnp.inf, F32), zero, zero))
        lacc, acc = lax.fori_loop(both, n2, second, (lacc, acc))
        macc = lax.fori_loop(both, n1, first, macc)

        @pl.when(g > 0)
        def _():
            w_new = wn[...]
            den = jnp.sum(lacc, axis=1, keepdims=True) + w_new
            o = ((acc + w_new.astype(BF16).astype(F32) * heads_of(vn, g - 1).astype(F32)) / den).astype(BF16)
            g0 = pl.multiple_of((g - 1) * TOKG, TOKG)
            for j in range(heads):
                os_[pl.ds(g0, TOKG), j * 128:(j + 1) * 128] = o[j * TOKG:(j + 1) * TOKG, :]

        peak = jnp.maximum(jnp.max(macc, axis=1, keepdims=True), s_new)
        pk[...] = jnp.broadcast_to(peak, (cols, 128))
        wn[...] = jnp.broadcast_to(jnp.exp2((s_new - peak) * scale), (cols, 128))
        return total, next_total, last

    lax.fori_loop(0, n_groups + 1, step, (jnp.int32(0), total0, total1))
    wo_cp.wait()


def attention(layer, n_tok, lens, w_out, kc, vc, proj=None, qkv=None):
    dma = pltpu.SemaphoreType.DMA
    first_layer = proj is not None
    out_shape = []
    if first_layer:
        x, tab, wq, wk, wv = proj
        model, qdim, kvdim = wq.shape[1], wq.shape[2], wk.shape[2]
        args = [lens, x, tab, wq, wk, wv, w_out, kc, vc]
        specs = [anyspec()] * 9
        out_shape = [VMEM((n_tok, qdim), BF16), VMEM(w_out.shape[1:], BF16)] + [jax.ShapeDtypeStruct((n_tok, 128), F32)] * 2
        scratch = [VMEM((n_tok, model), BF16), VMEM(tab.shape, F32), VMEM((model, qdim), BF16), VMEM((model, kvdim), BF16), VMEM((model, kvdim), BF16),
                   VMEM((n_tok, qdim), BF16), VMEM((n_tok, kvdim), BF16), VMEM((n_tok, kvdim), BF16), dma((5,))]
    else:
        qdim = qkv[0].shape[1]
        args = [lens, *qkv, w_out, kc, vc]
        specs = [anyspec()] + [vspec()] * 3 + [anyspec()] * 3
        out_shape = [VMEM((n_tok, qdim), BF16), VMEM(w_out.shape[1:], BF16)]
        scratch = []
    max_rows = TOKG * kc.shape[2]
    cols = (qdim // 128) * TOKG
    scratch += [VMEM((NSLOT, max_rows + TILE, 128), BF16), VMEM((NSLOT, max_rows + TILE, 128), BF16), VMEM((2, cols, max_rows), F32),
                VMEM((NSLOT, TOKG, 128), jnp.int32), VMEM((NSLOT, TOKG, 128), jnp.int32), VMEM((cols, 128), F32), VMEM((cols, 128), F32), pltpu.SMEM(lens.shape, jnp.int32), dma, dma((NSLOT,)), dma((NSLOT,)), dma]
    return pl.pallas_call(
        functools.partial(attn_kernel, layer, n_tok, first_layer),
        out_shape=out_shape,
        in_specs=specs,
        out_specs=[vspec()] * len(out_shape),
        scratch_shapes=scratch,
        compiler_params=pltpu.CompilerParams(vmem_limit_bytes=LIM_A if first_layer else LIM_B),
        name=f"attention{layer}",
    )(*args)


NCH = 4


def peers():
    me = lax.axis_index("ep")
    core = me % 2
    x = me // 2
    return me, x * 2 + (1 - core), (1 - x) * 2 + core, (1 - x) * 2 + (1 - core)


def barrier(devices):
    sem = pltpu.get_barrier_semaphore()
    for d in devices:
        pl.semaphore_signal(sem, inc=1, device_id=d, device_id_type=MESH)
    return lambda: pl.semaphore_wait(sem, len(devices))


def rcopy(src, dst, ssem, rsem, dev):
    return pltpu.make_async_remote_copy(src_ref=src, dst_ref=dst, send_sem=ssem, recv_sem=rsem, device_id=dev, device_id_type=MESH)


def weight_copies(layer, e, f, slot, hbm, buf, sems):
    wg_hbm, wu_hbm, wd_hbm = hbm
    cols = pl.ds(f * FT, FT) if isinstance(f, int) else pl.ds(pl.multiple_of(f * FT, FT), FT)
    return (pltpu.make_async_copy(wg_hbm.at[layer, e, :, cols], buf[0].at[slot], sems.at[slot, 0]),
            pltpu.make_async_copy(wu_hbm.at[layer, e, :, cols], buf[1].at[slot], sems.at[slot, 1]),
            pltpu.make_async_copy(wd_hbm.at[layer, e, cols, :], buf[2].at[slot], sems.at[slot, 2]))


def dispatch_kernel(layer, steps, n_loc, os_ref, x_ref, ids_ref, wr_ref, wo, wg_hbm, wu_hbm, wd_hbm, *refs):
    first_layer = layer == 0
    if first_layer:
        a_ref, uall, rrow, mcol, idsall, pg, pu, pd, idsbuf, *sems = refs
        psem, s_p, r_p, s_x, r_x, s_f, r_f, s_i, r_i = sems
    else:
        a_ref, uall, rrow, mcol, pg, pu, pd, *sems = refs
        psem, s_p, r_p, s_x, r_x, s_f, r_f = sems
        idsall = ids_ref
    n = os_ref.shape[0]
    ch = n // NCH
    pool = lax.axis_index("pool")
    me, part, xp, diag = peers()
    devs = [{"ep": part}, {"ep": xp}] + ([{"ep": diag}] if first_layer else [])
    arrive = barrier(devs)

    def rows(ep, c):
        return pl.ds(pl.multiple_of(ep * n + c * ch, ch), ch)

    ics = []
    if first_layer:
        t0 = pl.multiple_of(pool * n, n)
        idsbuf[...] = jnp.zeros(idsbuf.shape, jnp.int32)
        for l in range(ids_ref.shape[0]):
            idsbuf[2 * l:2 * l + 2, :] = ids_ref[l, :, pl.ds(t0, n)]
        idsall[me] = idsbuf[...]
    xs, ps = [], []
    half = n // 2
    for hf in range(2):
        r = pl.ds(hf * half, half)
        if first_layer:
            xr = x_ref[pl.ds(pl.multiple_of(pool * n + hf * half, half), half), :]
        else:
            xr = x_ref[r, :]
        a = (xr.astype(F32) + dot(os_ref[r, :], wo[...])).astype(BF16)
        a_ref[r, :] = a
        uall[pl.ds(pl.multiple_of(me * n + hf * half, half), half), :] = rms_bf16(a.astype(F32))
        if hf == 0:
            arrive()
        for c in range(hf * NCH // 2, (hf + 1) * NCH // 2):
            cp = rcopy(uall.at[rows(me, c)], uall.at[rows(me, c)], s_x.at[c], r_x.at[c], {"ep": xp})
            cp.start()
            xs.append(cp)
            cp = rcopy(uall.at[rows(me, c)], uall.at[rows(me, c)], s_p.at[c], r_p.at[c], {"ep": part})
            cp.start()
            ps.append(cp)
    if first_layer:
        for i, d in enumerate(devs):
            cp = rcopy(idsbuf, idsall.at[me], s_i.at[i], r_i.at[i], d)
            cp.start()
            ics.append(cp)
    hbm = (wg_hbm, wu_hbm, wd_hbm)

    def prefetch(f, _):
        for cp in weight_copies(layer, 0, f, f, hbm, (pg, pu, pd), psem):
            cp.start()
        return 0

    lax.fori_loop(0, steps, prefetch, 0)
    for cp in ics:
        cp.wait()

    tokens = 4 * n
    e0 = me * n_loc
    ids_row = [jnp.concatenate([idsall[b, 2 * layer + k:2 * layer + k + 1, :] for b in range(4)], axis=1) for k in range(2)]
    row8 = lax.broadcasted_iota(jnp.int32, (8, tokens), 0)
    hit = ((ids_row[0] == row8 + e0) | (ids_row[1] == row8 + e0)) & (row8 < n_loc)
    hit_f = hit.astype(F32)
    tri = (lax.broadcasted_iota(jnp.int32, (tokens, tokens), 0) < lax.broadcasted_iota(jnp.int32, (tokens, tokens), 1)).astype(F32).astype(BF16)
    rank = jnp.where(hit_f > 0, dot(hit_f.astype(BF16), tri), -1.0)
    rrow[...] = rank
    idf = jnp.where(row8 == 2, jnp.broadcast_to(ids_row[0].astype(F32), (8, tokens)),
                    jnp.where(row8 == 3, jnp.broadcast_to(ids_row[1].astype(F32), (8, tokens)), rank))
    mcol[...] = jnp.transpose(idf)

    w = wr_ref[layer]
    w1 = w.astype(BF16).astype(F32)
    w2 = (w - w1).astype(BF16).astype(F32)
    w3 = w - w1 - w2
    wr = jnp.concatenate([w1, w2, w3, jnp.zeros((104, w.shape[1]), F32)], axis=0).astype(BF16)
    e0f = e0.astype(F32)

    def gates(ep):
        r = pl.ds(pl.multiple_of(ep * n, n), n)
        lg = lax.dot_general(uall[r, :], wr, (((1,), (1,)), ((), ())), preferred_element_type=F32)
        lg = lg + pltpu.roll(lg, 120, 1) + pltpu.roll(lg, 112, 1)
        lane = lax.broadcasted_iota(jnp.int32, (n, 128), 1).astype(F32)
        col = mcol[r, :]
        id0, id1 = col[:, 2:3], col[:, 3:4]
        l0 = jnp.sum(jnp.where(lane == id0, lg, 0.0), axis=1, keepdims=True)
        l1 = jnp.sum(jnp.where(lane == id1, lg, 0.0), axis=1, keepdims=True)
        top = jnp.maximum(l0, l1)
        x0 = jnp.exp(l0 - top)
        x1 = jnp.exp(l1 - top)
        den = x0 + x1
        lane8 = lax.broadcasted_iota(jnp.int32, (n, 8), 1)
        expert = (lane8 - 2).astype(F32) + e0f
        g = jnp.where(id0 == expert, x0 / den, 0.0) + jnp.where(id1 == expert, x1 / den, 0.0)
        mcol[r, :] = jnp.where(lane8 < 2, col, g)

    gates(me)
    fs = []

    def forward(c):
        xs[c].wait_recv()
        cp = rcopy(uall.at[rows(xp, c)], uall.at[rows(xp, c)], s_f.at[c], r_f.at[c], {"ep": part})
        cp.start()
        fs.append(cp)

    for c in range(NCH - 1):
        forward(c)
    for cp in ps:
        cp.wait()
    gates(part)
    forward(NCH - 1)
    gates(xp)
    for cp in fs:
        cp.wait()
    gates(diag)
    for cp in xs:
        cp.wait_send()
    for f in range(steps):
        for cp in weight_copies(layer, 0, f, f, hbm, (pg, pu, pd), psem):
            cp.wait()


def dispatch(layer, os_, x, ids, wr, wo, wg, wu, wd):
    n, qdim = os_.shape
    model = wo.shape[1]
    n_loc, ff = wg.shape[1], wg.shape[3]
    steps = ff // FT
    dma = pltpu.SemaphoreType.DMA
    out_shape = [jax.ShapeDtypeStruct((n, model), BF16), jax.ShapeDtypeStruct((4 * n, model), BF16),
                 jax.ShapeDtypeStruct((8, 4 * n), F32), jax.ShapeDtypeStruct((4 * n, 8), F32)]
    scratch = []
    sems = [dma((steps, 3))] + [dma((NCH,))] * 6
    if layer == 0:
        out_shape.append(jax.ShapeDtypeStruct((4, 8, n), jnp.int32))
        scratch.append(VMEM((8, n), jnp.int32))
        sems += [dma((3,)), dma((3,))]
    n_small = len(out_shape)
    out_shape += [VMEM((steps, model, FT), BF16), VMEM((steps, model, FT), BF16), VMEM((steps, FT, model), BF16)]
    return pl.pallas_call(
        functools.partial(dispatch_kernel, layer, steps, n_loc),
        out_shape=out_shape,
        in_specs=[vspec()] * 5 + [anyspec()] * 3,
        out_specs=[vspec()] * n_small + [vspec()] * 3,
        scratch_shapes=scratch + sems,
        compiler_params=pltpu.CompilerParams(collective_id=2 * layer, has_side_effects=True, vmem_limit_bytes=LIM_D),
        name=f"dispatch{layer}",
    )(os_, x, ids, wr, wo, wg, wu, wd)


def expert_kernel(layer, u_ref, rrow_ref, mcol_ref, pg, pu, pd, wg_hbm, wu_hbm, wd_hbm, y_ref, wg, wu, wd, xe, yacc, sems):
    n = u_ref.shape[0]
    steps = pg.shape[0]
    n_loc = wg_hbm.shape[1]
    hbm = (wg_hbm, wu_hbm, wd_hbm)
    own = (wg, wu, wd)

    for e in range(1, n_loc):
        def issue(f, _, e=e):
            for c in weight_copies(layer, e, f, (e - 1) * steps + f, hbm, own, sems):
                c.start()
            return 0
        lax.fori_loop(0, steps, issue, 0)

    for e in range(n_loc):
        rank_row = rrow_ref[e:e + 1, :]
        count = jnp.sum((rank_row >= 0).astype(F32)).astype(jnp.int32)
        lo = 0
        for m in SIZES:
            @pl.when((count <= m) & ((count > lo) | (lo == 0)))
            def _(m=m, e=e):
                sel = (rank_row == lax.broadcasted_iota(jnp.int32, (m, n), 0).astype(F32)).astype(F32).astype(BF16)
                xe[pl.ds(0, m), :] = dot(sel, u_ref[...]).astype(BF16)
                yacc[pl.ds(0, m), :] = jnp.zeros((m, yacc.shape[1]), F32)

                def step(f, _):
                    if e == 0:
                        w1, w3, w2 = pg, pu, pd
                        slot = f
                    else:
                        w1, w3, w2 = own
                        slot = (e - 1) * steps + f
                        for c in weight_copies(layer, e, f, slot, hbm, own, sems):
                            c.wait()
                    gate = dot(xe[pl.ds(0, m), :], w1[slot])
                    up = dot(xe[pl.ds(0, m), :], w3[slot])
                    inner = (gate * jax.nn.sigmoid(gate) * up).astype(BF16)
                    yacc[pl.ds(0, m), :] += dot(inner, w2[slot])
                    return 0

                lax.fori_loop(0, steps, step, 0)
                y_ref[pl.ds(e * n, m), :] = yacc[pl.ds(0, m), :].astype(BF16)
                if m < n:
                    y_ref[pl.ds(e * n + m, n - m), :] = jnp.zeros((n - m, y_ref.shape[1]), BF16)
            lo = m


def experts(layer, u_all, rrow, mcol, pre, wg, wu, wd):
    n, model = u_all.shape
    steps = pre[0].shape[0]
    n_loc = wg.shape[1]
    slots = steps * (n_loc - 1)
    return pl.pallas_call(
        functools.partial(expert_kernel, layer),
        out_shape=jax.ShapeDtypeStruct((n_loc * n, model), BF16),
        in_specs=[vspec()] * 6 + [anyspec()] * 3,
        out_specs=vspec(),
        scratch_shapes=[VMEM((slots, model, FT), BF16), VMEM((slots, model, FT), BF16), VMEM((slots, FT, model), BF16),
                        VMEM((n, model), BF16), VMEM((n, model), F32), pltpu.SemaphoreType.DMA((slots, 3))],
        compiler_params=pltpu.CompilerParams(vmem_limit_bytes=LIM_E),
        name=f"experts{layer}",
    )(u_all, rrow, mcol, *pre, wg, wu, wd)


def combine_kernel(last, layer, y_ref, mcol_ref, a_ref, *refs):
    if last:
        out_ref, p_d, p_x, p_p, p_me, own, mid, far, *sems = refs
        s_o, r_o, s_m, r_m, s_f, r_f, s_y, r_y = sems
    else:
        (cos_ref, sin_ref, wq_hbm, wk_hbm, wv_hbm, out_ref, qs, kn, vn,
         p_d, p_x, p_p, p_me, own, mid, far, wq, wk, wv, *sems) = refs
        s_o, r_o, s_m, r_m, s_f, r_f, wsem = sems
    n = a_ref.shape[0]
    ch = n // CCH
    nn = mcol_ref.shape[0]
    me, part, xp, diag = peers()
    devs = [{"ep": part}, {"ep": xp}]
    if last:
        pool = lax.axis_index("pool")
        devs.append({"pool": 1 - pool})
    else:
        w_copies = [pltpu.make_async_copy(src.at[layer + 1], dst, wsem.at[i])
                    for i, (src, dst) in enumerate(((wq_hbm, wq), (wk_hbm, wk), (wv_hbm, wv)))]
        for c in w_copies:
            c.start()

    def partial(ep):
        col = mcol_ref[pl.ds(pl.multiple_of(ep * n, n), n), :]
        slot = lax.broadcasted_iota(jnp.int32, (n, nn), 1).astype(F32)
        total = None
        for e in range(y_ref.shape[0] // nn):
            sel = (col[:, e:e + 1] == slot).astype(F32).astype(BF16)
            t = dot(sel, y_ref[e * nn:(e + 1) * nn, :]) * col[:, 2 + e:3 + e]
            total = t if total is None else total + t
        return total

    arrive = barrier(devs)
    p_d[...] = partial(diag)
    arrive()
    depth = 4 if last else CCH
    mids, fars, ys = [], [], []
    for c in range(CCH):
        r = pl.ds(c * ch, ch)
        cp = rcopy(p_d.at[r], mid.at[r], s_m.at[c], r_m.at[c], devs[0])
        cp.start()
        mids.append(cp)
    p_x[...] = partial(xp)

    def send(c):
        r = pl.ds(c * ch, ch)
        mids[c].wait_recv()
        p_x[r, :] = p_x[r, :] + mid[r, :]
        if c >= depth:
            fars[c - depth].wait_send()
        cp = rcopy(p_x.at[r], far.at[r], s_f.at[c], r_f.at[c], devs[1])
        cp.start()
        fars.append(cp)

    def receive(c):
        r = pl.ds(c * ch, ch)
        fars[c].wait_recv()
        res = (p_me[r, :] + far[r, :]).astype(BF16)
        if last:
            o = pl.ds(pl.multiple_of(pool * n + c * ch, ch), ch)
            out_ref[o, :] = res
            cp = rcopy(out_ref.at[o], out_ref.at[o], s_y.at[c], r_y.at[c], devs[2])
            cp.start()
            ys.append(cp)
        else:
            out_ref[r, :] = res
            if c % (CCH // 2) == CCH // 2 - 1:
                r2 = pl.ds(c * ch + ch - n // 2, n // 2)
                h = rms_bf16(out_ref[r2, :].astype(F32))
                project(h, cos_ref[r2, :], sin_ref[r2, :], wq, wk, wv, qs, kn, vn, r2)

    for c in range(depth):
        send(c)
    p_p[...] = partial(part)
    own_cp = rcopy(p_p, own, s_o, r_o, devs[0])
    own_cp.start()
    p_me[...] = partial(me)
    own_cp.wait()
    p_me[...] = a_ref[...].astype(F32) + (p_me[...] + own[...])
    if not last:
        for c in w_copies:
            c.wait()
    for c in range(depth, CCH):
        send(c)
        receive(c - depth)
    for c in range(CCH - depth, CCH):
        receive(c)
    for c in range(CCH):
        mids[c].wait_send()
    for c in range(CCH - depth, CCH):
        fars[c].wait_send()
    for cp in ys:
        cp.wait()


def combine(layer, last, y, mcol, a, nxt=None):
    n, model = a.shape
    dma = pltpu.SemaphoreType.DMA
    sems = [dma, dma, dma((CCH,)), dma((CCH,)), dma((CCH,)), dma((CCH,))]
    args = [y, mcol, a]
    specs = [vspec()] * 3
    scratch = [VMEM((n, model), F32) for _ in range(7)]
    if last:
        sems += [dma((CCH,)), dma((CCH,))]
        out_shape = jax.ShapeDtypeStruct((2 * n, model), BF16)
        out_specs = vspec()
    else:
        cos, sin, wq, wk, wv = nxt
        args += [cos, sin, wq, wk, wv]
        specs += [vspec()] * 2 + [anyspec()] * 3
        sems += [dma((3,))]
        scratch += [VMEM(w.shape[1:], BF16) for w in (wq, wk, wv)]
        out_shape = [jax.ShapeDtypeStruct((n, model), BF16)] + [jax.ShapeDtypeStruct((n, w.shape[2]), BF16) for w in (wq, wk, wv)]
        out_specs = [vspec()] * 4
    return pl.pallas_call(
        functools.partial(combine_kernel, last, layer),
        out_shape=out_shape,
        in_specs=specs,
        out_specs=out_specs,
        scratch_shapes=scratch + sems,
        compiler_params=pltpu.CompilerParams(collective_id=2 * layer + 1, has_side_effects=True, vmem_limit_bytes=LIM_C),
        name=f"combine{layer}",
    )(*args)


def solution(mesh):
    def body(hidden, k_cache, v_cache, lengths, expert_ids, w_query, w_key, w_value, w_out, w_router, w_gate, w_up, w_down):
        n_layers, _, seq, kvh, hd = k_cache.shape
        n_tok = hidden.shape[0] // 2
        kc = k_cache.reshape(n_layers, -1, seq * kvh, hd)
        vc = v_cache.reshape(n_layers, -1, seq * kvh, hd)
        ids = expert_ids.transpose(0, 2, 1)
        wr = w_router.transpose(0, 2, 1)
        tab = jnp.asarray(rope_table(seq, hd))
        w_query, w_key, w_value, w_out, w_gate, w_up, w_down, kc, vc, tab, hidden_h, lens_h = (
            pltpu.with_memory_space_constraint(v, pltpu.HBM) for v in (w_query, w_key, w_value, w_out, w_gate, w_up, w_down, kc, vc, tab, hidden, lengths))
        state = hidden
        qkv = None
        for layer in range(n_layers):
            last = layer == n_layers - 1
            if layer == 0:
                att, wo, cos, sin = attention(layer, n_tok, lens_h, w_out, kc, vc, proj=(hidden_h, tab, w_query, w_key, w_value))
            else:
                att, wo = attention(layer, n_tok, lens_h, w_out, kc, vc, qkv=qkv)
            outs = dispatch(layer, att, state, ids, wr, wo, w_gate, w_up, w_down)
            a, u_all, rrow, mcol = outs[:4]
            if layer == 0:
                ids = outs[4]
            y = experts(layer, u_all, rrow, mcol, outs[-3:], w_gate, w_up, w_down)
            if last:
                return combine(layer, True, y, mcol, a)
            state, *qkv = combine(layer, False, y, mcol, a, nxt=(cos, sin, w_query, w_key, w_value))

    rows_spec = ("dp", "ep")
    in_specs = (P(rows_spec, None), P(None, rows_spec), P(None, rows_spec), P(rows_spec), P(None, rows_spec, None), P(), P(), P(), P(), P(), P(None, "ep"), P(None, "ep"), P(None, "ep"))
    return jax.shard_map(body, mesh=mesh, in_specs=in_specs, out_specs=P(rows_spec, None), check_vma=False)
```

```python
import functools

import numpy as np

import jax
import jax.numpy as jnp
from jax import lax
from jax.experimental import pallas as pl
from jax.experimental.pallas import tpu as pltpu
from jax.sharding import PartitionSpec as P

MESH = pl.DeviceIdType.MESH
EPSILON = 1e-6
ROPE_BASE = 10000.0
VMEM = pltpu.VMEM
F32 = jnp.float32
BF16 = jnp.bfloat16

TOKG = 16
TILE = 1024
FT = 512
NSLOT = 3
CCH = 8
LIM_A = 50 * 1024 * 1024
LIM_B = 50 * 1024 * 1024
LIM_D = 8 * 1024 * 1024
LIM_E = 27 * 1024 * 1024
LIM_C = 16 * 1024 * 1024
SIZES = (128, 400, 512)


def vspec():
    return pl.BlockSpec(memory_space=VMEM)


def anyspec():
    return pl.BlockSpec(memory_space=pltpu.HBM)


def sspec():
    return pl.BlockSpec(memory_space=pltpu.SMEM)


def dot(a, b):
    return jnp.dot(a, b, preferred_element_type=F32)


def rms_bf16(v):
    return (v * lax.rsqrt(jnp.mean(v * v, axis=-1, keepdims=True) + EPSILON)).astype(BF16)


def rope_table(seq, hd):
    half = hd // 2
    freqs = np.power(np.float32(ROPE_BASE), (np.float32(-2.0) * np.arange(half, dtype=np.float32) / np.float32(hd)))
    angle = np.arange(seq + 1, dtype=np.float32)[:, None] * freqs.astype(np.float32)[None, :]
    wide = angle.astype(np.float64)
    return np.concatenate([np.cos(wide), np.sin(wide)], axis=1).astype(np.float32)


def rope(vec, cos, sin):
    return vec * cos + pltpu.roll(vec, 64, 1) * sin


def project(h, cos, sin, wq, wk, wv, qs, kn, vn, rows):
    q = dot(h, wq[...])
    k = dot(h, wk[...])
    v = dot(h, wv[...])
    for j in range(q.shape[1] // 128):
        qs[rows, j * 128:(j + 1) * 128] = rope(q[:, j * 128:(j + 1) * 128], cos, sin).astype(BF16)
    for j in range(k.shape[1] // 128):
        kn[rows, j * 128:(j + 1) * 128] = rope(k[:, j * 128:(j + 1) * 128], cos, sin).astype(BF16)
    vn[rows, :] = v.astype(BF16)


def attn_kernel(layer, n_tok, first_layer, lens_in, *refs):
    if first_layer:
        (x_hbm, tab_hbm, wq_hbm, wk_hbm, wv_hbm, wo_hbm, kc, vc, os_, wo, cos_ref, sin_ref,
         x_ref, tab_ref, wq, wk, wv, qs, kn, vn, wsem, kbuf, vbuf, sbuf, mst, men, pk, wn, lens_ref, lsem, ksem, vsem, osem) = refs
    else:
        qs, kn, vn, wo_hbm, kc, vc, os_, wo, kbuf, vbuf, sbuf, mst, men, pk, wn, ksem, vsem, osem = refs
        lens_ref = lens_in
    t0 = lax.axis_index("pool") * n_tok
    if first_layer:
        lens_cp = pltpu.make_async_copy(lens_in, lens_ref, lsem)
        lens_cp.start()
    heads = qs.shape[1] // 128
    n_groups = n_tok // TOKG
    hpk = heads // 2
    cols = heads * TOKG

    def padded(ln):
        return pl.multiple_of(lax.shift_left(lax.shift_right_logical(ln + 7, 3), 4), 16)

    def start_keys(g):
        slot = lax.rem(g, NSLOT)
        off = 0
        for i in range(TOKG):
            tok = t0 + g * TOKG + i
            ln = lens_ref[tok]
            n = padded(ln)
            off = pl.multiple_of(off, 16)
            pltpu.make_async_copy(kc.at[layer, tok, pl.ds(0, n), :], kbuf.at[slot, pl.ds(off, n), :], ksem.at[slot]).start()
            mst[slot, i:i + 1, :] = jnp.full((1, 128), off, jnp.int32)
            men[slot, i:i + 1, :] = jnp.full((1, 128), off + 2 * ln, jnp.int32)
            off = off + n
        return jnp.asarray(off, jnp.int32)

    def start_vals(g):
        slot = lax.rem(g, NSLOT)
        off = 0
        for i in range(TOKG):
            tok = t0 + g * TOKG + i
            n = padded(lens_ref[tok])
            off = pl.multiple_of(off, 16)
            pltpu.make_async_copy(vc.at[layer, tok, pl.ds(0, n), :], vbuf.at[slot, pl.ds(off, n), :], vsem.at[slot]).start()
            off = off + n

    if first_layer:
        w_copies = [pltpu.make_async_copy(src.at[layer], dst, wsem.at[i])
                    for i, (src, dst) in enumerate(((wq_hbm, wq), (wk_hbm, wk), (wv_hbm, wv)))]
        x_cp = pltpu.make_async_copy(x_hbm.at[pl.ds(pl.multiple_of(t0, n_tok), n_tok), :], x_ref, wsem.at[3])
        tab_cp = pltpu.make_async_copy(tab_hbm, tab_ref, wsem.at[4])
        x_cp.start()
        tab_cp.start()
        for c in w_copies:
            c.start()
    if first_layer:
        lens_cp.wait()
    total0 = start_keys(jnp.int32(0))
    start_vals(jnp.int32(0))
    total1 = start_keys(jnp.int32(1))
    wo_cp = pltpu.make_async_copy(wo_hbm.at[layer], wo, osem)
    wo_cp.start()
    if first_layer:
        x_cp.wait()
        tab_cp.wait()
        h = rms_bf16(x_ref[...].astype(F32))

        def pick(i, _):
            cos_ref[pl.ds(i, 1), :] = tab_ref[pl.ds(lens_ref[t0 + i], 1), :]
            return 0
        lax.fori_loop(0, n_tok, pick, 0)
        both = cos_ref[...]
        swapped = pltpu.roll(both, 64, 1)
        low = lax.broadcasted_iota(jnp.int32, both.shape, 1) < 64
        cos = jnp.where(low, both, swapped)
        sin = jnp.where(low, -swapped, both)
        cos_ref[...] = cos
        sin_ref[...] = sin
        for c in w_copies:
            c.wait()
        project(h, cos, sin, wq, wk, wv, qs, kn, vn, pl.ds(0, n_tok))
    scale = 128.0 ** -0.5 * 1.4426950408889634

    lane = lax.broadcasted_iota(jnp.int32, (cols, 128), 1)
    kv = (lax.broadcasted_iota(jnp.int32, (cols, 128), 0) >= (hpk * TOKG)).astype(jnp.int32)
    mine = (lane & 1) == kv

    def heads_of(ref, g):
        row = ref[pl.ds(pl.multiple_of(g * TOKG, TOKG), TOKG), :]
        per = heads // (ref.shape[1] // 128)
        return jnp.concatenate([row[:, (j // per) * 128:(j // per + 1) * 128] for j in range(heads)], axis=0)

    def tiles_of(total, on):
        n = lax.shift_right_logical(total + TILE // 2 - 1, TILE.bit_length() - 1)
        return jnp.where(on, n, 0), jnp.where(on & (total > n * TILE), 1, 0)

    def step(g, totals):
        prev_total, total, next_total = totals
        prev_total = pl.multiple_of(prev_total, 16)
        total = pl.multiple_of(total, 16)
        slot = lax.rem(g, NSLOT)
        prev = lax.rem(g + NSLOT - 1, NSLOT)
        sl, sp = g & 1, 1 - (g & 1)
        last = lax.cond(g + 2 < n_groups, lambda: start_keys(g + 2), lambda: jnp.int32(0))

        @pl.when(g + 1 < n_groups)
        def _():
            start_vals(g + 1)

        gc = jnp.minimum(g, n_groups - 1)
        q2 = heads_of(qs, gc)
        s_new = jnp.sum(q2.astype(F32) * heads_of(kn, gc).astype(F32), axis=1, keepdims=True)
        start = jnp.where(mine, jnp.concatenate([mst[slot]] * heads, axis=0) - lane, 1 << 30)
        end = jnp.concatenate([men[slot]] * heads, axis=0) - lane
        n1, t1 = tiles_of(total, g < n_groups)
        n2, t2 = tiles_of(prev_total, g > 0)
        both = jnp.minimum(n1, n2)

        @pl.when(g < n_groups)
        def _():
            pltpu.make_async_copy(kbuf.at[slot, pl.ds(0, total), :], kbuf.at[slot, pl.ds(0, total), :], ksem.at[slot]).wait()

        @pl.when(g > 0)
        def _():
            vbuf[prev, pl.ds(prev_total, TILE), :] = jnp.zeros((TILE, 128), BF16)
            pltpu.make_async_copy(vbuf.at[prev, pl.ds(0, prev_total), :], vbuf.at[prev, pl.ds(0, prev_total), :], vsem.at[prev]).wait()

        def first(i, macc, rows=TILE):
            base = pl.multiple_of(i * TILE, TILE)
            for j in range(rows // 256):
                at = pl.multiple_of(base + j * 256, 256)
                s = lax.dot_general(q2, kbuf[slot, pl.ds(at, 256), :], (((1,), (1,)), ((), ())), preferred_element_type=F32)
                for p in range(2):
                    off = at + p * 128
                    part = jnp.where((start <= off) & (end > off), s[:, p * 128:(p + 1) * 128], -jnp.inf)
                    sbuf[sl, :, pl.ds(pl.multiple_of(off, 128), 128)] = part
                    macc = jnp.maximum(macc, part)
            return macc

        def second(i, carry, rows=TILE):
            lacc, acc = carry
            base = pl.multiple_of(i * TILE, TILE)
            top = pk[...]
            parts = []
            for j in range(rows // 128):
                p = jnp.exp2((sbuf[sp, :, pl.ds(pl.multiple_of(base + j * 128, 128), 128)] - top) * scale)
                lacc = lacc + p
                parts.append(p.astype(BF16))
            acc = acc + dot(jnp.concatenate(parts, axis=1), vbuf[prev, pl.ds(base, rows), :])
            return lacc, acc

        def joint(i, carry):
            macc, lacc, acc = carry
            return (first(i, macc),) + second(i, (lacc, acc))

        zero = jnp.zeros((cols, 128), F32)
        macc, lacc, acc = lax.fori_loop(0, both, joint, (jnp.full((cols, 128), -jnp.inf, F32), zero, zero))
        lacc, acc = lax.fori_loop(both, n2, second, (lacc, acc))
        macc = lax.fori_loop(both, n1, first, macc)
        lacc, acc = lax.fori_loop(n2, n2 + t2, functools.partial(second, rows=TILE // 2), (lacc, acc))
        macc = lax.fori_loop(n1, n1 + t1, functools.partial(first, rows=TILE // 2), macc)

        w_new = wn[...]
        gp = jnp.maximum(g - 1, 0)
        den = jnp.sum(lacc, axis=1, keepdims=True) + w_new
        o = ((acc + w_new.astype(BF16).astype(F32) * heads_of(vn, gp).astype(F32)) / den).astype(BF16)
        g0 = pl.multiple_of(gp * TOKG, TOKG)
        for j in range(heads):
            os_[pl.ds(g0, TOKG), j * 128:(j + 1) * 128] = o[j * TOKG:(j + 1) * TOKG, :]

        peak = jnp.maximum(jnp.max(macc, axis=1, keepdims=True), s_new)
        pk[...] = jnp.broadcast_to(peak, (cols, 128))
        wn[...] = jnp.broadcast_to(jnp.exp2((s_new - peak) * scale), (cols, 128))
        return total, next_total, last

    wn[...] = jnp.ones((cols, 128), F32)
    lax.fori_loop(0, n_groups + 1, step, (jnp.int32(0), total0, total1))
    wo_cp.wait()


def attention(layer, n_tok, lens, w_out, kc, vc, proj=None, qkv=None):
    dma = pltpu.SemaphoreType.DMA
    first_layer = proj is not None
    out_shape = []
    if first_layer:
        x, tab, wq, wk, wv = proj
        model, qdim, kvdim = wq.shape[1], wq.shape[2], wk.shape[2]
        args = [lens, x, tab, wq, wk, wv, w_out, kc, vc]
        specs = [anyspec()] * 9
        out_shape = [VMEM((n_tok, qdim), BF16), VMEM(w_out.shape[1:], BF16)] + [jax.ShapeDtypeStruct((n_tok, 128), F32)] * 2
        scratch = [VMEM((n_tok, model), BF16), VMEM(tab.shape, F32), VMEM((model, qdim), BF16), VMEM((model, kvdim), BF16), VMEM((model, kvdim), BF16),
                   VMEM((n_tok, qdim), BF16), VMEM((n_tok, kvdim), BF16), VMEM((n_tok, kvdim), BF16), dma((5,))]
    else:
        qdim = qkv[0].shape[1]
        args = [lens, *qkv, w_out, kc, vc]
        specs = [sspec()] + [vspec()] * 3 + [anyspec()] * 3
        out_shape = [VMEM((n_tok, qdim), BF16), VMEM(w_out.shape[1:], BF16)]
        scratch = []
    max_rows = TOKG * kc.shape[2]
    cols = (qdim // 128) * TOKG
    scratch += [VMEM((NSLOT, max_rows + TILE, 128), BF16), VMEM((NSLOT, max_rows + TILE, 128), BF16), VMEM((2, cols, max_rows), F32),
                VMEM((NSLOT, TOKG, 128), jnp.int32), VMEM((NSLOT, TOKG, 128), jnp.int32), VMEM((cols, 128), F32), VMEM((cols, 128), F32), *([pltpu.SMEM(lens.shape, jnp.int32), dma] if first_layer else []), dma((NSLOT,)), dma((NSLOT,)), dma]
    return pl.pallas_call(
        functools.partial(attn_kernel, layer, n_tok, first_layer),
        out_shape=out_shape,
        in_specs=specs,
        out_specs=[vspec()] * len(out_shape),
        scratch_shapes=scratch,
        compiler_params=pltpu.CompilerParams(vmem_limit_bytes=LIM_A if first_layer else LIM_B),
        name=f"attention{layer}",
    )(*args)


NCH = 4


def peers():
    me = lax.axis_index("ep")
    core = me % 2
    x = me // 2
    return me, x * 2 + (1 - core), (1 - x) * 2 + core, (1 - x) * 2 + (1 - core)


def barrier(devices):
    sem = pltpu.get_barrier_semaphore()
    for d in devices:
        pl.semaphore_signal(sem, inc=1, device_id=d, device_id_type=MESH)
    return lambda: pl.semaphore_wait(sem, len(devices))


def rcopy(src, dst, ssem, rsem, dev):
    return pltpu.make_async_remote_copy(src_ref=src, dst_ref=dst, send_sem=ssem, recv_sem=rsem, device_id=dev, device_id_type=MESH)


def weight_copies(layer, e, f, slot, hbm, buf, sems):
    wg_hbm, wu_hbm, wd_hbm = hbm
    cols = pl.ds(f * FT, FT) if isinstance(f, int) else pl.ds(pl.multiple_of(f * FT, FT), FT)
    return (pltpu.make_async_copy(wg_hbm.at[layer, e, :, cols], buf[0].at[slot], sems.at[slot, 0]),
            pltpu.make_async_copy(wu_hbm.at[layer, e, :, cols], buf[1].at[slot], sems.at[slot, 1]),
            pltpu.make_async_copy(wd_hbm.at[layer, e, cols, :], buf[2].at[slot], sems.at[slot, 2]))


def dispatch_kernel(layer, steps, n_loc, os_ref, x_ref, ids_ref, wr_ref, wo, wg_hbm, wu_hbm, wd_hbm, *refs):
    first_layer = layer == 0
    if first_layer:
        a_ref, uall, rrow, mcol, idsall, pg, pu, pd, idsbuf, *sems = refs
        psem, s_p, r_p, s_x, r_x, s_f, r_f, s_i, r_i = sems
    else:
        a_ref, uall, rrow, mcol, pg, pu, pd, *sems = refs
        psem, s_p, r_p, s_x, r_x, s_f, r_f = sems
        idsall = ids_ref
    n = os_ref.shape[0]
    ch = n // NCH
    pool = lax.axis_index("pool")
    me, part, xp, diag = peers()
    devs = [{"ep": part}, {"ep": xp}]
    arrive = barrier(devs)

    def rows(ep, c):
        return pl.ds(pl.multiple_of(ep * n + c * ch, ch), ch)

    ics = []
    if first_layer:
        t0 = pl.multiple_of(pool * n, n)
        idsbuf[...] = jnp.zeros(idsbuf.shape, jnp.int32)
        for l in range(ids_ref.shape[0]):
            idsbuf[2 * l:2 * l + 2, :] = ids_ref[l, :, pl.ds(t0, n)]
        idsall[me] = idsbuf[...]
    xs, ps = [], []
    half = n // 2
    for hf in range(2):
        r = pl.ds(hf * half, half)
        if first_layer:
            xr = x_ref[pl.ds(pl.multiple_of(pool * n + hf * half, half), half), :]
        else:
            xr = x_ref[r, :]
        a = (xr.astype(F32) + dot(os_ref[r, :], wo[...])).astype(BF16)
        a_ref[r, :] = a
        uall[pl.ds(pl.multiple_of(me * n + hf * half, half), half), :] = rms_bf16(a.astype(F32))
        if hf == 0:
            arrive()
        for c in range(hf * NCH // 2, (hf + 1) * NCH // 2):
            cp = rcopy(uall.at[rows(me, c)], uall.at[rows(me, c)], s_x.at[c], r_x.at[c], {"ep": xp})
            cp.start()
            xs.append(cp)
            cp = rcopy(uall.at[rows(me, c)], uall.at[rows(me, c)], s_p.at[c], r_p.at[c], {"ep": part})
            cp.start()
            ps.append(cp)
    if first_layer:
        for i, d in enumerate(devs):
            cp = rcopy(idsbuf, idsall.at[me], s_i.at[i], r_i.at[i], d)
            cp.start()
            ics.append(cp)
    hbm = (wg_hbm, wu_hbm, wd_hbm)

    def prefetch(f, _):
        for cp in weight_copies(layer, 0, f, f, hbm, (pg, pu, pd), psem):
            cp.start()
        return 0

    lax.fori_loop(0, steps, prefetch, 0)
    if first_layer:
        ics[1].wait_recv()
        cp = rcopy(idsall.at[xp], idsall.at[xp], s_i.at[2], r_i.at[2], devs[0])
        cp.start()
        cp.wait()
        ics[0].wait()
        ics[1].wait_send()

    tokens = 4 * n
    e0 = me * n_loc
    ids_row = [jnp.concatenate([idsall[b, 2 * layer + k:2 * layer + k + 1, :] for b in range(4)], axis=1) for k in range(2)]
    row8 = lax.broadcasted_iota(jnp.int32, (8, tokens), 0)
    hit = ((ids_row[0] == row8 + e0) | (ids_row[1] == row8 + e0)) & (row8 < n_loc)
    hit_f = hit.astype(F32)
    tri = (lax.broadcasted_iota(jnp.int32, (tokens, tokens), 0) < lax.broadcasted_iota(jnp.int32, (tokens, tokens), 1)).astype(F32).astype(BF16)
    rank = jnp.where(hit_f > 0, dot(hit_f.astype(BF16), tri), -1.0)
    rrow[...] = rank
    idf = jnp.where(row8 == 2, jnp.broadcast_to(ids_row[0].astype(F32), (8, tokens)),
                    jnp.where(row8 == 3, jnp.broadcast_to(ids_row[1].astype(F32), (8, tokens)), rank))
    mcol[...] = jnp.transpose(idf)

    w = wr_ref[layer]
    w1 = w.astype(BF16).astype(F32)
    w2 = (w - w1).astype(BF16).astype(F32)
    w3 = w - w1 - w2
    wr = jnp.concatenate([w1, w2, w3, jnp.zeros((104, w.shape[1]), F32)], axis=0).astype(BF16)
    e0f = e0.astype(F32)

    def gates(ep):
        r = pl.ds(pl.multiple_of(ep * n, n), n)
        lg = lax.dot_general(uall[r, :], wr, (((1,), (1,)), ((), ())), preferred_element_type=F32)
        lg = lg + pltpu.roll(lg, 120, 1) + pltpu.roll(lg, 112, 1)
        lane = lax.broadcasted_iota(jnp.int32, (n, 128), 1).astype(F32)
        col = mcol[r, :]
        id0, id1 = col[:, 2:3], col[:, 3:4]
        l0 = jnp.sum(jnp.where(lane == id0, lg, 0.0), axis=1, keepdims=True)
        l1 = jnp.sum(jnp.where(lane == id1, lg, 0.0), axis=1, keepdims=True)
        top = jnp.maximum(l0, l1)
        x0 = jnp.exp(l0 - top)
        x1 = jnp.exp(l1 - top)
        den = x0 + x1
        lane8 = lax.broadcasted_iota(jnp.int32, (n, 8), 1)
        expert = (lane8 - 2).astype(F32) + e0f
        g = jnp.where(id0 == expert, x0 / den, 0.0) + jnp.where(id1 == expert, x1 / den, 0.0)
        mcol[r, :] = jnp.where(lane8 < 2, col, g)

    gates(me)
    fs = []

    def forward(c):
        xs[c].wait_recv()
        cp = rcopy(uall.at[rows(xp, c)], uall.at[rows(xp, c)], s_f.at[c], r_f.at[c], {"ep": part})
        cp.start()
        fs.append(cp)

    for c in range(NCH - 1):
        forward(c)
    for cp in ps:
        cp.wait()
    gates(part)
    forward(NCH - 1)
    gates(xp)
    for cp in fs:
        cp.wait()
    gates(diag)
    for cp in xs:
        cp.wait_send()
    for f in range(steps):
        for cp in weight_copies(layer, 0, f, f, hbm, (pg, pu, pd), psem):
            cp.wait()


def dispatch(layer, os_, x, ids, wr, wo, wg, wu, wd):
    n, qdim = os_.shape
    model = wo.shape[1]
    n_loc, ff = wg.shape[1], wg.shape[3]
    steps = ff // FT
    dma = pltpu.SemaphoreType.DMA
    out_shape = [jax.ShapeDtypeStruct((n, model), BF16), jax.ShapeDtypeStruct((4 * n, model), BF16),
                 jax.ShapeDtypeStruct((8, 4 * n), F32), jax.ShapeDtypeStruct((4 * n, 8), F32)]
    scratch = []
    sems = [dma((steps, 3))] + [dma((NCH,))] * 6
    if layer == 0:
        out_shape.append(jax.ShapeDtypeStruct((4, 8, n), jnp.int32))
        scratch.append(VMEM((8, n), jnp.int32))
        sems += [dma((3,)), dma((3,))]
    n_small = len(out_shape)
    out_shape += [VMEM((steps, model, FT), BF16), VMEM((steps, model, FT), BF16), VMEM((steps, FT, model), BF16)]
    return pl.pallas_call(
        functools.partial(dispatch_kernel, layer, steps, n_loc),
        out_shape=out_shape,
        in_specs=[vspec()] * 5 + [anyspec()] * 3,
        out_specs=[vspec()] * n_small + [vspec()] * 3,
        scratch_shapes=scratch + sems,
        compiler_params=pltpu.CompilerParams(collective_id=2 * layer, has_side_effects=True, vmem_limit_bytes=LIM_D),
        name=f"dispatch{layer}",
    )(os_, x, ids, wr, wo, wg, wu, wd)


def expert_kernel(layer, u_ref, rrow_ref, mcol_ref, pg, pu, pd, wg_hbm, wu_hbm, wd_hbm, y_ref, wg, wu, wd, xe, yacc, sems):
    n = u_ref.shape[0]
    steps = pg.shape[0]
    n_loc = wg_hbm.shape[1]
    hbm = (wg_hbm, wu_hbm, wd_hbm)
    own = (wg, wu, wd)

    for e in range(1, n_loc):
        def issue(f, _, e=e):
            for c in weight_copies(layer, e, f, (e - 1) * steps + f, hbm, own, sems):
                c.start()
            return 0
        lax.fori_loop(0, steps, issue, 0)

    for e in range(n_loc):
        rank_row = rrow_ref[e:e + 1, :]
        count = jnp.sum((rank_row >= 0).astype(F32)).astype(jnp.int32)
        lo = 0
        for m in SIZES:
            @pl.when((count <= m) & ((count > lo) | (lo == 0)))
            def _(m=m, e=e):
                sel = (rank_row == lax.broadcasted_iota(jnp.int32, (m, n), 0).astype(F32)).astype(F32).astype(BF16)
                xe[pl.ds(0, m), :] = dot(sel, u_ref[...]).astype(BF16)
                yacc[pl.ds(0, m), :] = jnp.zeros((m, yacc.shape[1]), F32)

                def step(f, _):
                    if e == 0:
                        w1, w3, w2 = pg, pu, pd
                        slot = f
                    else:
                        w1, w3, w2 = own
                        slot = (e - 1) * steps + f
                        for c in weight_copies(layer, e, f, slot, hbm, own, sems):
                            c.wait()
                    gate = dot(xe[pl.ds(0, m), :], w1[slot])
                    up = dot(xe[pl.ds(0, m), :], w3[slot])
                    inner = (gate * jax.nn.sigmoid(gate) * up).astype(BF16)
                    yacc[pl.ds(0, m), :] += dot(inner, w2[slot])
                    return 0

                lax.fori_loop(0, steps, step, 0)
                y_ref[pl.ds(e * n, m), :] = yacc[pl.ds(0, m), :].astype(BF16)
                if m < n:
                    y_ref[pl.ds(e * n + m, n - m), :] = jnp.zeros((n - m, y_ref.shape[1]), BF16)
            lo = m


def experts(layer, u_all, rrow, mcol, pre, wg, wu, wd):
    n, model = u_all.shape
    steps = pre[0].shape[0]
    n_loc = wg.shape[1]
    slots = steps * (n_loc - 1)
    return pl.pallas_call(
        functools.partial(expert_kernel, layer),
        out_shape=jax.ShapeDtypeStruct((n_loc * n, model), BF16),
        in_specs=[vspec()] * 6 + [anyspec()] * 3,
        out_specs=vspec(),
        scratch_shapes=[VMEM((slots, model, FT), BF16), VMEM((slots, model, FT), BF16), VMEM((slots, FT, model), BF16),
                        VMEM((n, model), BF16), VMEM((n, model), F32), pltpu.SemaphoreType.DMA((slots, 3))],
        compiler_params=pltpu.CompilerParams(vmem_limit_bytes=LIM_E),
        name=f"experts{layer}",
    )(u_all, rrow, mcol, *pre, wg, wu, wd)


def combine_kernel(last, layer, y_ref, mcol_ref, a_ref, *refs):
    if last:
        out_ref, p_d, p_x, p_p, p_me, own, mid, far, *sems = refs
        s_o, r_o, s_m, r_m, s_f, r_f, s_y, r_y = sems
    else:
        (cos_ref, sin_ref, wq_hbm, wk_hbm, wv_hbm, out_ref, qs, kn, vn,
         p_d, p_x, p_p, p_me, own, mid, far, wq, wk, wv, *sems) = refs
        s_o, r_o, s_m, r_m, s_f, r_f, wsem = sems
    n = a_ref.shape[0]
    ch = n // CCH
    nn = mcol_ref.shape[0]
    me, part, xp, diag = peers()
    devs = [{"ep": part}, {"ep": xp}]
    if last:
        pool = lax.axis_index("pool")
        devs.append({"pool": 1 - pool})
    else:
        w_copies = [pltpu.make_async_copy(src.at[layer + 1], dst, wsem.at[i])
                    for i, (src, dst) in enumerate(((wq_hbm, wq), (wk_hbm, wk), (wv_hbm, wv)))]
        for c in w_copies:
            c.start()

    def partial(ep):
        col = mcol_ref[pl.ds(pl.multiple_of(ep * n, n), n), :]
        slot = lax.broadcasted_iota(jnp.int32, (n, nn), 1).astype(F32)
        total = None
        for e in range(y_ref.shape[0] // nn):
            sel = (col[:, e:e + 1] == slot).astype(F32).astype(BF16)
            t = dot(sel, y_ref[e * nn:(e + 1) * nn, :]) * col[:, 2 + e:3 + e]
            total = t if total is None else total + t
        return total

    arrive = barrier(devs)
    p_d[...] = partial(diag)
    arrive()
    depth = 4 if last else CCH
    mids, fars, ys = [], [], []
    for c in range(CCH):
        r = pl.ds(c * ch, ch)
        cp = rcopy(p_d.at[r], mid.at[r], s_m.at[c], r_m.at[c], devs[0])
        cp.start()
        mids.append(cp)
    p_x[...] = partial(xp)

    def send(c):
        r = pl.ds(c * ch, ch)
        mids[c].wait_recv()
        p_x[r, :] = p_x[r, :] + mid[r, :]
        if c >= depth:
            fars[c - depth].wait_send()
        cp = rcopy(p_x.at[r], far.at[r], s_f.at[c], r_f.at[c], devs[1])
        cp.start()
        fars.append(cp)

    def receive(c):
        r = pl.ds(c * ch, ch)
        fars[c].wait_recv()
        res = (p_me[r, :] + far[r, :]).astype(BF16)
        if last:
            o = pl.ds(pl.multiple_of(pool * n + c * ch, ch), ch)
            out_ref[o, :] = res
            cp = rcopy(out_ref.at[o], out_ref.at[o], s_y.at[c], r_y.at[c], devs[2])
            cp.start()
            ys.append(cp)
        else:
            out_ref[r, :] = res
            if c % (CCH // 2) == CCH // 2 - 1:
                r2 = pl.ds(c * ch + ch - n // 2, n // 2)
                h = rms_bf16(out_ref[r2, :].astype(F32))
                project(h, cos_ref[r2, :], sin_ref[r2, :], wq, wk, wv, qs, kn, vn, r2)

    for c in range(depth):
        send(c)
    p_p[...] = partial(part)
    own_cp = rcopy(p_p, own, s_o, r_o, devs[0])
    own_cp.start()
    p_me[...] = partial(me)
    own_cp.wait()
    p_me[...] = a_ref[...].astype(F32) + (p_me[...] + own[...])
    if not last:
        for c in w_copies:
            c.wait()
    for c in range(depth, CCH):
        send(c)
        receive(c - depth)
    for c in range(CCH - depth, CCH):
        receive(c)
    for c in range(CCH):
        mids[c].wait_send()
    for c in range(CCH - depth, CCH):
        fars[c].wait_send()
    for cp in ys:
        cp.wait()


def combine(layer, last, y, mcol, a, nxt=None):
    n, model = a.shape
    dma = pltpu.SemaphoreType.DMA
    sems = [dma, dma, dma((CCH,)), dma((CCH,)), dma((CCH,)), dma((CCH,))]
    args = [y, mcol, a]
    specs = [vspec()] * 3
    scratch = [VMEM((n, model), F32) for _ in range(7)]
    if last:
        sems += [dma((CCH,)), dma((CCH,))]
        out_shape = jax.ShapeDtypeStruct((2 * n, model), BF16)
        out_specs = vspec()
    else:
        cos, sin, wq, wk, wv = nxt
        args += [cos, sin, wq, wk, wv]
        specs += [vspec()] * 2 + [anyspec()] * 3
        sems += [dma((3,))]
        scratch += [VMEM(w.shape[1:], BF16) for w in (wq, wk, wv)]
        out_shape = [jax.ShapeDtypeStruct((n, model), BF16)] + [jax.ShapeDtypeStruct((n, w.shape[2]), BF16) for w in (wq, wk, wv)]
        out_specs = [vspec()] * 4
    return pl.pallas_call(
        functools.partial(combine_kernel, last, layer),
        out_shape=out_shape,
        in_specs=specs,
        out_specs=out_specs,
        scratch_shapes=scratch + sems,
        compiler_params=pltpu.CompilerParams(collective_id=2 * layer + 1, has_side_effects=True, vmem_limit_bytes=LIM_C),
        name=f"combine{layer}",
    )(*args)


def solution(mesh):
    def body(hidden, k_cache, v_cache, lengths, expert_ids, w_query, w_key, w_value, w_out, w_router, w_gate, w_up, w_down):
        n_layers, _, seq, kvh, hd = k_cache.shape
        n_tok = hidden.shape[0] // 2
        kc = k_cache.reshape(n_layers, -1, seq * kvh, hd)
        vc = v_cache.reshape(n_layers, -1, seq * kvh, hd)
        ids = expert_ids.transpose(0, 2, 1)
        wr = w_router.transpose(0, 2, 1)
        tab = jnp.asarray(rope_table(seq, hd))
        w_query, w_key, w_value, w_out, w_gate, w_up, w_down, kc, vc, tab, hidden_h, lens_h = (
            pltpu.with_memory_space_constraint(v, pltpu.HBM) for v in (w_query, w_key, w_value, w_out, w_gate, w_up, w_down, kc, vc, tab, hidden, lengths))
        state = hidden
        qkv = None
        for layer in range(n_layers):
            last = layer == n_layers - 1
            if layer == 0:
                att, wo, cos, sin = attention(layer, n_tok, lens_h, w_out, kc, vc, proj=(hidden_h, tab, w_query, w_key, w_value))
            else:
                att, wo = attention(layer, n_tok, lengths, w_out, kc, vc, qkv=qkv)
            outs = dispatch(layer, att, state, ids, wr, wo, w_gate, w_up, w_down)
            a, u_all, rrow, mcol = outs[:4]
            if layer == 0:
                ids = outs[4]
            y = experts(layer, u_all, rrow, mcol, outs[-3:], w_gate, w_up, w_down)
            if last:
                return combine(layer, True, y, mcol, a)
            state, *qkv = combine(layer, False, y, mcol, a, nxt=(cos, sin, w_query, w_key, w_value))

    rows_spec = ("dp", "ep")
    in_specs = (P(rows_spec, None), P(None, rows_spec), P(None, rows_spec), P(rows_spec), P(None, rows_spec, None), P(), P(), P(), P(), P(), P(None, "ep"), P(None, "ep"), P(None, "ep"))
    return jax.shard_map(body, mesh=mesh, in_specs=in_specs, out_specs=P(rows_spec, None), check_vma=False)
```

```python
import functools

import numpy as np

import jax
import jax.numpy as jnp
from jax import lax
from jax.experimental import pallas as pl
from jax.experimental.pallas import tpu as pltpu
from jax.sharding import PartitionSpec as P

MESH = pl.DeviceIdType.MESH
EPSILON = 1e-6
ROPE_BASE = 10000.0
VMEM = pltpu.VMEM
F32 = jnp.float32
BF16 = jnp.bfloat16

TOKG = 16
TILE = 1024
FT = 512
NSLOT = 3
CCH = 8
LIM_A = 50 * 1024 * 1024
LIM_B = 50 * 1024 * 1024
LIM_D = 8 * 1024 * 1024
LIM_E = 27 * 1024 * 1024
LIM_C = 16 * 1024 * 1024
SIZES = (128, 400, 512)


def vspec():
    return pl.BlockSpec(memory_space=VMEM)


def anyspec():
    return pl.BlockSpec(memory_space=pltpu.HBM)


def sspec():
    return pl.BlockSpec(memory_space=pltpu.SMEM)


def dot(a, b):
    return jnp.dot(a, b, preferred_element_type=F32)


def rms_bf16(v):
    return (v * lax.rsqrt(jnp.mean(v * v, axis=-1, keepdims=True) + EPSILON)).astype(BF16)


def rope_table(seq, hd):
    half = hd // 2
    freqs = np.power(np.float32(ROPE_BASE), (np.float32(-2.0) * np.arange(half, dtype=np.float32) / np.float32(hd)))
    angle = np.arange(seq + 1, dtype=np.float32)[:, None] * freqs.astype(np.float32)[None, :]
    wide = angle.astype(np.float64)
    return np.concatenate([np.cos(wide), np.sin(wide)], axis=1).astype(np.float32)


def rope(vec, cos, sin):
    return vec * cos + pltpu.roll(vec, 64, 1) * sin


def project(h, cos, sin, wq, wk, wv, qs, kn, vn, rows):
    q = dot(h, wq[...])
    k = dot(h, wk[...])
    v = dot(h, wv[...])
    for j in range(q.shape[1] // 128):
        qs[rows, j * 128:(j + 1) * 128] = rope(q[:, j * 128:(j + 1) * 128], cos, sin).astype(BF16)
    for j in range(k.shape[1] // 128):
        kn[rows, j * 128:(j + 1) * 128] = rope(k[:, j * 128:(j + 1) * 128], cos, sin).astype(BF16)
    vn[rows, :] = v.astype(BF16)


def attn_kernel(layer, n_tok, first_layer, lens_in, *refs):
    if first_layer:
        (x_hbm, tab_hbm, wq_hbm, wk_hbm, wv_hbm, wo_hbm, kc, vc, os_, wo, cos_ref, sin_ref,
         x_ref, tab_ref, wq, wk, wv, qs, kn, vn, wsem, kbuf, vbuf, sbuf, mst, men, lens_ref, lsem, ksem, vsem, osem) = refs
    else:
        qs, kn, vn, wo_hbm, kc, vc, os_, wo, kbuf, vbuf, sbuf, mst, men, ksem, vsem, osem = refs
        lens_ref = lens_in
    t0 = lax.axis_index("pool") * n_tok
    if first_layer:
        lens_cp = pltpu.make_async_copy(lens_in, lens_ref, lsem)
        lens_cp.start()
    heads = qs.shape[1] // 128
    n_groups = n_tok // TOKG
    hpk = heads // 2
    cols = heads * TOKG

    def padded(ln):
        return pl.multiple_of(lax.shift_left(lax.shift_right_logical(ln + 7, 3), 4), 16)

    def start_group(g):
        slot = lax.rem(g, NSLOT)
        off = 0
        for i in range(TOKG):
            tok = t0 + g * TOKG + i
            ln = lens_ref[tok]
            n = padded(ln)
            off = pl.multiple_of(off, 16)
            pltpu.make_async_copy(kc.at[layer, tok, pl.ds(0, n), :], kbuf.at[slot, pl.ds(off, n), :], ksem.at[slot]).start()
            pltpu.make_async_copy(vc.at[layer, tok, pl.ds(0, n), :], vbuf.at[slot, pl.ds(off, n), :], vsem.at[slot]).start()
            mst[slot, i:i + 1, :] = jnp.full((1, 128), off, jnp.int32)
            men[slot, i:i + 1, :] = jnp.full((1, 128), off + 2 * ln, jnp.int32)
            off = off + n
        return jnp.asarray(off, jnp.int32)

    if first_layer:
        w_copies = [pltpu.make_async_copy(src.at[layer], dst, wsem.at[i])
                    for i, (src, dst) in enumerate(((wq_hbm, wq), (wk_hbm, wk), (wv_hbm, wv)))]
        x_cp = pltpu.make_async_copy(x_hbm.at[pl.ds(pl.multiple_of(t0, n_tok), n_tok), :], x_ref, wsem.at[3])
        tab_cp = pltpu.make_async_copy(tab_hbm, tab_ref, wsem.at[4])
        x_cp.start()
        tab_cp.start()
        for c in w_copies:
            c.start()
    if first_layer:
        lens_cp.wait()
    totals0 = tuple(start_group(jnp.int32(g)) for g in range(NSLOT - 1))
    wo_cp = pltpu.make_async_copy(wo_hbm.at[layer], wo, osem)
    wo_cp.start()
    if first_layer:
        x_cp.wait()
        tab_cp.wait()
        h = rms_bf16(x_ref[...].astype(F32))

        def pick(i, _):
            cos_ref[pl.ds(i, 1), :] = tab_ref[pl.ds(lens_ref[t0 + i], 1), :]
            return 0
        lax.fori_loop(0, n_tok, pick, 0)
        both = cos_ref[...]
        swapped = pltpu.roll(both, 64, 1)
        low = lax.broadcasted_iota(jnp.int32, both.shape, 1) < 64
        cos = jnp.where(low, both, swapped)
        sin = jnp.where(low, -swapped, both)
        cos_ref[...] = cos
        sin_ref[...] = sin
        for c in w_copies:
            c.wait()
        project(h, cos, sin, wq, wk, wv, qs, kn, vn, pl.ds(0, n_tok))
    scale = 128.0 ** -0.5 * 1.4426950408889634

    lane = lax.broadcasted_iota(jnp.int32, (cols, 128), 1)
    kv = (lax.broadcasted_iota(jnp.int32, (cols, 128), 0) >= (hpk * TOKG)).astype(jnp.int32)
    mine = (lane & 1) == kv

    def heads_of(ref, g):
        row = ref[pl.ds(pl.multiple_of(g * TOKG, TOKG), TOKG), :]
        per = heads // (ref.shape[1] // 128)
        return jnp.concatenate([row[:, (j // per) * 128:(j // per + 1) * 128] for j in range(heads)], axis=0)

    def step(g, totals):
        total = pl.multiple_of(totals[0], 16)
        slot = lax.rem(g, NSLOT)
        last = lax.cond(g + NSLOT - 1 < n_groups, lambda: start_group(g + NSLOT - 1), lambda: jnp.int32(0))
        q2 = heads_of(qs, g)
        s_new = jnp.sum(q2.astype(F32) * heads_of(kn, g).astype(F32), axis=1, keepdims=True)
        start = jnp.where(mine, jnp.concatenate([mst[slot]] * heads, axis=0) - lane, 1 << 30)
        end = jnp.concatenate([men[slot]] * heads, axis=0) - lane
        n = lax.shift_right_logical(total + TILE // 2 - 1, TILE.bit_length() - 1)
        m = n + jnp.where(total > n * TILE, 1, 0)
        vbuf[slot, pl.ds(total, TILE), :] = jnp.zeros((TILE, 128), BF16)
        pltpu.make_async_copy(kbuf.at[slot, pl.ds(0, total), :], kbuf.at[slot, pl.ds(0, total), :], ksem.at[slot]).wait()

        def first(i, macc, rows=TILE):
            base = pl.multiple_of(i * TILE, TILE)
            for j in range(rows // 256):
                at = pl.multiple_of(base + j * 256, 256)
                s = lax.dot_general(q2, kbuf[slot, pl.ds(at, 256), :], (((1,), (1,)), ((), ())), preferred_element_type=F32)
                for p in range(2):
                    off = at + p * 128
                    part = jnp.where((start <= off) & (end > off), s[:, p * 128:(p + 1) * 128], -jnp.inf)
                    sbuf[:, pl.ds(pl.multiple_of(off, 128), 128)] = part
                    macc = jnp.maximum(macc, part)
            return macc

        macc = lax.fori_loop(0, n, first, jnp.full((cols, 128), -jnp.inf, F32))
        macc = lax.fori_loop(n, m, functools.partial(first, rows=TILE // 2), macc)
        peak = jnp.maximum(jnp.max(macc, axis=1, keepdims=True), s_new)
        w_new = jnp.exp2((s_new - peak) * scale)
        peakb = jnp.broadcast_to(peak, (cols, 128))
        pltpu.make_async_copy(vbuf.at[slot, pl.ds(0, total), :], vbuf.at[slot, pl.ds(0, total), :], vsem.at[slot]).wait()

        def second(i, carry, rows=TILE):
            lacc, acc = carry
            base = pl.multiple_of(i * TILE, TILE)
            parts = []
            for j in range(rows // 128):
                p = jnp.exp2((sbuf[:, pl.ds(pl.multiple_of(base + j * 128, 128), 128)] - peakb) * scale)
                lacc = lacc + p
                parts.append(p.astype(BF16))
            acc = acc + dot(jnp.concatenate(parts, axis=1), vbuf[slot, pl.ds(base, rows), :])
            return lacc, acc

        zero = jnp.zeros((cols, 128), F32)
        lacc, acc = lax.fori_loop(0, n, second, (zero, zero))
        lacc, acc = lax.fori_loop(n, m, functools.partial(second, rows=TILE // 2), (lacc, acc))
        den = jnp.sum(lacc, axis=1, keepdims=True) + w_new
        o = ((acc + w_new.astype(BF16).astype(F32) * heads_of(vn, g).astype(F32)) / den).astype(BF16)
        g0 = pl.multiple_of(g * TOKG, TOKG)
        for j in range(heads):
            os_[pl.ds(g0, TOKG), j * 128:(j + 1) * 128] = o[j * TOKG:(j + 1) * TOKG, :]
        return totals[1:] + (last,)

    lax.fori_loop(0, n_groups, step, totals0)
    wo_cp.wait()


def attention(layer, n_tok, lens, w_out, kc, vc, proj=None, qkv=None):
    dma = pltpu.SemaphoreType.DMA
    first_layer = proj is not None
    out_shape = []
    if first_layer:
        x, tab, wq, wk, wv = proj
        model, qdim, kvdim = wq.shape[1], wq.shape[2], wk.shape[2]
        args = [lens, x, tab, wq, wk, wv, w_out, kc, vc]
        specs = [anyspec()] * 9
        out_shape = [VMEM((n_tok, qdim), BF16), VMEM(w_out.shape[1:], BF16)] + [jax.ShapeDtypeStruct((n_tok, 128), F32)] * 2
        scratch = [VMEM((n_tok, model), BF16), VMEM(tab.shape, F32), VMEM((model, qdim), BF16), VMEM((model, kvdim), BF16), VMEM((model, kvdim), BF16),
                   VMEM((n_tok, qdim), BF16), VMEM((n_tok, kvdim), BF16), VMEM((n_tok, kvdim), BF16), dma((5,))]
    else:
        qdim = qkv[0].shape[1]
        args = [lens, *qkv, w_out, kc, vc]
        specs = [sspec()] + [vspec()] * 3 + [anyspec()] * 3
        out_shape = [VMEM((n_tok, qdim), BF16), VMEM(w_out.shape[1:], BF16)]
        scratch = []
    max_rows = TOKG * kc.shape[2]
    cols = (qdim // 128) * TOKG
    scratch += [VMEM((NSLOT, max_rows + TILE, 128), BF16), VMEM((NSLOT, max_rows + TILE, 128), BF16), VMEM((cols, max_rows), F32),
                VMEM((NSLOT, TOKG, 128), jnp.int32), VMEM((NSLOT, TOKG, 128), jnp.int32), *([pltpu.SMEM(lens.shape, jnp.int32), dma] if first_layer else []), dma((NSLOT,)), dma((NSLOT,)), dma]
    return pl.pallas_call(
        functools.partial(attn_kernel, layer, n_tok, first_layer),
        out_shape=out_shape,
        in_specs=specs,
        out_specs=[vspec()] * len(out_shape),
        scratch_shapes=scratch,
        compiler_params=pltpu.CompilerParams(vmem_limit_bytes=LIM_A if first_layer else LIM_B),
        name=f"attention{layer}",
    )(*args)


NCH = 4


def peers():
    me = lax.axis_index("ep")
    core = me % 2
    x = me // 2
    return me, x * 2 + (1 - core), (1 - x) * 2 + core, (1 - x) * 2 + (1 - core)


def barrier(devices):
    sem = pltpu.get_barrier_semaphore()
    for d in devices:
        pl.semaphore_signal(sem, inc=1, device_id=d, device_id_type=MESH)
    return lambda: pl.semaphore_wait(sem, len(devices))


def rcopy(src, dst, ssem, rsem, dev):
    return pltpu.make_async_remote_copy(src_ref=src, dst_ref=dst, send_sem=ssem, recv_sem=rsem, device_id=dev, device_id_type=MESH)


def weight_copies(layer, e, f, slot, hbm, buf, sems):
    wg_hbm, wu_hbm, wd_hbm = hbm
    cols = pl.ds(f * FT, FT) if isinstance(f, int) else pl.ds(pl.multiple_of(f * FT, FT), FT)
    return (pltpu.make_async_copy(wg_hbm.at[layer, e, :, cols], buf[0].at[slot], sems.at[slot, 0]),
            pltpu.make_async_copy(wu_hbm.at[layer, e, :, cols], buf[1].at[slot], sems.at[slot, 1]),
            pltpu.make_async_copy(wd_hbm.at[layer, e, cols, :], buf[2].at[slot], sems.at[slot, 2]))


def dispatch_kernel(layer, steps, n_loc, os_ref, x_ref, ids_ref, wr_ref, wo, wg_hbm, wu_hbm, wd_hbm, *refs):
    first_layer = layer == 0
    if first_layer:
        a_ref, uall, rrow, mcol, idsall, pg, pu, pd, idsbuf, *sems = refs
        psem, s_p, r_p, s_x, r_x, s_f, r_f, s_i, r_i = sems
    else:
        a_ref, uall, rrow, mcol, pg, pu, pd, *sems = refs
        psem, s_p, r_p, s_x, r_x, s_f, r_f = sems
        idsall = ids_ref
    n = os_ref.shape[0]
    ch = n // NCH
    pool = lax.axis_index("pool")
    me, part, xp, diag = peers()
    devs = [{"ep": part}, {"ep": xp}]
    arrive = barrier(devs)

    def rows(ep, c):
        return pl.ds(pl.multiple_of(ep * n + c * ch, ch), ch)

    ics = []
    if first_layer:
        t0 = pl.multiple_of(pool * n, n)
        idsbuf[...] = jnp.zeros(idsbuf.shape, jnp.int32)
        for l in range(ids_ref.shape[0]):
            idsbuf[2 * l:2 * l + 2, :] = ids_ref[l, :, pl.ds(t0, n)]
        idsall[me] = idsbuf[...]
    xs, ps = [], []
    half = n // 2
    for hf in range(2):
        r = pl.ds(hf * half, half)
        if first_layer:
            xr = x_ref[pl.ds(pl.multiple_of(pool * n + hf * half, half), half), :]
        else:
            xr = x_ref[r, :]
        a = (xr.astype(F32) + dot(os_ref[r, :], wo[...])).astype(BF16)
        a_ref[r, :] = a
        uall[pl.ds(pl.multiple_of(me * n + hf * half, half), half), :] = rms_bf16(a.astype(F32))
        if hf == 0:
            arrive()
            if first_layer:
                for i, d in enumerate(devs):
                    cp = rcopy(idsbuf, idsall.at[me], s_i.at[i], r_i.at[i], d)
                    cp.start()
                    ics.append(cp)
        for c in range(hf * NCH // 2, (hf + 1) * NCH // 2):
            cp = rcopy(uall.at[rows(me, c)], uall.at[rows(me, c)], s_x.at[c], r_x.at[c], {"ep": xp})
            cp.start()
            xs.append(cp)
            cp = rcopy(uall.at[rows(me, c)], uall.at[rows(me, c)], s_p.at[c], r_p.at[c], {"ep": part})
            cp.start()
            ps.append(cp)
    hbm = (wg_hbm, wu_hbm, wd_hbm)

    def prefetch(f, _):
        for cp in weight_copies(layer, 0, f, f, hbm, (pg, pu, pd), psem):
            cp.start()
        return 0

    lax.fori_loop(0, steps, prefetch, 0)
    if first_layer:
        ics[1].wait_recv()
        cp = rcopy(idsall.at[xp], idsall.at[xp], s_i.at[2], r_i.at[2], devs[0])
        cp.start()
        cp.wait()
        ics[0].wait()
        ics[1].wait_send()

    tokens = 4 * n
    e0 = me * n_loc
    ids_row = [jnp.concatenate([idsall[b, 2 * layer + k:2 * layer + k + 1, :] for b in range(4)], axis=1) for k in range(2)]
    row8 = lax.broadcasted_iota(jnp.int32, (8, tokens), 0)
    hit = ((ids_row[0] == row8 + e0) | (ids_row[1] == row8 + e0)) & (row8 < n_loc)
    hit_f = hit.astype(F32)
    tri = (lax.broadcasted_iota(jnp.int32, (tokens, tokens), 0) < lax.broadcasted_iota(jnp.int32, (tokens, tokens), 1)).astype(F32).astype(BF16)
    rank = jnp.where(hit_f > 0, dot(hit_f.astype(BF16), tri), -1.0)
    rrow[...] = rank
    idf = jnp.where(row8 == 2, jnp.broadcast_to(ids_row[0].astype(F32), (8, tokens)),
                    jnp.where(row8 == 3, jnp.broadcast_to(ids_row[1].astype(F32), (8, tokens)), rank))
    mcol[...] = jnp.transpose(idf)

    w = wr_ref[layer]
    w1 = w.astype(BF16).astype(F32)
    w2 = (w - w1).astype(BF16).astype(F32)
    w3 = w - w1 - w2
    wr = jnp.concatenate([w1, w2, w3, jnp.zeros((104, w.shape[1]), F32)], axis=0).astype(BF16)
    e0f = e0.astype(F32)

    def gates(ep):
        r = pl.ds(pl.multiple_of(ep * n, n), n)
        lg = lax.dot_general(uall[r, :], wr, (((1,), (1,)), ((), ())), preferred_element_type=F32)
        lg = lg + pltpu.roll(lg, 120, 1) + pltpu.roll(lg, 112, 1)
        lane = lax.broadcasted_iota(jnp.int32, (n, 128), 1).astype(F32)
        col = mcol[r, :]
        id0, id1 = col[:, 2:3], col[:, 3:4]
        l0 = jnp.sum(jnp.where(lane == id0, lg, 0.0), axis=1, keepdims=True)
        l1 = jnp.sum(jnp.where(lane == id1, lg, 0.0), axis=1, keepdims=True)
        top = jnp.maximum(l0, l1)
        x0 = jnp.exp(l0 - top)
        x1 = jnp.exp(l1 - top)
        den = x0 + x1
        lane8 = lax.broadcasted_iota(jnp.int32, (n, 8), 1)
        expert = (lane8 - 2).astype(F32) + e0f
        g = jnp.where(id0 == expert, x0 / den, 0.0) + jnp.where(id1 == expert, x1 / den, 0.0)
        mcol[r, :] = jnp.where(lane8 < 2, col, g)

    gates(me)
    fs = []

    def forward(c):
        xs[c].wait_recv()
        cp = rcopy(uall.at[rows(xp, c)], uall.at[rows(xp, c)], s_f.at[c], r_f.at[c], {"ep": part})
        cp.start()
        fs.append(cp)

    for c in range(NCH - 1):
        forward(c)
    for cp in ps:
        cp.wait()
    gates(part)
    forward(NCH - 1)
    gates(xp)
    for cp in fs:
        cp.wait()
    gates(diag)
    for cp in xs:
        cp.wait_send()
    for f in range(steps):
        for cp in weight_copies(layer, 0, f, f, hbm, (pg, pu, pd), psem):
            cp.wait()


def dispatch(layer, os_, x, ids, wr, wo, wg, wu, wd):
    n, qdim = os_.shape
    model = wo.shape[1]
    n_loc, ff = wg.shape[1], wg.shape[3]
    steps = ff // FT
    dma = pltpu.SemaphoreType.DMA
    out_shape = [jax.ShapeDtypeStruct((n, model), BF16), jax.ShapeDtypeStruct((4 * n, model), BF16),
                 jax.ShapeDtypeStruct((8, 4 * n), F32), jax.ShapeDtypeStruct((4 * n, 8), F32)]
    scratch = []
    sems = [dma((steps, 3))] + [dma((NCH,))] * 6
    if layer == 0:
        out_shape.append(jax.ShapeDtypeStruct((4, 8, n), jnp.int32))
        scratch.append(VMEM((8, n), jnp.int32))
        sems += [dma((3,)), dma((3,))]
    n_small = len(out_shape)
    out_shape += [VMEM((steps, model, FT), BF16), VMEM((steps, model, FT), BF16), VMEM((steps, FT, model), BF16)]
    return pl.pallas_call(
        functools.partial(dispatch_kernel, layer, steps, n_loc),
        out_shape=out_shape,
        in_specs=[vspec()] * 5 + [anyspec()] * 3,
        out_specs=[vspec()] * n_small + [vspec()] * 3,
        scratch_shapes=scratch + sems,
        compiler_params=pltpu.CompilerParams(collective_id=2 * layer, has_side_effects=True, vmem_limit_bytes=LIM_D),
        name=f"dispatch{layer}",
    )(os_, x, ids, wr, wo, wg, wu, wd)


def expert_kernel(layer, u_ref, rrow_ref, mcol_ref, pg, pu, pd, wg_hbm, wu_hbm, wd_hbm, y_ref, wg, wu, wd, xe, yacc, sems):
    n = u_ref.shape[0]
    steps = pg.shape[0]
    n_loc = wg_hbm.shape[1]
    hbm = (wg_hbm, wu_hbm, wd_hbm)
    own = (wg, wu, wd)

    for e in range(1, n_loc):
        def issue(f, _, e=e):
            for c in weight_copies(layer, e, f, (e - 1) * steps + f, hbm, own, sems):
                c.start()
            return 0
        lax.fori_loop(0, steps, issue, 0)

    for e in range(n_loc):
        rank_row = rrow_ref[e:e + 1, :]
        count = jnp.sum((rank_row >= 0).astype(F32)).astype(jnp.int32)
        lo = 0
        for m in SIZES:
            @pl.when((count <= m) & ((count > lo) | (lo == 0)))
            def _(m=m, e=e):
                sel = (rank_row == lax.broadcasted_iota(jnp.int32, (m, n), 0).astype(F32)).astype(F32).astype(BF16)
                xe[pl.ds(0, m), :] = dot(sel, u_ref[...]).astype(BF16)
                yacc[pl.ds(0, m), :] = jnp.zeros((m, yacc.shape[1]), F32)

                def step(f, _):
                    if e == 0:
                        w1, w3, w2 = pg, pu, pd
                        slot = f
                    else:
                        w1, w3, w2 = own
                        slot = (e - 1) * steps + f
                        for c in weight_copies(layer, e, f, slot, hbm, own, sems):
                            c.wait()
                    gate = dot(xe[pl.ds(0, m), :], w1[slot])
                    up = dot(xe[pl.ds(0, m), :], w3[slot])
                    inner = (gate * jax.nn.sigmoid(gate) * up).astype(BF16)
                    yacc[pl.ds(0, m), :] += dot(inner, w2[slot])
                    return 0

                lax.fori_loop(0, steps, step, 0)
                y_ref[pl.ds(e * n, m), :] = yacc[pl.ds(0, m), :].astype(BF16)
                if m < n:
                    y_ref[pl.ds(e * n + m, n - m), :] = jnp.zeros((n - m, y_ref.shape[1]), BF16)
            lo = m


def experts(layer, u_all, rrow, mcol, pre, wg, wu, wd):
    n, model = u_all.shape
    steps = pre[0].shape[0]
    n_loc = wg.shape[1]
    slots = steps * (n_loc - 1)
    return pl.pallas_call(
        functools.partial(expert_kernel, layer),
        out_shape=jax.ShapeDtypeStruct((n_loc * n, model), BF16),
        in_specs=[vspec()] * 6 + [anyspec()] * 3,
        out_specs=vspec(),
        scratch_shapes=[VMEM((slots, model, FT), BF16), VMEM((slots, model, FT), BF16), VMEM((slots, FT, model), BF16),
                        VMEM((n, model), BF16), VMEM((n, model), F32), pltpu.SemaphoreType.DMA((slots, 3))],
        compiler_params=pltpu.CompilerParams(vmem_limit_bytes=LIM_E),
        name=f"experts{layer}",
    )(u_all, rrow, mcol, *pre, wg, wu, wd)


def combine_kernel(last, layer, y_ref, mcol_ref, a_ref, *refs):
    if last:
        out_ref, p_d, p_x, p_p, p_me, own, mid, far, *sems = refs
        s_o, r_o, s_m, r_m, s_f, r_f, s_y, r_y = sems
    else:
        (cos_ref, sin_ref, wq_hbm, wk_hbm, wv_hbm, out_ref, qs, kn, vn,
         p_d, p_x, p_p, p_me, own, mid, far, wq, wk, wv, *sems) = refs
        s_o, r_o, s_m, r_m, s_f, r_f, wsem = sems
    n = a_ref.shape[0]
    ch = n // CCH
    nn = mcol_ref.shape[0]
    me, part, xp, diag = peers()
    devs = [{"ep": part}, {"ep": xp}]
    if last:
        pool = lax.axis_index("pool")
        devs.append({"pool": 1 - pool})
    else:
        w_copies = [pltpu.make_async_copy(src.at[layer + 1], dst, wsem.at[i])
                    for i, (src, dst) in enumerate(((wq_hbm, wq), (wk_hbm, wk), (wv_hbm, wv)))]
        for c in w_copies:
            c.start()

    def partial(ep):
        col = mcol_ref[pl.ds(pl.multiple_of(ep * n, n), n), :]
        slot = lax.broadcasted_iota(jnp.int32, (n, nn), 1).astype(F32)
        total = None
        for e in range(y_ref.shape[0] // nn):
            sel = (col[:, e:e + 1] == slot).astype(F32).astype(BF16)
            t = dot(sel, y_ref[e * nn:(e + 1) * nn, :]) * col[:, 2 + e:3 + e]
            total = t if total is None else total + t
        return total

    arrive = barrier(devs)
    p_d[...] = partial(diag)
    arrive()
    depth = 4 if last else CCH
    mids, fars, ys = [], [], []
    for c in range(CCH):
        r = pl.ds(c * ch, ch)
        cp = rcopy(p_d.at[r], mid.at[r], s_m.at[c], r_m.at[c], devs[0])
        cp.start()
        mids.append(cp)
    p_x[...] = partial(xp)

    def send(c):
        r = pl.ds(c * ch, ch)
        mids[c].wait_recv()
        p_x[r, :] = p_x[r, :] + mid[r, :]
        if c >= depth:
            fars[c - depth].wait_send()
        cp = rcopy(p_x.at[r], far.at[r], s_f.at[c], r_f.at[c], devs[1])
        cp.start()
        fars.append(cp)

    def receive(c):
        r = pl.ds(c * ch, ch)
        fars[c].wait_recv()
        res = (p_me[r, :] + far[r, :]).astype(BF16)
        if last:
            o = pl.ds(pl.multiple_of(pool * n + c * ch, ch), ch)
            out_ref[o, :] = res
            cp = rcopy(out_ref.at[o], out_ref.at[o], s_y.at[c], r_y.at[c], devs[2])
            cp.start()
            ys.append(cp)
        else:
            out_ref[r, :] = res
            if c % (CCH // 2) == CCH // 2 - 1:
                r2 = pl.ds(c * ch + ch - n // 2, n // 2)
                h = rms_bf16(out_ref[r2, :].astype(F32))
                project(h, cos_ref[r2, :], sin_ref[r2, :], wq, wk, wv, qs, kn, vn, r2)

    for c in range(depth):
        send(c)
    p_p[...] = partial(part)
    own_cp = rcopy(p_p, own, s_o, r_o, devs[0])
    own_cp.start()
    p_me[...] = partial(me)
    own_cp.wait()
    p_me[...] = a_ref[...].astype(F32) + (p_me[...] + own[...])
    if not last:
        for c in w_copies:
            c.wait()
    for c in range(depth, CCH):
        send(c)
        receive(c - depth)
    for c in range(CCH - depth, CCH):
        receive(c)
    for c in range(CCH):
        mids[c].wait_send()
    for c in range(CCH - depth, CCH):
        fars[c].wait_send()
    for cp in ys:
        cp.wait()


def combine(layer, last, y, mcol, a, nxt=None):
    n, model = a.shape
    dma = pltpu.SemaphoreType.DMA
    sems = [dma, dma, dma((CCH,)), dma((CCH,)), dma((CCH,)), dma((CCH,))]
    args = [y, mcol, a]
    specs = [vspec()] * 3
    scratch = [VMEM((n, model), F32) for _ in range(7)]
    if last:
        sems += [dma((CCH,)), dma((CCH,))]
        out_shape = jax.ShapeDtypeStruct((2 * n, model), BF16)
        out_specs = vspec()
    else:
        cos, sin, wq, wk, wv = nxt
        args += [cos, sin, wq, wk, wv]
        specs += [vspec()] * 2 + [anyspec()] * 3
        sems += [dma((3,))]
        scratch += [VMEM(w.shape[1:], BF16) for w in (wq, wk, wv)]
        out_shape = [jax.ShapeDtypeStruct((n, model), BF16)] + [jax.ShapeDtypeStruct((n, w.shape[2]), BF16) for w in (wq, wk, wv)]
        out_specs = [vspec()] * 4
    return pl.pallas_call(
        functools.partial(combine_kernel, last, layer),
        out_shape=out_shape,
        in_specs=specs,
        out_specs=out_specs,
        scratch_shapes=scratch + sems,
        compiler_params=pltpu.CompilerParams(collective_id=2 * layer + 1, has_side_effects=True, vmem_limit_bytes=LIM_C),
        name=f"combine{layer}",
    )(*args)


def solution(mesh):
    def body(hidden, k_cache, v_cache, lengths, expert_ids, w_query, w_key, w_value, w_out, w_router, w_gate, w_up, w_down):
        n_layers, _, seq, kvh, hd = k_cache.shape
        n_tok = hidden.shape[0] // 2
        kc = k_cache.reshape(n_layers, -1, seq * kvh, hd)
        vc = v_cache.reshape(n_layers, -1, seq * kvh, hd)
        ids = expert_ids.transpose(0, 2, 1)
        wr = w_router.transpose(0, 2, 1)
        tab = jnp.asarray(rope_table(seq, hd))
        w_query, w_key, w_value, w_out, w_gate, w_up, w_down, kc, vc, tab, hidden_h, lens_h = (
            pltpu.with_memory_space_constraint(v, pltpu.HBM) for v in (w_query, w_key, w_value, w_out, w_gate, w_up, w_down, kc, vc, tab, hidden, lengths))
        state = hidden
        qkv = None
        for layer in range(n_layers):
            last = layer == n_layers - 1
            if layer == 0:
                att, wo, cos, sin = attention(layer, n_tok, lens_h, w_out, kc, vc, proj=(hidden_h, tab, w_query, w_key, w_value))
            else:
                att, wo = attention(layer, n_tok, lengths, w_out, kc, vc, qkv=qkv)
            outs = dispatch(layer, att, state, ids, wr, wo, w_gate, w_up, w_down)
            a, u_all, rrow, mcol = outs[:4]
            if layer == 0:
                ids = outs[4]
            y = experts(layer, u_all, rrow, mcol, outs[-3:], w_gate, w_up, w_down)
            if last:
                return combine(layer, True, y, mcol, a)
            state, *qkv = combine(layer, False, y, mcol, a, nxt=(cos, sin, w_query, w_key, w_value))

    rows_spec = ("dp", "ep")
    in_specs = (P(rows_spec, None), P(None, rows_spec), P(None, rows_spec), P(rows_spec), P(None, rows_spec, None), P(), P(), P(), P(), P(), P(None, "ep"), P(None, "ep"), P(None, "ep"))
    return jax.shard_map(body, mesh=mesh, in_specs=in_specs, out_specs=P(rows_spec, None), check_vma=False)
```

```python
import functools

import numpy as np

import jax
import jax.numpy as jnp
from jax import lax
from jax.experimental import pallas as pl
from jax.experimental.pallas import tpu as pltpu
from jax.sharding import PartitionSpec as P

MESH = pl.DeviceIdType.MESH
EPSILON = 1e-6
ROPE_BASE = 10000.0
VMEM = pltpu.VMEM
F32 = jnp.float32
BF16 = jnp.bfloat16

TOKG = 16
TILE = 1024
FT = 512
NSLOT = 3
CCH = 8
LIM_A = 50 * 1024 * 1024
LIM_B = 50 * 1024 * 1024
LIM_D = 8 * 1024 * 1024
LIM_E = 27 * 1024 * 1024
LIM_C = 16 * 1024 * 1024
SIZES = (128, 400, 512)


def vspec():
    return pl.BlockSpec(memory_space=VMEM)


def anyspec():
    return pl.BlockSpec(memory_space=pltpu.HBM)


def sspec():
    return pl.BlockSpec(memory_space=pltpu.SMEM)


def dot(a, b):
    return jnp.dot(a, b, preferred_element_type=F32)


def rms_bf16(v):
    return (v * lax.rsqrt(jnp.mean(v * v, axis=-1, keepdims=True) + EPSILON)).astype(BF16)


def rope_table(seq, hd):
    half = hd // 2
    freqs = np.power(np.float32(ROPE_BASE), (np.float32(-2.0) * np.arange(half, dtype=np.float32) / np.float32(hd)))
    angle = np.arange(seq + 1, dtype=np.float32)[:, None] * freqs.astype(np.float32)[None, :]
    wide = angle.astype(np.float64)
    return np.concatenate([np.cos(wide), np.sin(wide)], axis=1).astype(np.float32)


def rope(vec, cos, sin):
    return vec * cos + pltpu.roll(vec, 64, 1) * sin


def project(h, cos, sin, wq, wk, wv, qs, kn, vn, rows):
    q = dot(h, wq[...])
    k = dot(h, wk[...])
    v = dot(h, wv[...])
    for j in range(q.shape[1] // 128):
        qs[rows, j * 128:(j + 1) * 128] = rope(q[:, j * 128:(j + 1) * 128], cos, sin).astype(BF16)
    for j in range(k.shape[1] // 128):
        kn[rows, j * 128:(j + 1) * 128] = rope(k[:, j * 128:(j + 1) * 128], cos, sin).astype(BF16)
    vn[rows, :] = v.astype(BF16)


def attn_kernel(layer, n_tok, first_layer, lens_in, *refs):
    if first_layer:
        (x_hbm, tab_hbm, wq_hbm, wk_hbm, wv_hbm, wo_hbm, kc, vc, os_, wo, cos_ref, sin_ref,
         x_ref, tab_ref, wq, wk, wv, qs, kn, vn, wsem, kbuf, vbuf, sbuf, mst, men, lens_ref, lsem, ksem, vsem, osem) = refs
    else:
        qs, kn, vn, wo_hbm, kc, vc, os_, wo, kbuf, vbuf, sbuf, mst, men, ksem, vsem, osem = refs
        lens_ref = lens_in
    t0 = lax.axis_index("pool") * n_tok
    if first_layer:
        lens_cp = pltpu.make_async_copy(lens_in, lens_ref, lsem)
        lens_cp.start()
    heads = qs.shape[1] // 128
    n_groups = n_tok // TOKG
    hpk = heads // 2
    cols = heads * TOKG

    def padded(ln):
        return pl.multiple_of(lax.shift_left(lax.shift_right_logical(ln + 7, 3), 4), 16)

    def start_group(g):
        slot = lax.rem(g, NSLOT)
        off = 0
        for i in range(TOKG):
            tok = t0 + g * TOKG + i
            ln = lens_ref[tok]
            n = padded(ln)
            off = pl.multiple_of(off, 16)
            pltpu.make_async_copy(kc.at[layer, tok, pl.ds(0, n), :], kbuf.at[slot, pl.ds(off, n), :], ksem.at[slot]).start()
            pltpu.make_async_copy(vc.at[layer, tok, pl.ds(0, n), :], vbuf.at[slot, pl.ds(off, n), :], vsem.at[slot]).start()
            mst[slot, i:i + 1, :] = jnp.full((1, 128), off, jnp.int32)
            men[slot, i:i + 1, :] = jnp.full((1, 128), off + 2 * ln, jnp.int32)
            off = off + n
        return jnp.asarray(off, jnp.int32)

    if first_layer:
        w_copies = [pltpu.make_async_copy(src.at[layer], dst, wsem.at[i])
                    for i, (src, dst) in enumerate(((wq_hbm, wq), (wk_hbm, wk), (wv_hbm, wv)))]
        x_cp = pltpu.make_async_copy(x_hbm.at[pl.ds(pl.multiple_of(t0, n_tok), n_tok), :], x_ref, wsem.at[3])
        tab_cp = pltpu.make_async_copy(tab_hbm, tab_ref, wsem.at[4])
        x_cp.start()
        tab_cp.start()
        for c in w_copies:
            c.start()
    if first_layer:
        lens_cp.wait()
    totals0 = tuple(start_group(jnp.int32(g)) for g in range(NSLOT - 1))
    wo_cp = pltpu.make_async_copy(wo_hbm.at[layer], wo, osem)
    wo_cp.start()
    if first_layer:
        x_cp.wait()
        tab_cp.wait()
        h = rms_bf16(x_ref[...].astype(F32))

        def pick(i, _):
            cos_ref[pl.ds(i, 1), :] = tab_ref[pl.ds(lens_ref[t0 + i], 1), :]
            return 0
        lax.fori_loop(0, n_tok, pick, 0, unroll=8)
        both = cos_ref[...]
        swapped = pltpu.roll(both, 64, 1)
        low = lax.broadcasted_iota(jnp.int32, both.shape, 1) < 64
        cos = jnp.where(low, both, swapped)
        sin = jnp.where(low, -swapped, both)
        cos_ref[...] = cos
        sin_ref[...] = sin
        for c in w_copies:
            c.wait()
        project(h, cos, sin, wq, wk, wv, qs, kn, vn, pl.ds(0, n_tok))
    scale = 128.0 ** -0.5 * 1.4426950408889634

    lane = lax.broadcasted_iota(jnp.int32, (cols, 128), 1)
    kv = (lax.broadcasted_iota(jnp.int32, (cols, 128), 0) >= (hpk * TOKG)).astype(jnp.int32)
    mine = (lane & 1) == kv

    def heads_of(ref, g):
        row = ref[pl.ds(pl.multiple_of(g * TOKG, TOKG), TOKG), :]
        per = heads // (ref.shape[1] // 128)
        return jnp.concatenate([row[:, (j // per) * 128:(j // per + 1) * 128] for j in range(heads)], axis=0)

    def step(g, totals):
        total = pl.multiple_of(totals[0], 16)
        slot = lax.rem(g, NSLOT)
        last = lax.cond(g + NSLOT - 1 < n_groups, lambda: start_group(g + NSLOT - 1), lambda: jnp.int32(0))
        q2 = heads_of(qs, g)
        s_new = jnp.sum(q2.astype(F32) * heads_of(kn, g).astype(F32), axis=1, keepdims=True)
        start = jnp.where(mine, jnp.concatenate([mst[slot]] * heads, axis=0) - lane, 1 << 30)
        end = jnp.concatenate([men[slot]] * heads, axis=0) - lane
        n = lax.shift_right_logical(total + TILE // 2 - 1, TILE.bit_length() - 1)
        m = n + jnp.where(total > n * TILE, 1, 0)
        vbuf[slot, pl.ds(total, TILE), :] = jnp.zeros((TILE, 128), BF16)
        pltpu.make_async_copy(kbuf.at[slot, pl.ds(0, total), :], kbuf.at[slot, pl.ds(0, total), :], ksem.at[slot]).wait()

        def first(i, macc, rows=TILE):
            base = pl.multiple_of(i * TILE, TILE)
            for j in range(rows // 256):
                at = pl.multiple_of(base + j * 256, 256)
                s = lax.dot_general(q2, kbuf[slot, pl.ds(at, 256), :], (((1,), (1,)), ((), ())), preferred_element_type=F32)
                for p in range(2):
                    off = at + p * 128
                    part = jnp.where((start <= off) & (end > off), s[:, p * 128:(p + 1) * 128], -jnp.inf)
                    sbuf[:, pl.ds(pl.multiple_of(off, 128), 128)] = part
                    macc = jnp.maximum(macc, part)
            return macc

        macc = lax.fori_loop(0, n, first, jnp.full((cols, 128), -jnp.inf, F32))
        macc = lax.fori_loop(n, m, functools.partial(first, rows=TILE // 2), macc)
        peak = jnp.maximum(jnp.max(macc, axis=1, keepdims=True), s_new)
        w_new = jnp.exp2((s_new - peak) * scale)
        peakb = jnp.broadcast_to(peak, (cols, 128))
        pltpu.make_async_copy(vbuf.at[slot, pl.ds(0, total), :], vbuf.at[slot, pl.ds(0, total), :], vsem.at[slot]).wait()

        def second(i, carry, rows=TILE):
            lacc, acc = carry
            base = pl.multiple_of(i * TILE, TILE)
            parts = []
            for j in range(rows // 128):
                p = jnp.exp2((sbuf[:, pl.ds(pl.multiple_of(base + j * 128, 128), 128)] - peakb) * scale)
                lacc = lacc + p
                parts.append(p.astype(BF16))
            acc = acc + dot(jnp.concatenate(parts, axis=1), vbuf[slot, pl.ds(base, rows), :])
            return lacc, acc

        zero = jnp.zeros((cols, 128), F32)
        lacc, acc = lax.fori_loop(0, n, second, (zero, zero))
        lacc, acc = lax.fori_loop(n, m, functools.partial(second, rows=TILE // 2), (lacc, acc))
        den = jnp.sum(lacc, axis=1, keepdims=True) + w_new
        o = ((acc + w_new.astype(BF16).astype(F32) * heads_of(vn, g).astype(F32)) / den).astype(BF16)
        g0 = pl.multiple_of(g * TOKG, TOKG)
        for j in range(heads):
            os_[pl.ds(g0, TOKG), j * 128:(j + 1) * 128] = o[j * TOKG:(j + 1) * TOKG, :]
        return totals[1:] + (last,)

    lax.fori_loop(0, n_groups, step, totals0)
    wo_cp.wait()


def attention(layer, n_tok, lens, w_out, kc, vc, proj=None, qkv=None):
    dma = pltpu.SemaphoreType.DMA
    first_layer = proj is not None
    out_shape = []
    if first_layer:
        x, tab, wq, wk, wv = proj
        model, qdim, kvdim = wq.shape[1], wq.shape[2], wk.shape[2]
        args = [lens, x, tab, wq, wk, wv, w_out, kc, vc]
        specs = [anyspec()] * 9
        out_shape = [VMEM((n_tok, qdim), BF16), VMEM(w_out.shape[1:], BF16)] + [jax.ShapeDtypeStruct((n_tok, 128), F32)] * 2
        scratch = [VMEM((n_tok, model), BF16), VMEM(tab.shape, F32), VMEM((model, qdim), BF16), VMEM((model, kvdim), BF16), VMEM((model, kvdim), BF16),
                   VMEM((n_tok, qdim), BF16), VMEM((n_tok, kvdim), BF16), VMEM((n_tok, kvdim), BF16), dma((5,))]
    else:
        qdim = qkv[0].shape[1]
        args = [lens, *qkv, w_out, kc, vc]
        specs = [sspec()] + [vspec()] * 3 + [anyspec()] * 3
        out_shape = [VMEM((n_tok, qdim), BF16), VMEM(w_out.shape[1:], BF16)]
        scratch = []
    max_rows = TOKG * kc.shape[2]
    cols = (qdim // 128) * TOKG
    scratch += [VMEM((NSLOT, max_rows + TILE, 128), BF16), VMEM((NSLOT, max_rows + TILE, 128), BF16), VMEM((cols, max_rows), F32),
                VMEM((NSLOT, TOKG, 128), jnp.int32), VMEM((NSLOT, TOKG, 128), jnp.int32), *([pltpu.SMEM(lens.shape, jnp.int32), dma] if first_layer else []), dma((NSLOT,)), dma((NSLOT,)), dma]
    return pl.pallas_call(
        functools.partial(attn_kernel, layer, n_tok, first_layer),
        out_shape=out_shape,
        in_specs=specs,
        out_specs=[vspec()] * len(out_shape),
        scratch_shapes=scratch,
        compiler_params=pltpu.CompilerParams(vmem_limit_bytes=LIM_A if first_layer else LIM_B),
        name=f"attention{layer}",
    )(*args)


NCH = 4


def peers():
    me = lax.axis_index("ep")
    core = me % 2
    x = me // 2
    return me, x * 2 + (1 - core), (1 - x) * 2 + core, (1 - x) * 2 + (1 - core)


def barrier(devices):
    sem = pltpu.get_barrier_semaphore()
    for d in devices:
        pl.semaphore_signal(sem, inc=1, device_id=d, device_id_type=MESH)
    return lambda: pl.semaphore_wait(sem, len(devices))


def rcopy(src, dst, ssem, rsem, dev):
    return pltpu.make_async_remote_copy(src_ref=src, dst_ref=dst, send_sem=ssem, recv_sem=rsem, device_id=dev, device_id_type=MESH)


def weight_copies(layer, e, f, slot, hbm, buf, sems):
    wg_hbm, wu_hbm, wd_hbm = hbm
    cols = pl.ds(f * FT, FT) if isinstance(f, int) else pl.ds(pl.multiple_of(f * FT, FT), FT)
    return (pltpu.make_async_copy(wg_hbm.at[layer, e, :, cols], buf[0].at[slot], sems.at[slot, 0]),
            pltpu.make_async_copy(wu_hbm.at[layer, e, :, cols], buf[1].at[slot], sems.at[slot, 1]),
            pltpu.make_async_copy(wd_hbm.at[layer, e, cols, :], buf[2].at[slot], sems.at[slot, 2]))


def dispatch_kernel(layer, steps, n_loc, os_ref, x_ref, ids_ref, wr_ref, wo, wg_hbm, wu_hbm, wd_hbm, *refs):
    first_layer = layer == 0
    if first_layer:
        a_ref, uall, rrow, mcol, idsall, pg, pu, pd, idsbuf, *sems = refs
        psem, s_p, r_p, s_x, r_x, s_f, r_f, s_i, r_i = sems
    else:
        a_ref, uall, rrow, mcol, pg, pu, pd, *sems = refs
        psem, s_p, r_p, s_x, r_x, s_f, r_f = sems
        idsall = ids_ref
    n = os_ref.shape[0]
    ch = n // NCH
    pool = lax.axis_index("pool")
    me, part, xp, diag = peers()
    devs = [{"ep": part}, {"ep": xp}]
    arrive = barrier(devs)

    def rows(ep, c):
        return pl.ds(pl.multiple_of(ep * n + c * ch, ch), ch)

    ics = []
    if first_layer:
        t0 = pl.multiple_of(pool * n, n)
        idsbuf[...] = jnp.zeros(idsbuf.shape, jnp.int32)
        for l in range(ids_ref.shape[0]):
            idsbuf[2 * l:2 * l + 2, :] = ids_ref[l, :, pl.ds(t0, n)]
        idsall[me] = idsbuf[...]
    xs, ps = [], []
    half = n // 2
    for hf in range(2):
        r = pl.ds(hf * half, half)
        if first_layer:
            xr = x_ref[pl.ds(pl.multiple_of(pool * n + hf * half, half), half), :]
        else:
            xr = x_ref[r, :]
        a = (xr.astype(F32) + dot(os_ref[r, :], wo[...])).astype(BF16)
        a_ref[r, :] = a
        uall[pl.ds(pl.multiple_of(me * n + hf * half, half), half), :] = rms_bf16(a.astype(F32))
        if hf == 0:
            arrive()
            if first_layer:
                for i, d in enumerate(devs):
                    cp = rcopy(idsbuf, idsall.at[me], s_i.at[i], r_i.at[i], d)
                    cp.start()
                    ics.append(cp)
        for c in range(hf * NCH // 2, (hf + 1) * NCH // 2):
            cp = rcopy(uall.at[rows(me, c)], uall.at[rows(me, c)], s_x.at[c], r_x.at[c], {"ep": xp})
            cp.start()
            xs.append(cp)
            cp = rcopy(uall.at[rows(me, c)], uall.at[rows(me, c)], s_p.at[c], r_p.at[c], {"ep": part})
            cp.start()
            ps.append(cp)
    hbm = (wg_hbm, wu_hbm, wd_hbm)

    def prefetch(f, _):
        for cp in weight_copies(layer, 0, f, f, hbm, (pg, pu, pd), psem):
            cp.start()
        return 0

    lax.fori_loop(0, steps, prefetch, 0)
    if first_layer:
        ics[1].wait_recv()
        cp = rcopy(idsall.at[xp], idsall.at[xp], s_i.at[2], r_i.at[2], devs[0])
        cp.start()
        cp.wait()
        ics[0].wait()
        ics[1].wait_send()

    tokens = 4 * n
    e0 = me * n_loc
    ids_row = [jnp.concatenate([idsall[b, 2 * layer + k:2 * layer + k + 1, :] for b in range(4)], axis=1) for k in range(2)]
    row8 = lax.broadcasted_iota(jnp.int32, (8, tokens), 0)
    hit = ((ids_row[0] == row8 + e0) | (ids_row[1] == row8 + e0)) & (row8 < n_loc)
    hit_f = hit.astype(F32)
    tri = (lax.broadcasted_iota(jnp.int32, (tokens, tokens), 0) < lax.broadcasted_iota(jnp.int32, (tokens, tokens), 1)).astype(F32).astype(BF16)
    rank = jnp.where(hit_f > 0, dot(hit_f.astype(BF16), tri), -1.0)
    rrow[...] = rank
    idf = jnp.where(row8 == 2, jnp.broadcast_to(ids_row[0].astype(F32), (8, tokens)),
                    jnp.where(row8 == 3, jnp.broadcast_to(ids_row[1].astype(F32), (8, tokens)), rank))
    mcol[...] = jnp.transpose(idf)

    w = wr_ref[layer]
    w1 = w.astype(BF16).astype(F32)
    w2 = (w - w1).astype(BF16).astype(F32)
    w3 = w - w1 - w2
    wr = jnp.concatenate([w1, w2, w3, jnp.zeros((104, w.shape[1]), F32)], axis=0).astype(BF16)
    e0f = e0.astype(F32)

    def gates(ep):
        r = pl.ds(pl.multiple_of(ep * n, n), n)
        lg = lax.dot_general(uall[r, :], wr, (((1,), (1,)), ((), ())), preferred_element_type=F32)
        lg = lg + pltpu.roll(lg, 120, 1) + pltpu.roll(lg, 112, 1)
        lane = lax.broadcasted_iota(jnp.int32, (n, 128), 1).astype(F32)
        col = mcol[r, :]
        id0, id1 = col[:, 2:3], col[:, 3:4]
        l0 = jnp.sum(jnp.where(lane == id0, lg, 0.0), axis=1, keepdims=True)
        l1 = jnp.sum(jnp.where(lane == id1, lg, 0.0), axis=1, keepdims=True)
        top = jnp.maximum(l0, l1)
        x0 = jnp.exp(l0 - top)
        x1 = jnp.exp(l1 - top)
        den = x0 + x1
        lane8 = lax.broadcasted_iota(jnp.int32, (n, 8), 1)
        expert = (lane8 - 2).astype(F32) + e0f
        g = jnp.where(id0 == expert, x0 / den, 0.0) + jnp.where(id1 == expert, x1 / den, 0.0)
        mcol[r, :] = jnp.where(lane8 < 2, col, g)

    gates(me)
    fs = []

    def forward(c):
        xs[c].wait_recv()
        cp = rcopy(uall.at[rows(xp, c)], uall.at[rows(xp, c)], s_f.at[c], r_f.at[c], {"ep": part})
        cp.start()
        fs.append(cp)

    for c in range(NCH - 1):
        forward(c)
    for cp in ps:
        cp.wait()
    gates(part)
    forward(NCH - 1)
    gates(xp)
    for cp in fs:
        cp.wait()
    gates(diag)
    for cp in xs:
        cp.wait_send()
    for f in range(steps):
        for cp in weight_copies(layer, 0, f, f, hbm, (pg, pu, pd), psem):
            cp.wait()


def dispatch(layer, os_, x, ids, wr, wo, wg, wu, wd):
    n, qdim = os_.shape
    model = wo.shape[1]
    n_loc, ff = wg.shape[1], wg.shape[3]
    steps = ff // FT
    dma = pltpu.SemaphoreType.DMA
    out_shape = [jax.ShapeDtypeStruct((n, model), BF16), jax.ShapeDtypeStruct((4 * n, model), BF16),
                 jax.ShapeDtypeStruct((8, 4 * n), F32), jax.ShapeDtypeStruct((4 * n, 8), F32)]
    scratch = []
    sems = [dma((steps, 3))] + [dma((NCH,))] * 6
    if layer == 0:
        out_shape.append(jax.ShapeDtypeStruct((4, 8, n), jnp.int32))
        scratch.append(VMEM((8, n), jnp.int32))
        sems += [dma((3,)), dma((3,))]
    n_small = len(out_shape)
    out_shape += [VMEM((steps, model, FT), BF16), VMEM((steps, model, FT), BF16), VMEM((steps, FT, model), BF16)]
    return pl.pallas_call(
        functools.partial(dispatch_kernel, layer, steps, n_loc),
        out_shape=out_shape,
        in_specs=[vspec()] * 5 + [anyspec()] * 3,
        out_specs=[vspec()] * n_small + [vspec()] * 3,
        scratch_shapes=scratch + sems,
        compiler_params=pltpu.CompilerParams(collective_id=2 * layer, has_side_effects=True, vmem_limit_bytes=LIM_D),
        name=f"dispatch{layer}",
    )(os_, x, ids, wr, wo, wg, wu, wd)


def expert_kernel(layer, u_ref, rrow_ref, mcol_ref, pg, pu, pd, wg_hbm, wu_hbm, wd_hbm, y_ref, wg, wu, wd, xe, yacc, sems):
    n = u_ref.shape[0]
    steps = pg.shape[0]
    n_loc = wg_hbm.shape[1]
    hbm = (wg_hbm, wu_hbm, wd_hbm)
    own = (wg, wu, wd)

    for e in range(1, n_loc):
        def issue(f, _, e=e):
            for c in weight_copies(layer, e, f, (e - 1) * steps + f, hbm, own, sems):
                c.start()
            return 0
        lax.fori_loop(0, steps, issue, 0)

    for e in range(n_loc):
        rank_row = rrow_ref[e:e + 1, :]
        count = jnp.sum((rank_row >= 0).astype(F32)).astype(jnp.int32)
        lo = 0
        for m in SIZES:
            @pl.when((count <= m) & ((count > lo) | (lo == 0)))
            def _(m=m, e=e):
                sel = (rank_row == lax.broadcasted_iota(jnp.int32, (m, n), 0).astype(F32)).astype(F32).astype(BF16)
                xe[pl.ds(0, m), :] = dot(sel, u_ref[...]).astype(BF16)
                yacc[pl.ds(0, m), :] = jnp.zeros((m, yacc.shape[1]), F32)

                def step(f, _):
                    if e == 0:
                        w1, w3, w2 = pg, pu, pd
                        slot = f
                    else:
                        w1, w3, w2 = own
                        slot = (e - 1) * steps + f
                        for c in weight_copies(layer, e, f, slot, hbm, own, sems):
                            c.wait()
                    inner = []
                    for j in range(FT // 256):
                        at = pl.ds(j * 256, 256)
                        gate = dot(xe[pl.ds(0, m), :], w1[slot, :, at])
                        up = dot(xe[pl.ds(0, m), :], w3[slot, :, at])
                        inner.append((gate * jax.nn.sigmoid(gate) * up).astype(BF16))
                    yacc[pl.ds(0, m), :] += dot(jnp.concatenate(inner, axis=1), w2[slot])
                    return 0

                lax.fori_loop(0, steps, step, 0)
                y_ref[pl.ds(e * n, m), :] = yacc[pl.ds(0, m), :].astype(BF16)
                if m < n:
                    y_ref[pl.ds(e * n + m, n - m), :] = jnp.zeros((n - m, y_ref.shape[1]), BF16)
            lo = m


def experts(layer, u_all, rrow, mcol, pre, wg, wu, wd):
    n, model = u_all.shape
    steps = pre[0].shape[0]
    n_loc = wg.shape[1]
    slots = steps * (n_loc - 1)
    return pl.pallas_call(
        functools.partial(expert_kernel, layer),
        out_shape=jax.ShapeDtypeStruct((n_loc * n, model), BF16),
        in_specs=[vspec()] * 6 + [anyspec()] * 3,
        out_specs=vspec(),
        scratch_shapes=[VMEM((slots, model, FT), BF16), VMEM((slots, model, FT), BF16), VMEM((slots, FT, model), BF16),
                        VMEM((n, model), BF16), VMEM((n, model), F32), pltpu.SemaphoreType.DMA((slots, 3))],
        compiler_params=pltpu.CompilerParams(vmem_limit_bytes=LIM_E),
        name=f"experts{layer}",
    )(u_all, rrow, mcol, *pre, wg, wu, wd)


def combine_kernel(last, layer, y_ref, mcol_ref, a_ref, *refs):
    if last:
        out_ref, p_d, p_x, p_p, p_me, own, mid, far, *sems = refs
        s_o, r_o, s_m, r_m, s_f, r_f, s_y, r_y = sems
    else:
        (cos_ref, sin_ref, wq_hbm, wk_hbm, wv_hbm, out_ref, qs, kn, vn,
         p_d, p_x, p_p, p_me, own, mid, far, wq, wk, wv, *sems) = refs
        s_o, r_o, s_m, r_m, s_f, r_f, wsem = sems
    n = a_ref.shape[0]
    ch = n // CCH
    nn = mcol_ref.shape[0]
    me, part, xp, diag = peers()
    devs = [{"ep": part}, {"ep": xp}]
    if last:
        pool = lax.axis_index("pool")
        devs.append({"pool": 1 - pool})
    else:
        w_copies = [pltpu.make_async_copy(src.at[layer + 1], dst, wsem.at[i])
                    for i, (src, dst) in enumerate(((wq_hbm, wq), (wk_hbm, wk), (wv_hbm, wv)))]
        for c in w_copies:
            c.start()

    def partial(ep):
        col = mcol_ref[pl.ds(pl.multiple_of(ep * n, n), n), :]
        slot = lax.broadcasted_iota(jnp.int32, (n, nn), 1).astype(F32)
        total = None
        for e in range(y_ref.shape[0] // nn):
            sel = (col[:, e:e + 1] == slot).astype(F32).astype(BF16)
            t = dot(sel, y_ref[e * nn:(e + 1) * nn, :]) * col[:, 2 + e:3 + e]
            total = t if total is None else total + t
        return total

    arrive = barrier(devs)
    p_d[...] = partial(diag)
    arrive()
    depth = 4 if last else CCH
    mids, fars, ys = [], [], []
    for c in range(CCH):
        r = pl.ds(c * ch, ch)
        cp = rcopy(p_d.at[r], mid.at[r], s_m.at[c], r_m.at[c], devs[0])
        cp.start()
        mids.append(cp)
    p_x[...] = partial(xp)

    def send(c):
        r = pl.ds(c * ch, ch)
        mids[c].wait_recv()
        p_x[r, :] = p_x[r, :] + mid[r, :]
        if c >= depth:
            fars[c - depth].wait_send()
        cp = rcopy(p_x.at[r], far.at[r], s_f.at[c], r_f.at[c], devs[1])
        cp.start()
        fars.append(cp)

    def receive(c):
        r = pl.ds(c * ch, ch)
        fars[c].wait_recv()
        res = (p_me[r, :] + far[r, :]).astype(BF16)
        if last:
            o = pl.ds(pl.multiple_of(pool * n + c * ch, ch), ch)
            out_ref[o, :] = res
            cp = rcopy(out_ref.at[o], out_ref.at[o], s_y.at[c], r_y.at[c], devs[2])
            cp.start()
            ys.append(cp)
        else:
            out_ref[r, :] = res
            if c % (CCH // 2) == CCH // 2 - 1:
                r2 = pl.ds(c * ch + ch - n // 2, n // 2)
                h = rms_bf16(out_ref[r2, :].astype(F32))
                project(h, cos_ref[r2, :], sin_ref[r2, :], wq, wk, wv, qs, kn, vn, r2)

    for c in range(depth):
        send(c)
    p_p[...] = partial(part)
    own_cp = rcopy(p_p, own, s_o, r_o, devs[0])
    own_cp.start()
    p_me[...] = partial(me)
    own_cp.wait()
    p_me[...] = a_ref[...].astype(F32) + (p_me[...] + own[...])
    if not last:
        for c in w_copies:
            c.wait()
    for c in range(depth, CCH):
        send(c)
        receive(c - depth)
    for c in range(CCH - depth, CCH):
        receive(c)
    for c in range(CCH):
        mids[c].wait_send()
    for c in range(CCH - depth, CCH):
        fars[c].wait_send()
    for cp in ys:
        cp.wait()


def combine(layer, last, y, mcol, a, nxt=None):
    n, model = a.shape
    dma = pltpu.SemaphoreType.DMA
    sems = [dma, dma, dma((CCH,)), dma((CCH,)), dma((CCH,)), dma((CCH,))]
    args = [y, mcol, a]
    specs = [vspec()] * 3
    scratch = [VMEM((n, model), F32) for _ in range(7)]
    if last:
        sems += [dma((CCH,)), dma((CCH,))]
        out_shape = jax.ShapeDtypeStruct((2 * n, model), BF16)
        out_specs = vspec()
    else:
        cos, sin, wq, wk, wv = nxt
        args += [cos, sin, wq, wk, wv]
        specs += [vspec()] * 2 + [anyspec()] * 3
        sems += [dma((3,))]
        scratch += [VMEM(w.shape[1:], BF16) for w in (wq, wk, wv)]
        out_shape = [jax.ShapeDtypeStruct((n, model), BF16)] + [jax.ShapeDtypeStruct((n, w.shape[2]), BF16) for w in (wq, wk, wv)]
        out_specs = [vspec()] * 4
    return pl.pallas_call(
        functools.partial(combine_kernel, last, layer),
        out_shape=out_shape,
        in_specs=specs,
        out_specs=out_specs,
        scratch_shapes=scratch + sems,
        compiler_params=pltpu.CompilerParams(collective_id=2 * layer + 1, has_side_effects=True, vmem_limit_bytes=LIM_C),
        name=f"combine{layer}",
    )(*args)


def solution(mesh):
    def body(hidden, k_cache, v_cache, lengths, expert_ids, w_query, w_key, w_value, w_out, w_router, w_gate, w_up, w_down):
        n_layers, _, seq, kvh, hd = k_cache.shape
        n_tok = hidden.shape[0] // 2
        kc = k_cache.reshape(n_layers, -1, seq * kvh, hd)
        vc = v_cache.reshape(n_layers, -1, seq * kvh, hd)
        ids = expert_ids.transpose(0, 2, 1)
        wr = w_router.transpose(0, 2, 1)
        tab = jnp.asarray(rope_table(seq, hd))
        w_query, w_key, w_value, w_out, w_gate, w_up, w_down, kc, vc, tab, hidden_h, lens_h = (
            pltpu.with_memory_space_constraint(v, pltpu.HBM) for v in (w_query, w_key, w_value, w_out, w_gate, w_up, w_down, kc, vc, tab, hidden, lengths))
        state = hidden
        qkv = None
        for layer in range(n_layers):
            last = layer == n_layers - 1
            if layer == 0:
                att, wo, cos, sin = attention(layer, n_tok, lens_h, w_out, kc, vc, proj=(hidden_h, tab, w_query, w_key, w_value))
            else:
                att, wo = attention(layer, n_tok, lengths, w_out, kc, vc, qkv=qkv)
            outs = dispatch(layer, att, state, ids, wr, wo, w_gate, w_up, w_down)
            a, u_all, rrow, mcol = outs[:4]
            if layer == 0:
                ids = outs[4]
            y = experts(layer, u_all, rrow, mcol, outs[-3:], w_gate, w_up, w_down)
            if last:
                return combine(layer, True, y, mcol, a)
            state, *qkv = combine(layer, False, y, mcol, a, nxt=(cos, sin, w_query, w_key, w_value))

    rows_spec = ("dp", "ep")
    in_specs = (P(rows_spec, None), P(None, rows_spec), P(None, rows_spec), P(rows_spec), P(None, rows_spec, None), P(), P(), P(), P(), P(), P(None, "ep"), P(None, "ep"), P(None, "ep"))
    return jax.shard_map(body, mesh=mesh, in_specs=in_specs, out_specs=P(rows_spec, None), check_vma=False)
```

```python
import functools

import numpy as np

import jax
import jax.numpy as jnp
from jax import lax
from jax.experimental import pallas as pl
from jax.experimental.pallas import tpu as pltpu
from jax.sharding import PartitionSpec as P

MESH = pl.DeviceIdType.MESH
EPSILON = 1e-6
ROPE_BASE = 10000.0
VMEM = pltpu.VMEM
F32 = jnp.float32
BF16 = jnp.bfloat16

TOKG = 16
TILE = 1024
FT = 512
NSLOT = 3
CCH = 8
LIM_A = 50 * 1024 * 1024
LIM_B = 50 * 1024 * 1024
LIM_D = 8 * 1024 * 1024
LIM_E = 27 * 1024 * 1024
LIM_C = 16 * 1024 * 1024
SIZES = (128, 400, 512)


def vspec():
    return pl.BlockSpec(memory_space=VMEM)


def anyspec():
    return pl.BlockSpec(memory_space=pltpu.HBM)


def sspec():
    return pl.BlockSpec(memory_space=pltpu.SMEM)


def dot(a, b):
    return jnp.dot(a, b, preferred_element_type=F32)


def rms_bf16(v):
    return (v * lax.rsqrt(jnp.mean(v * v, axis=-1, keepdims=True) + EPSILON)).astype(BF16)


def rope_table(seq, hd):
    half = hd // 2
    freqs = np.power(np.float32(ROPE_BASE), (np.float32(-2.0) * np.arange(half, dtype=np.float32) / np.float32(hd)))
    angle = np.arange(seq + 1, dtype=np.float32)[:, None] * freqs.astype(np.float32)[None, :]
    wide = angle.astype(np.float64)
    return np.concatenate([np.cos(wide), np.sin(wide)], axis=1).astype(np.float32)


def rope(vec, cos, sin):
    return vec * cos + pltpu.roll(vec, 64, 1) * sin


def project(h, cos, sin, wq, wk, wv, qs, kn, vn, rows):
    q = dot(h, wq[...])
    k = dot(h, wk[...])
    v = dot(h, wv[...])
    for j in range(q.shape[1] // 128):
        qs[rows, j * 128:(j + 1) * 128] = rope(q[:, j * 128:(j + 1) * 128], cos, sin).astype(BF16)
    for j in range(k.shape[1] // 128):
        kn[rows, j * 128:(j + 1) * 128] = rope(k[:, j * 128:(j + 1) * 128], cos, sin).astype(BF16)
    vn[rows, :] = v.astype(BF16)


def attn_kernel(layer, n_tok, first_layer, lens_in, *refs):
    if first_layer:
        (x_hbm, tab_hbm, wq_hbm, wk_hbm, wv_hbm, wo_hbm, kc, vc, os_, wo, cos_ref, sin_ref,
         x_ref, tab_ref, wq, wk, wv, qs, kn, vn, wsem, kbuf, vbuf, sbuf, mst, men, lens_ref, lsem, ksem, vsem, osem) = refs
    else:
        qs, kn, vn, wo_hbm, kc, vc, os_, wo, kbuf, vbuf, sbuf, mst, men, ksem, vsem, osem = refs
        lens_ref = lens_in
    t0 = lax.axis_index("pool") * n_tok
    if first_layer:
        lens_cp = pltpu.make_async_copy(lens_in, lens_ref, lsem)
        lens_cp.start()
    heads = qs.shape[1] // 128
    n_groups = n_tok // TOKG
    hpk = heads // 2
    cols = heads * TOKG

    def padded(ln):
        return pl.multiple_of(lax.shift_left(lax.shift_right_logical(ln + 7, 3), 4), 16)

    def start_group(g):
        slot = lax.rem(g, NSLOT)
        off = 0
        for i in range(TOKG):
            tok = t0 + g * TOKG + i
            ln = lens_ref[tok]
            n = padded(ln)
            off = pl.multiple_of(off, 16)
            pltpu.make_async_copy(kc.at[layer, tok, pl.ds(0, n), :], kbuf.at[slot, pl.ds(off, n), :], ksem.at[slot]).start()
            pltpu.make_async_copy(vc.at[layer, tok, pl.ds(0, n), :], vbuf.at[slot, pl.ds(off, n), :], vsem.at[slot]).start()
            mst[slot, i:i + 1, :] = jnp.full((1, 128), off, jnp.int32)
            men[slot, i:i + 1, :] = jnp.full((1, 128), off + 2 * ln, jnp.int32)
            off = off + n
        return jnp.asarray(off, jnp.int32)

    if first_layer:
        w_copies = [pltpu.make_async_copy(src.at[layer], dst, wsem.at[i])
                    for i, (src, dst) in enumerate(((wq_hbm, wq), (wk_hbm, wk), (wv_hbm, wv)))]
        x_cp = pltpu.make_async_copy(x_hbm.at[pl.ds(pl.multiple_of(t0, n_tok), n_tok), :], x_ref, wsem.at[3])
        tab_cp = pltpu.make_async_copy(tab_hbm, tab_ref, wsem.at[4])
        x_cp.start()
        tab_cp.start()
        for c in w_copies:
            c.start()
    if first_layer:
        lens_cp.wait()
    totals0 = tuple(start_group(jnp.int32(g)) for g in range(NSLOT - 1))
    wo_cp = pltpu.make_async_copy(wo_hbm.at[layer], wo, osem)
    wo_cp.start()
    if first_layer:
        x_cp.wait()
        tab_cp.wait()
        h = rms_bf16(x_ref[...].astype(F32))

        def pick(i, _):
            cos_ref[pl.ds(i, 1), :] = tab_ref[pl.ds(lens_ref[t0 + i], 1), :]
            return 0
        lax.fori_loop(0, n_tok, pick, 0, unroll=8)
        both = cos_ref[...]
        swapped = pltpu.roll(both, 64, 1)
        low = lax.broadcasted_iota(jnp.int32, both.shape, 1) < 64
        cos = jnp.where(low, both, swapped)
        sin = jnp.where(low, -swapped, both)
        cos_ref[...] = cos
        sin_ref[...] = sin
        for c in w_copies:
            c.wait()
        project(h, cos, sin, wq, wk, wv, qs, kn, vn, pl.ds(0, n_tok))
    scale = 128.0 ** -0.5 * 1.4426950408889634

    lane = lax.broadcasted_iota(jnp.int32, (cols, 128), 1)
    kv = (lax.broadcasted_iota(jnp.int32, (cols, 128), 0) >= (hpk * TOKG)).astype(jnp.int32)
    mine = (lane & 1) == kv

    def heads_of(ref, g):
        row = ref[pl.ds(pl.multiple_of(g * TOKG, TOKG), TOKG), :]
        per = heads // (ref.shape[1] // 128)
        return jnp.concatenate([row[:, (j // per) * 128:(j // per + 1) * 128] for j in range(heads)], axis=0)

    def step(g, totals):
        total = pl.multiple_of(totals[0], 16)
        slot = lax.rem(g, NSLOT)
        last = lax.cond(g + NSLOT - 1 < n_groups, lambda: start_group(g + NSLOT - 1), lambda: jnp.int32(0))
        q2 = heads_of(qs, g)
        s_new = jnp.sum(q2.astype(F32) * heads_of(kn, g).astype(F32), axis=1, keepdims=True)
        start = jnp.where(mine, jnp.concatenate([mst[slot]] * heads, axis=0) - lane, 1 << 30)
        end = jnp.concatenate([men[slot]] * heads, axis=0) - lane
        n = lax.shift_right_logical(total + TILE // 2 - 1, TILE.bit_length() - 1)
        m = n + jnp.where(total > n * TILE, 1, 0)
        vbuf[slot, pl.ds(total, TILE), :] = jnp.zeros((TILE, 128), BF16)
        pltpu.make_async_copy(kbuf.at[slot, pl.ds(0, total), :], kbuf.at[slot, pl.ds(0, total), :], ksem.at[slot]).wait()

        def first(i, macc, rows=TILE):
            base = pl.multiple_of(i * TILE, TILE)
            for j in range(rows // 256):
                at = pl.multiple_of(base + j * 256, 256)
                s = lax.dot_general(q2, kbuf[slot, pl.ds(at, 256), :], (((1,), (1,)), ((), ())), preferred_element_type=F32)
                for p in range(2):
                    off = at + p * 128
                    part = jnp.where((start <= off) & (end > off), s[:, p * 128:(p + 1) * 128], -jnp.inf)
                    sbuf[:, pl.ds(pl.multiple_of(off, 128), 128)] = part
                    macc = jnp.maximum(macc, part)
            return macc

        macc = lax.fori_loop(0, n, first, jnp.full((cols, 128), -jnp.inf, F32))
        macc = lax.fori_loop(n, m, functools.partial(first, rows=TILE // 2), macc)
        peak = jnp.maximum(jnp.max(macc, axis=1, keepdims=True), s_new)
        w_new = jnp.exp2((s_new - peak) * scale)
        peakb = jnp.broadcast_to(peak, (cols, 128))
        pltpu.make_async_copy(vbuf.at[slot, pl.ds(0, total), :], vbuf.at[slot, pl.ds(0, total), :], vsem.at[slot]).wait()

        def second(i, carry, rows=TILE):
            lacc, acc = carry
            base = pl.multiple_of(i * TILE, TILE)
            parts = []
            for j in range(rows // 128):
                p = jnp.exp2((sbuf[:, pl.ds(pl.multiple_of(base + j * 128, 128), 128)] - peakb) * scale)
                lacc = lacc + p
                parts.append(p.astype(BF16))
                if len(parts) == 4:
                    at = pl.multiple_of(base + (j - 3) * 128, 512)
                    acc = acc + dot(jnp.concatenate(parts, axis=1), vbuf[slot, pl.ds(at, 512), :])
                    parts = []
            return lacc, acc

        zero = jnp.zeros((cols, 128), F32)
        lacc, acc = lax.fori_loop(0, n, second, (zero, zero))
        lacc, acc = lax.fori_loop(n, m, functools.partial(second, rows=TILE // 2), (lacc, acc))
        den = jnp.sum(lacc, axis=1, keepdims=True) + w_new
        o = ((acc + w_new.astype(BF16).astype(F32) * heads_of(vn, g).astype(F32)) / den).astype(BF16)
        g0 = pl.multiple_of(g * TOKG, TOKG)
        for j in range(heads):
            os_[pl.ds(g0, TOKG), j * 128:(j + 1) * 128] = o[j * TOKG:(j + 1) * TOKG, :]
        return totals[1:] + (last,)

    lax.fori_loop(0, n_groups, step, totals0)
    wo_cp.wait()


def attention(layer, n_tok, lens, w_out, kc, vc, proj=None, qkv=None):
    dma = pltpu.SemaphoreType.DMA
    first_layer = proj is not None
    out_shape = []
    if first_layer:
        x, tab, wq, wk, wv = proj
        model, qdim, kvdim = wq.shape[1], wq.shape[2], wk.shape[2]
        args = [lens, x, tab, wq, wk, wv, w_out, kc, vc]
        specs = [anyspec()] * 9
        out_shape = [VMEM((n_tok, qdim), BF16), VMEM(w_out.shape[1:], BF16)] + [jax.ShapeDtypeStruct((n_tok, 128), F32)] * 2
        scratch = [VMEM((n_tok, model), BF16), VMEM(tab.shape, F32), VMEM((model, qdim), BF16), VMEM((model, kvdim), BF16), VMEM((model, kvdim), BF16),
                   VMEM((n_tok, qdim), BF16), VMEM((n_tok, kvdim), BF16), VMEM((n_tok, kvdim), BF16), dma((5,))]
    else:
        qdim = qkv[0].shape[1]
        args = [lens, *qkv, w_out, kc, vc]
        specs = [sspec()] + [vspec()] * 3 + [anyspec()] * 3
        out_shape = [VMEM((n_tok, qdim), BF16), VMEM(w_out.shape[1:], BF16)]
        scratch = []
    max_rows = TOKG * kc.shape[2]
    cols = (qdim // 128) * TOKG
    scratch += [VMEM((NSLOT, max_rows + TILE, 128), BF16), VMEM((NSLOT, max_rows + TILE, 128), BF16), VMEM((cols, max_rows), F32),
                VMEM((NSLOT, TOKG, 128), jnp.int32), VMEM((NSLOT, TOKG, 128), jnp.int32), *([pltpu.SMEM(lens.shape, jnp.int32), dma] if first_layer else []), dma((NSLOT,)), dma((NSLOT,)), dma]
    return pl.pallas_call(
        functools.partial(attn_kernel, layer, n_tok, first_layer),
        out_shape=out_shape,
        in_specs=specs,
        out_specs=[vspec()] * len(out_shape),
        scratch_shapes=scratch,
        compiler_params=pltpu.CompilerParams(vmem_limit_bytes=LIM_A if first_layer else LIM_B),
        name=f"attention{layer}",
    )(*args)


NCH = 4


def peers():
    me = lax.axis_index("ep")
    core = me % 2
    x = me // 2
    return me, x * 2 + (1 - core), (1 - x) * 2 + core, (1 - x) * 2 + (1 - core)


def barrier(devices):
    sem = pltpu.get_barrier_semaphore()
    for d in devices:
        pl.semaphore_signal(sem, inc=1, device_id=d, device_id_type=MESH)
    return lambda: pl.semaphore_wait(sem, len(devices))


def rcopy(src, dst, ssem, rsem, dev):
    return pltpu.make_async_remote_copy(src_ref=src, dst_ref=dst, send_sem=ssem, recv_sem=rsem, device_id=dev, device_id_type=MESH)


def weight_copies(layer, e, f, slot, hbm, buf, sems):
    wg_hbm, wu_hbm, wd_hbm = hbm
    cols = pl.ds(f * FT, FT) if isinstance(f, int) else pl.ds(pl.multiple_of(f * FT, FT), FT)
    return (pltpu.make_async_copy(wg_hbm.at[layer, e, :, cols], buf[0].at[slot], sems.at[slot, 0]),
            pltpu.make_async_copy(wu_hbm.at[layer, e, :, cols], buf[1].at[slot], sems.at[slot, 1]),
            pltpu.make_async_copy(wd_hbm.at[layer, e, cols, :], buf[2].at[slot], sems.at[slot, 2]))


def dispatch_kernel(layer, steps, n_loc, os_ref, x_ref, ids_ref, wr_ref, wo, wg_hbm, wu_hbm, wd_hbm, *refs):
    first_layer = layer == 0
    if first_layer:
        a_ref, uall, rrow, mcol, idsall, pg, pu, pd, idsbuf, *sems = refs
        psem, s_p, r_p, s_x, r_x, s_f, r_f, s_i, r_i = sems
    else:
        a_ref, uall, rrow, mcol, pg, pu, pd, *sems = refs
        psem, s_p, r_p, s_x, r_x, s_f, r_f = sems
        idsall = ids_ref
    n = os_ref.shape[0]
    ch = n // NCH
    pool = lax.axis_index("pool")
    me, part, xp, diag = peers()
    devs = [{"ep": part}, {"ep": xp}]
    arrive = barrier(devs)

    def rows(ep, c):
        return pl.ds(pl.multiple_of(ep * n + c * ch, ch), ch)

    ics = []
    if first_layer:
        t0 = pl.multiple_of(pool * n, n)
        idsbuf[...] = jnp.zeros(idsbuf.shape, jnp.int32)
        for l in range(ids_ref.shape[0]):
            idsbuf[2 * l:2 * l + 2, :] = ids_ref[l, :, pl.ds(t0, n)]
        idsall[me] = idsbuf[...]
    xs, ps = [], []
    half = n // 2
    for hf in range(2):
        r = pl.ds(hf * half, half)
        if first_layer:
            xr = x_ref[pl.ds(pl.multiple_of(pool * n + hf * half, half), half), :]
        else:
            xr = x_ref[r, :]
        a = (xr.astype(F32) + dot(os_ref[r, :], wo[...])).astype(BF16)
        a_ref[r, :] = a
        uall[pl.ds(pl.multiple_of(me * n + hf * half, half), half), :] = rms_bf16(a.astype(F32))
        if hf == 0:
            arrive()
            if first_layer:
                for i, d in enumerate(devs):
                    cp = rcopy(idsbuf, idsall.at[me], s_i.at[i], r_i.at[i], d)
                    cp.start()
                    ics.append(cp)
        for c in range(hf * NCH // 2, (hf + 1) * NCH // 2):
            cp = rcopy(uall.at[rows(me, c)], uall.at[rows(me, c)], s_x.at[c], r_x.at[c], {"ep": xp})
            cp.start()
            xs.append(cp)
            cp = rcopy(uall.at[rows(me, c)], uall.at[rows(me, c)], s_p.at[c], r_p.at[c], {"ep": part})
            cp.start()
            ps.append(cp)
    hbm = (wg_hbm, wu_hbm, wd_hbm)

    def prefetch(f, _):
        for cp in weight_copies(layer, 0, f, f, hbm, (pg, pu, pd), psem):
            cp.start()
        return 0

    lax.fori_loop(0, steps, prefetch, 0)
    if first_layer:
        ics[1].wait_recv()
        cp = rcopy(idsall.at[xp], idsall.at[xp], s_i.at[2], r_i.at[2], devs[0])
        cp.start()
        cp.wait()
        ics[0].wait()
        ics[1].wait_send()

    tokens = 4 * n
    e0 = me * n_loc
    ids_row = [jnp.concatenate([idsall[b, 2 * layer + k:2 * layer + k + 1, :] for b in range(4)], axis=1) for k in range(2)]
    row8 = lax.broadcasted_iota(jnp.int32, (8, tokens), 0)
    hit = ((ids_row[0] == row8 + e0) | (ids_row[1] == row8 + e0)) & (row8 < n_loc)
    hit_f = hit.astype(F32)
    tri = (lax.broadcasted_iota(jnp.int32, (tokens, tokens), 0) < lax.broadcasted_iota(jnp.int32, (tokens, tokens), 1)).astype(F32).astype(BF16)
    rank = jnp.where(hit_f > 0, dot(hit_f.astype(BF16), tri), -1.0)
    rrow[...] = rank
    idf = jnp.where(row8 == 2, jnp.broadcast_to(ids_row[0].astype(F32), (8, tokens)),
                    jnp.where(row8 == 3, jnp.broadcast_to(ids_row[1].astype(F32), (8, tokens)), rank))
    mcol[...] = jnp.transpose(idf)

    w = wr_ref[layer]
    w1 = w.astype(BF16).astype(F32)
    w2 = (w - w1).astype(BF16).astype(F32)
    w3 = w - w1 - w2
    wr = jnp.concatenate([w1, w2, w3, jnp.zeros((104, w.shape[1]), F32)], axis=0).astype(BF16)
    e0f = e0.astype(F32)

    def gates(ep):
        r = pl.ds(pl.multiple_of(ep * n, n), n)
        lg = lax.dot_general(uall[r, :], wr, (((1,), (1,)), ((), ())), preferred_element_type=F32)
        lg = lg + pltpu.roll(lg, 120, 1) + pltpu.roll(lg, 112, 1)
        lane = lax.broadcasted_iota(jnp.int32, (n, 128), 1).astype(F32)
        col = mcol[r, :]
        id0, id1 = col[:, 2:3], col[:, 3:4]
        l0 = jnp.sum(jnp.where(lane == id0, lg, 0.0), axis=1, keepdims=True)
        l1 = jnp.sum(jnp.where(lane == id1, lg, 0.0), axis=1, keepdims=True)
        top = jnp.maximum(l0, l1)
        x0 = jnp.exp(l0 - top)
        x1 = jnp.exp(l1 - top)
        den = x0 + x1
        lane8 = lax.broadcasted_iota(jnp.int32, (n, 8), 1)
        expert = (lane8 - 2).astype(F32) + e0f
        g = jnp.where(id0 == expert, x0 / den, 0.0) + jnp.where(id1 == expert, x1 / den, 0.0)
        mcol[r, :] = jnp.where(lane8 < 2, col, g)

    gates(me)
    fs = []

    def forward(c):
        xs[c].wait_recv()
        cp = rcopy(uall.at[rows(xp, c)], uall.at[rows(xp, c)], s_f.at[c], r_f.at[c], {"ep": part})
        cp.start()
        fs.append(cp)

    for c in range(NCH - 1):
        forward(c)
    for cp in ps:
        cp.wait()
    gates(part)
    forward(NCH - 1)
    gates(xp)
    for cp in fs:
        cp.wait()
    gates(diag)
    for cp in xs:
        cp.wait_send()
    for f in range(steps):
        for cp in weight_copies(layer, 0, f, f, hbm, (pg, pu, pd), psem):
            cp.wait()


def dispatch(layer, os_, x, ids, wr, wo, wg, wu, wd):
    n, qdim = os_.shape
    model = wo.shape[1]
    n_loc, ff = wg.shape[1], wg.shape[3]
    steps = ff // FT
    dma = pltpu.SemaphoreType.DMA
    out_shape = [jax.ShapeDtypeStruct((n, model), BF16), jax.ShapeDtypeStruct((4 * n, model), BF16),
                 jax.ShapeDtypeStruct((8, 4 * n), F32), jax.ShapeDtypeStruct((4 * n, 8), F32)]
    scratch = []
    sems = [dma((steps, 3))] + [dma((NCH,))] * 6
    if layer == 0:
        out_shape.append(jax.ShapeDtypeStruct((4, 8, n), jnp.int32))
        scratch.append(VMEM((8, n), jnp.int32))
        sems += [dma((3,)), dma((3,))]
    n_small = len(out_shape)
    out_shape += [VMEM((steps, model, FT), BF16), VMEM((steps, model, FT), BF16), VMEM((steps, FT, model), BF16)]
    return pl.pallas_call(
        functools.partial(dispatch_kernel, layer, steps, n_loc),
        out_shape=out_shape,
        in_specs=[vspec()] * 5 + [anyspec()] * 3,
        out_specs=[vspec()] * n_small + [vspec()] * 3,
        scratch_shapes=scratch + sems,
        compiler_params=pltpu.CompilerParams(collective_id=2 * layer, has_side_effects=True, vmem_limit_bytes=LIM_D),
        name=f"dispatch{layer}",
    )(os_, x, ids, wr, wo, wg, wu, wd)


def expert_kernel(layer, u_ref, rrow_ref, mcol_ref, pg, pu, pd, wg_hbm, wu_hbm, wd_hbm, y_ref, wg, wu, wd, xe, yacc, sems):
    n = u_ref.shape[0]
    steps = pg.shape[0]
    n_loc = wg_hbm.shape[1]
    hbm = (wg_hbm, wu_hbm, wd_hbm)
    own = (wg, wu, wd)

    for e in range(1, n_loc):
        def issue(f, _, e=e):
            for c in weight_copies(layer, e, f, (e - 1) * steps + f, hbm, own, sems):
                c.start()
            return 0
        lax.fori_loop(0, steps, issue, 0)

    for e in range(n_loc):
        rank_row = rrow_ref[e:e + 1, :]
        count = jnp.sum((rank_row >= 0).astype(F32)).astype(jnp.int32)
        lo = 0
        for m in SIZES:
            @pl.when((count <= m) & ((count > lo) | (lo == 0)))
            def _(m=m, e=e):
                sel = (rank_row == lax.broadcasted_iota(jnp.int32, (m, n), 0).astype(F32)).astype(F32).astype(BF16)
                xe[pl.ds(0, m), :] = dot(sel, u_ref[...]).astype(BF16)
                yacc[pl.ds(0, m), :] = jnp.zeros((m, yacc.shape[1]), F32)

                def step(f, _):
                    if e == 0:
                        w1, w3, w2 = pg, pu, pd
                        slot = f
                    else:
                        w1, w3, w2 = own
                        slot = (e - 1) * steps + f
                        for c in weight_copies(layer, e, f, slot, hbm, own, sems):
                            c.wait()
                    inner = []
                    for j in range(FT // 256):
                        at = pl.ds(j * 256, 256)
                        gate = dot(xe[pl.ds(0, m), :], w1[slot, :, at])
                        up = dot(xe[pl.ds(0, m), :], w3[slot, :, at])
                        inner.append((gate * jax.nn.sigmoid(gate) * up).astype(BF16))
                    inner = jnp.concatenate(inner, axis=1)
                    half = yacc.shape[1] // 2
                    for j in range(2):
                        at = pl.ds(j * half, half)
                        yacc[pl.ds(0, m), at] += dot(inner, w2[slot, :, at])
                    return 0

                lax.fori_loop(0, steps, step, 0)
                y_ref[pl.ds(e * n, m), :] = yacc[pl.ds(0, m), :].astype(BF16)
                if m < n:
                    y_ref[pl.ds(e * n + m, n - m), :] = jnp.zeros((n - m, y_ref.shape[1]), BF16)
            lo = m


def experts(layer, u_all, rrow, mcol, pre, wg, wu, wd):
    n, model = u_all.shape
    steps = pre[0].shape[0]
    n_loc = wg.shape[1]
    slots = steps * (n_loc - 1)
    return pl.pallas_call(
        functools.partial(expert_kernel, layer),
        out_shape=jax.ShapeDtypeStruct((n_loc * n, model), BF16),
        in_specs=[vspec()] * 6 + [anyspec()] * 3,
        out_specs=vspec(),
        scratch_shapes=[VMEM((slots, model, FT), BF16), VMEM((slots, model, FT), BF16), VMEM((slots, FT, model), BF16),
                        VMEM((n, model), BF16), VMEM((n, model), F32), pltpu.SemaphoreType.DMA((slots, 3))],
        compiler_params=pltpu.CompilerParams(vmem_limit_bytes=LIM_E),
        name=f"experts{layer}",
    )(u_all, rrow, mcol, *pre, wg, wu, wd)


def combine_kernel(last, layer, y_ref, mcol_ref, a_ref, *refs):
    if last:
        out_ref, p_d, p_x, p_p, p_me, own, mid, far, *sems = refs
        s_o, r_o, s_m, r_m, s_f, r_f, s_y, r_y = sems
    else:
        (cos_ref, sin_ref, wq_hbm, wk_hbm, wv_hbm, out_ref, qs, kn, vn,
         p_d, p_x, p_p, p_me, own, mid, far, wq, wk, wv, *sems) = refs
        s_o, r_o, s_m, r_m, s_f, r_f, wsem = sems
    n = a_ref.shape[0]
    ch = n // CCH
    nn = mcol_ref.shape[0]
    me, part, xp, diag = peers()
    devs = [{"ep": part}, {"ep": xp}]
    if last:
        pool = lax.axis_index("pool")
        devs.append({"pool": 1 - pool})
    else:
        w_copies = [pltpu.make_async_copy(src.at[layer + 1], dst, wsem.at[i])
                    for i, (src, dst) in enumerate(((wq_hbm, wq), (wk_hbm, wk), (wv_hbm, wv)))]
        for c in w_copies:
            c.start()

    def partial(ep):
        col = mcol_ref[pl.ds(pl.multiple_of(ep * n, n), n), :]
        slot = lax.broadcasted_iota(jnp.int32, (n, nn), 1).astype(F32)
        total = None
        for e in range(y_ref.shape[0] // nn):
            sel = (col[:, e:e + 1] == slot).astype(F32).astype(BF16)
            t = dot(sel, y_ref[e * nn:(e + 1) * nn, :]) * col[:, 2 + e:3 + e]
            total = t if total is None else total + t
        return total

    arrive = barrier(devs)
    p_d[...] = partial(diag)
    arrive()
    depth = 4 if last else CCH
    mids, fars, ys = [], [], []
    for c in range(CCH):
        r = pl.ds(c * ch, ch)
        cp = rcopy(p_d.at[r], mid.at[r], s_m.at[c], r_m.at[c], devs[0])
        cp.start()
        mids.append(cp)
    p_x[...] = partial(xp)

    def send(c):
        r = pl.ds(c * ch, ch)
        mids[c].wait_recv()
        p_x[r, :] = p_x[r, :] + mid[r, :]
        if c >= depth:
            fars[c - depth].wait_send()
        cp = rcopy(p_x.at[r], far.at[r], s_f.at[c], r_f.at[c], devs[1])
        cp.start()
        fars.append(cp)

    def receive(c):
        r = pl.ds(c * ch, ch)
        fars[c].wait_recv()
        res = (p_me[r, :] + far[r, :]).astype(BF16)
        if last:
            o = pl.ds(pl.multiple_of(pool * n + c * ch, ch), ch)
            out_ref[o, :] = res
            cp = rcopy(out_ref.at[o], out_ref.at[o], s_y.at[c], r_y.at[c], devs[2])
            cp.start()
            ys.append(cp)
        else:
            out_ref[r, :] = res
            if c % (CCH // 2) == CCH // 2 - 1:
                r2 = pl.ds(c * ch + ch - n // 2, n // 2)
                h = rms_bf16(out_ref[r2, :].astype(F32))
                project(h, cos_ref[r2, :], sin_ref[r2, :], wq, wk, wv, qs, kn, vn, r2)

    for c in range(depth):
        send(c)
    p_p[...] = partial(part)
    own_cp = rcopy(p_p, own, s_o, r_o, devs[0])
    own_cp.start()
    p_me[...] = partial(me)
    own_cp.wait()
    p_me[...] = a_ref[...].astype(F32) + (p_me[...] + own[...])
    if not last:
        for c in w_copies:
            c.wait()
    for c in range(depth, CCH):
        send(c)
        receive(c - depth)
    for c in range(CCH - depth, CCH):
        receive(c)
    for c in range(CCH):
        mids[c].wait_send()
    for c in range(CCH - depth, CCH):
        fars[c].wait_send()
    for cp in ys:
        cp.wait()


def combine(layer, last, y, mcol, a, nxt=None):
    n, model = a.shape
    dma = pltpu.SemaphoreType.DMA
    sems = [dma, dma, dma((CCH,)), dma((CCH,)), dma((CCH,)), dma((CCH,))]
    args = [y, mcol, a]
    specs = [vspec()] * 3
    scratch = [VMEM((n, model), F32) for _ in range(7)]
    if last:
        sems += [dma((CCH,)), dma((CCH,))]
        out_shape = jax.ShapeDtypeStruct((2 * n, model), BF16)
        out_specs = vspec()
    else:
        cos, sin, wq, wk, wv = nxt
        args += [cos, sin, wq, wk, wv]
        specs += [vspec()] * 2 + [anyspec()] * 3
        sems += [dma((3,))]
        scratch += [VMEM(w.shape[1:], BF16) for w in (wq, wk, wv)]
        out_shape = [jax.ShapeDtypeStruct((n, model), BF16)] + [jax.ShapeDtypeStruct((n, w.shape[2]), BF16) for w in (wq, wk, wv)]
        out_specs = [vspec()] * 4
    return pl.pallas_call(
        functools.partial(combine_kernel, last, layer),
        out_shape=out_shape,
        in_specs=specs,
        out_specs=out_specs,
        scratch_shapes=scratch + sems,
        compiler_params=pltpu.CompilerParams(collective_id=2 * layer + 1, has_side_effects=True, vmem_limit_bytes=LIM_C),
        name=f"combine{layer}",
    )(*args)


def solution(mesh):
    def body(hidden, k_cache, v_cache, lengths, expert_ids, w_query, w_key, w_value, w_out, w_router, w_gate, w_up, w_down):
        n_layers, _, seq, kvh, hd = k_cache.shape
        n_tok = hidden.shape[0] // 2
        kc = k_cache.reshape(n_layers, -1, seq * kvh, hd)
        vc = v_cache.reshape(n_layers, -1, seq * kvh, hd)
        ids = expert_ids.transpose(0, 2, 1)
        wr = w_router.transpose(0, 2, 1)
        tab = jnp.asarray(rope_table(seq, hd))
        w_query, w_key, w_value, w_out, w_gate, w_up, w_down, kc, vc, tab, hidden_h, lens_h = (
            pltpu.with_memory_space_constraint(v, pltpu.HBM) for v in (w_query, w_key, w_value, w_out, w_gate, w_up, w_down, kc, vc, tab, hidden, lengths))
        state = hidden
        qkv = None
        for layer in range(n_layers):
            last = layer == n_layers - 1
            if layer == 0:
                att, wo, cos, sin = attention(layer, n_tok, lens_h, w_out, kc, vc, proj=(hidden_h, tab, w_query, w_key, w_value))
            else:
                att, wo = attention(layer, n_tok, lengths, w_out, kc, vc, qkv=qkv)
            outs = dispatch(layer, att, state, ids, wr, wo, w_gate, w_up, w_down)
            a, u_all, rrow, mcol = outs[:4]
            if layer == 0:
                ids = outs[4]
            y = experts(layer, u_all, rrow, mcol, outs[-3:], w_gate, w_up, w_down)
            if last:
                return combine(layer, True, y, mcol, a)
            state, *qkv = combine(layer, False, y, mcol, a, nxt=(cos, sin, w_query, w_key, w_value))

    rows_spec = ("dp", "ep")
    in_specs = (P(rows_spec, None), P(None, rows_spec), P(None, rows_spec), P(rows_spec), P(None, rows_spec, None), P(), P(), P(), P(), P(), P(None, "ep"), P(None, "ep"), P(None, "ep"))
    return jax.shard_map(body, mesh=mesh, in_specs=in_specs, out_specs=P(rows_spec, None), check_vma=False)
```

```python
import functools

import numpy as np

import jax
import jax.numpy as jnp
from jax import lax
from jax.experimental import pallas as pl
from jax.experimental.pallas import tpu as pltpu
from jax.sharding import PartitionSpec as P

MESH = pl.DeviceIdType.MESH
EPSILON = 1e-6
ROPE_BASE = 10000.0
VMEM = pltpu.VMEM
F32 = jnp.float32
BF16 = jnp.bfloat16

TOKG = 16
TILE = 1024
FT = 512
NSLOT = 3
CCH = 8
LIM_A = 50 * 1024 * 1024
LIM_B = 50 * 1024 * 1024
LIM_D = 8 * 1024 * 1024
LIM_E = 27 * 1024 * 1024
LIM_C = 16 * 1024 * 1024
SIZES = (64, 112, 400, 512)


def vspec():
    return pl.BlockSpec(memory_space=VMEM)


def anyspec():
    return pl.BlockSpec(memory_space=pltpu.HBM)


def sspec():
    return pl.BlockSpec(memory_space=pltpu.SMEM)


def dot(a, b):
    return jnp.dot(a, b, preferred_element_type=F32)


def rms_bf16(v):
    return (v * lax.rsqrt(jnp.mean(v * v, axis=-1, keepdims=True) + EPSILON)).astype(BF16)


def rope_table(seq, hd):
    half = hd // 2
    freqs = np.power(np.float32(ROPE_BASE), (np.float32(-2.0) * np.arange(half, dtype=np.float32) / np.float32(hd)))
    angle = np.arange(seq + 1, dtype=np.float32)[:, None] * freqs.astype(np.float32)[None, :]
    wide = angle.astype(np.float64)
    return np.concatenate([np.cos(wide), np.sin(wide)], axis=1).astype(np.float32)


def rope(vec, cos, sin):
    return vec * cos + pltpu.roll(vec, 64, 1) * sin


def project(h, cos, sin, wq, wk, wv, qs, kn, vn, rows):
    q = dot(h, wq[...])
    k = dot(h, wk[...])
    v = dot(h, wv[...])
    for j in range(q.shape[1] // 128):
        qs[rows, j * 128:(j + 1) * 128] = rope(q[:, j * 128:(j + 1) * 128], cos, sin).astype(BF16)
    for j in range(k.shape[1] // 128):
        kn[rows, j * 128:(j + 1) * 128] = rope(k[:, j * 128:(j + 1) * 128], cos, sin).astype(BF16)
    vn[rows, :] = v.astype(BF16)


def attn_kernel(layer, n_tok, first_layer, lens_in, *refs):
    if first_layer:
        (x_hbm, tab_hbm, wq_hbm, wk_hbm, wv_hbm, wo_hbm, kc, vc, os_, wo, cos_ref, sin_ref,
         x_ref, tab_ref, wq, wk, wv, qs, kn, vn, wsem, kbuf, vbuf, sbuf, mst, men, lens_ref, lsem, ksem, vsem, osem) = refs
    else:
        qs, kn, vn, wo_hbm, kc, vc, os_, wo, kbuf, vbuf, sbuf, mst, men, ksem, vsem, osem = refs
        lens_ref = lens_in
    t0 = lax.axis_index("pool") * n_tok
    if first_layer:
        lens_cp = pltpu.make_async_copy(lens_in, lens_ref, lsem)
        lens_cp.start()
    heads = qs.shape[1] // 128
    n_groups = n_tok // TOKG
    hpk = heads // 2
    cols = heads * TOKG

    def padded(ln):
        return pl.multiple_of(lax.shift_left(lax.shift_right_logical(ln + 7, 3), 4), 16)

    def start_group(g):
        slot = lax.rem(g, NSLOT)
        off = 0
        for i in range(TOKG):
            tok = t0 + g * TOKG + i
            ln = lens_ref[tok]
            n = padded(ln)
            off = pl.multiple_of(off, 16)
            pltpu.make_async_copy(kc.at[layer, tok, pl.ds(0, n), :], kbuf.at[slot, pl.ds(off, n), :], ksem.at[slot]).start()
            pltpu.make_async_copy(vc.at[layer, tok, pl.ds(0, n), :], vbuf.at[slot, pl.ds(off, n), :], vsem.at[slot]).start()
            mst[slot, i:i + 1, :] = jnp.full((1, 128), off, jnp.int32)
            men[slot, i:i + 1, :] = jnp.full((1, 128), off + 2 * ln, jnp.int32)
            off = off + n
        return jnp.asarray(off, jnp.int32)

    if first_layer:
        w_copies = [pltpu.make_async_copy(src.at[layer], dst, wsem.at[i])
                    for i, (src, dst) in enumerate(((wq_hbm, wq), (wk_hbm, wk), (wv_hbm, wv)))]
        x_cp = pltpu.make_async_copy(x_hbm.at[pl.ds(pl.multiple_of(t0, n_tok), n_tok), :], x_ref, wsem.at[3])
        tab_cp = pltpu.make_async_copy(tab_hbm, tab_ref, wsem.at[4])
        x_cp.start()
        tab_cp.start()
        for c in w_copies:
            c.start()
    if first_layer:
        lens_cp.wait()
    totals0 = tuple(start_group(jnp.int32(g)) for g in range(NSLOT - 1))
    wo_cp = pltpu.make_async_copy(wo_hbm.at[layer], wo, osem)
    wo_cp.start()
    if first_layer:
        x_cp.wait()
        tab_cp.wait()
        h = rms_bf16(x_ref[...].astype(F32))

        def pick(i, _):
            cos_ref[pl.ds(i, 1), :] = tab_ref[pl.ds(lens_ref[t0 + i], 1), :]
            return 0
        lax.fori_loop(0, n_tok, pick, 0, unroll=8)
        both = cos_ref[...]
        swapped = pltpu.roll(both, 64, 1)
        low = lax.broadcasted_iota(jnp.int32, both.shape, 1) < 64
        cos = jnp.where(low, both, swapped)
        sin = jnp.where(low, -swapped, both)
        cos_ref[...] = cos
        sin_ref[...] = sin
        for c in w_copies:
            c.wait()
        project(h, cos, sin, wq, wk, wv, qs, kn, vn, pl.ds(0, n_tok))
    scale = 128.0 ** -0.5 * 1.4426950408889634

    lane = lax.broadcasted_iota(jnp.int32, (cols, 128), 1)
    kv = (lax.broadcasted_iota(jnp.int32, (cols, 128), 0) >= (hpk * TOKG)).astype(jnp.int32)
    mine = (lane & 1) == kv

    def heads_of(ref, g):
        row = ref[pl.ds(pl.multiple_of(g * TOKG, TOKG), TOKG), :]
        per = heads // (ref.shape[1] // 128)
        return jnp.concatenate([row[:, (j // per) * 128:(j // per + 1) * 128] for j in range(heads)], axis=0)

    def step(g, totals):
        total = pl.multiple_of(totals[0], 16)
        slot = lax.rem(g, NSLOT)
        last = lax.cond(g + NSLOT - 1 < n_groups, lambda: start_group(g + NSLOT - 1), lambda: jnp.int32(0))
        q2 = heads_of(qs, g)
        s_new = jnp.sum(q2.astype(F32) * heads_of(kn, g).astype(F32), axis=1, keepdims=True)
        start = jnp.where(mine, jnp.concatenate([mst[slot]] * heads, axis=0) - lane, 1 << 30)
        end = jnp.concatenate([men[slot]] * heads, axis=0) - lane
        n = lax.shift_right_logical(total + TILE // 2 - 1, TILE.bit_length() - 1)
        m = n + jnp.where(total > n * TILE, 1, 0)
        vbuf[slot, pl.ds(total, TILE), :] = jnp.zeros((TILE, 128), BF16)
        pltpu.make_async_copy(kbuf.at[slot, pl.ds(0, total), :], kbuf.at[slot, pl.ds(0, total), :], ksem.at[slot]).wait()

        def first(i, macc, rows=TILE):
            base = pl.multiple_of(i * TILE, TILE)
            for j in range(rows // 256):
                at = pl.multiple_of(base + j * 256, 256)
                s = lax.dot_general(q2, kbuf[slot, pl.ds(at, 256), :], (((1,), (1,)), ((), ())), preferred_element_type=F32)
                for p in range(2):
                    off = at + p * 128
                    part = jnp.where((start <= off) & (end > off), s[:, p * 128:(p + 1) * 128], -jnp.inf)
                    sbuf[:, pl.ds(pl.multiple_of(off, 128), 128)] = part
                    macc = jnp.maximum(macc, part)
            return macc

        macc = lax.fori_loop(0, n, first, jnp.full((cols, 128), -jnp.inf, F32))
        macc = lax.fori_loop(n, m, functools.partial(first, rows=TILE // 2), macc)
        peak = jnp.maximum(jnp.max(macc, axis=1, keepdims=True), s_new)
        w_new = jnp.exp2((s_new - peak) * scale)
        peakb = jnp.broadcast_to(peak, (cols, 128))
        pltpu.make_async_copy(vbuf.at[slot, pl.ds(0, total), :], vbuf.at[slot, pl.ds(0, total), :], vsem.at[slot]).wait()

        def second(i, carry, rows=TILE):
            lacc, acc = carry
            base = pl.multiple_of(i * TILE, TILE)
            parts = []
            for j in range(rows // 128):
                p = jnp.exp2((sbuf[:, pl.ds(pl.multiple_of(base + j * 128, 128), 128)] - peakb) * scale)
                lacc = lacc + p
                parts.append(p.astype(BF16))
            acc = acc + dot(jnp.concatenate(parts, axis=1), vbuf[slot, pl.ds(base, rows), :])
            return lacc, acc

        zero = jnp.zeros((cols, 128), F32)
        lacc, acc = lax.fori_loop(0, n, second, (zero, zero))
        lacc, acc = lax.fori_loop(n, m, functools.partial(second, rows=TILE // 2), (lacc, acc))
        den = jnp.sum(lacc, axis=1, keepdims=True) + w_new
        o = ((acc + w_new.astype(BF16).astype(F32) * heads_of(vn, g).astype(F32)) / den).astype(BF16)
        g0 = pl.multiple_of(g * TOKG, TOKG)
        for j in range(heads):
            os_[pl.ds(g0, TOKG), j * 128:(j + 1) * 128] = o[j * TOKG:(j + 1) * TOKG, :]
        return totals[1:] + (last,)

    lax.fori_loop(0, n_groups, step, totals0)
    wo_cp.wait()


def attention(layer, n_tok, lens, w_out, kc, vc, proj=None, qkv=None):
    dma = pltpu.SemaphoreType.DMA
    first_layer = proj is not None
    out_shape = []
    if first_layer:
        x, tab, wq, wk, wv = proj
        model, qdim, kvdim = wq.shape[1], wq.shape[2], wk.shape[2]
        args = [lens, x, tab, wq, wk, wv, w_out, kc, vc]
        specs = [anyspec()] * 9
        out_shape = [VMEM((n_tok, qdim), BF16), VMEM(w_out.shape[1:], BF16)] + [jax.ShapeDtypeStruct((n_tok, 128), F32)] * 2
        scratch = [VMEM((n_tok, model), BF16), VMEM(tab.shape, F32), VMEM((model, qdim), BF16), VMEM((model, kvdim), BF16), VMEM((model, kvdim), BF16),
                   VMEM((n_tok, qdim), BF16), VMEM((n_tok, kvdim), BF16), VMEM((n_tok, kvdim), BF16), dma((5,))]
    else:
        qdim = qkv[0].shape[1]
        args = [lens, *qkv, w_out, kc, vc]
        specs = [sspec()] + [vspec()] * 3 + [anyspec()] * 3
        out_shape = [VMEM((n_tok, qdim), BF16), VMEM(w_out.shape[1:], BF16)]
        scratch = []
    max_rows = TOKG * kc.shape[2]
    cols = (qdim // 128) * TOKG
    scratch += [VMEM((NSLOT, max_rows + TILE, 128), BF16), VMEM((NSLOT, max_rows + TILE, 128), BF16), VMEM((cols, max_rows), F32),
                VMEM((NSLOT, TOKG, 128), jnp.int32), VMEM((NSLOT, TOKG, 128), jnp.int32), *([pltpu.SMEM(lens.shape, jnp.int32), dma] if first_layer else []), dma((NSLOT,)), dma((NSLOT,)), dma]
    return pl.pallas_call(
        functools.partial(attn_kernel, layer, n_tok, first_layer),
        out_shape=out_shape,
        in_specs=specs,
        out_specs=[vspec()] * len(out_shape),
        scratch_shapes=scratch,
        compiler_params=pltpu.CompilerParams(vmem_limit_bytes=LIM_A if first_layer else LIM_B),
        name=f"attention{layer}",
    )(*args)


NCH = 4


def peers():
    me = lax.axis_index("ep")
    core = me % 2
    x = me // 2
    return me, x * 2 + (1 - core), (1 - x) * 2 + core, (1 - x) * 2 + (1 - core)


def barrier(devices):
    sem = pltpu.get_barrier_semaphore()
    for d in devices:
        pl.semaphore_signal(sem, inc=1, device_id=d, device_id_type=MESH)
    return lambda: pl.semaphore_wait(sem, len(devices))


def rcopy(src, dst, ssem, rsem, dev):
    return pltpu.make_async_remote_copy(src_ref=src, dst_ref=dst, send_sem=ssem, recv_sem=rsem, device_id=dev, device_id_type=MESH)


def weight_copies(layer, e, f, slot, hbm, buf, sems):
    wg_hbm, wu_hbm, wd_hbm = hbm
    cols = pl.ds(f * FT, FT) if isinstance(f, int) else pl.ds(pl.multiple_of(f * FT, FT), FT)
    return (pltpu.make_async_copy(wg_hbm.at[layer, e, :, cols], buf[0].at[slot], sems.at[slot, 0]),
            pltpu.make_async_copy(wu_hbm.at[layer, e, :, cols], buf[1].at[slot], sems.at[slot, 1]),
            pltpu.make_async_copy(wd_hbm.at[layer, e, cols, :], buf[2].at[slot], sems.at[slot, 2]))


def dispatch_kernel(layer, steps, n_loc, os_ref, x_ref, ids_ref, wr_ref, wo, wg_hbm, wu_hbm, wd_hbm, *refs):
    first_layer = layer == 0
    if first_layer:
        a_ref, uall, rrow, mcol, idsall, pg, pu, pd, idsbuf, *sems = refs
        psem, s_p, r_p, s_x, r_x, s_f, r_f, s_i, r_i = sems
    else:
        a_ref, uall, rrow, mcol, pg, pu, pd, *sems = refs
        psem, s_p, r_p, s_x, r_x, s_f, r_f = sems
        idsall = ids_ref
    n = os_ref.shape[0]
    ch = n // NCH
    pool = lax.axis_index("pool")
    me, part, xp, diag = peers()
    devs = [{"ep": part}, {"ep": xp}]
    arrive = barrier(devs)

    def rows(ep, c):
        return pl.ds(pl.multiple_of(ep * n + c * ch, ch), ch)

    ics = []
    if first_layer:
        t0 = pl.multiple_of(pool * n, n)
        idsbuf[...] = jnp.zeros(idsbuf.shape, jnp.int32)
        for l in range(ids_ref.shape[0]):
            idsbuf[2 * l:2 * l + 2, :] = ids_ref[l, :, pl.ds(t0, n)]
        idsall[me] = idsbuf[...]
    xs, ps = [], []
    half = n // 2
    for hf in range(2):
        r = pl.ds(hf * half, half)
        if first_layer:
            xr = x_ref[pl.ds(pl.multiple_of(pool * n + hf * half, half), half), :]
        else:
            xr = x_ref[r, :]
        a = (xr.astype(F32) + dot(os_ref[r, :], wo[...])).astype(BF16)
        a_ref[r, :] = a
        uall[pl.ds(pl.multiple_of(me * n + hf * half, half), half), :] = rms_bf16(a.astype(F32))
        if hf == 0:
            arrive()
            if first_layer:
                for i, d in enumerate(devs):
                    cp = rcopy(idsbuf, idsall.at[me], s_i.at[i], r_i.at[i], d)
                    cp.start()
                    ics.append(cp)
        for c in range(hf * NCH // 2, (hf + 1) * NCH // 2):
            cp = rcopy(uall.at[rows(me, c)], uall.at[rows(me, c)], s_x.at[c], r_x.at[c], {"ep": xp})
            cp.start()
            xs.append(cp)
            cp = rcopy(uall.at[rows(me, c)], uall.at[rows(me, c)], s_p.at[c], r_p.at[c], {"ep": part})
            cp.start()
            ps.append(cp)
    hbm = (wg_hbm, wu_hbm, wd_hbm)

    def prefetch(f, _):
        for cp in weight_copies(layer, 0, f, f, hbm, (pg, pu, pd), psem):
            cp.start()
        return 0

    lax.fori_loop(0, steps, prefetch, 0)
    if first_layer:
        ics[1].wait_recv()
        cp = rcopy(idsall.at[xp], idsall.at[xp], s_i.at[2], r_i.at[2], devs[0])
        cp.start()
        cp.wait()
        ics[0].wait()
        ics[1].wait_send()

    tokens = 4 * n
    e0 = me * n_loc
    ids_row = [jnp.concatenate([idsall[b, 2 * layer + k:2 * layer + k + 1, :] for b in range(4)], axis=1) for k in range(2)]
    row8 = lax.broadcasted_iota(jnp.int32, (8, tokens), 0)
    hit = ((ids_row[0] == row8 + e0) | (ids_row[1] == row8 + e0)) & (row8 < n_loc)
    hit_f = hit.astype(F32)
    tri = (lax.broadcasted_iota(jnp.int32, (tokens, tokens), 0) < lax.broadcasted_iota(jnp.int32, (tokens, tokens), 1)).astype(F32).astype(BF16)
    rank = jnp.where(hit_f > 0, dot(hit_f.astype(BF16), tri), -1.0)
    rrow[...] = rank
    idf = jnp.where(row8 == 2, jnp.broadcast_to(ids_row[0].astype(F32), (8, tokens)),
                    jnp.where(row8 == 3, jnp.broadcast_to(ids_row[1].astype(F32), (8, tokens)), rank))
    mcol[...] = jnp.transpose(idf)

    w = wr_ref[layer]
    w1 = w.astype(BF16).astype(F32)
    w2 = (w - w1).astype(BF16).astype(F32)
    w3 = w - w1 - w2
    wr = jnp.concatenate([w1, w2, w3, jnp.zeros((104, w.shape[1]), F32)], axis=0).astype(BF16)
    e0f = e0.astype(F32)

    def gates(ep):
        r = pl.ds(pl.multiple_of(ep * n, n), n)
        lg = lax.dot_general(uall[r, :], wr, (((1,), (1,)), ((), ())), preferred_element_type=F32)
        lg = lg + pltpu.roll(lg, 120, 1) + pltpu.roll(lg, 112, 1)
        lane = lax.broadcasted_iota(jnp.int32, (n, 128), 1).astype(F32)
        col = mcol[r, :]
        id0, id1 = col[:, 2:3], col[:, 3:4]
        l0 = jnp.sum(jnp.where(lane == id0, lg, 0.0), axis=1, keepdims=True)
        l1 = jnp.sum(jnp.where(lane == id1, lg, 0.0), axis=1, keepdims=True)
        top = jnp.maximum(l0, l1)
        x0 = jnp.exp(l0 - top)
        x1 = jnp.exp(l1 - top)
        den = x0 + x1
        lane8 = lax.broadcasted_iota(jnp.int32, (n, 8), 1)
        expert = (lane8 - 2).astype(F32) + e0f
        g = jnp.where(id0 == expert, x0 / den, 0.0) + jnp.where(id1 == expert, x1 / den, 0.0)
        mcol[r, :] = jnp.where(lane8 < 2, col, g)

    gates(me)
    fs = []

    def forward(c):
        xs[c].wait_recv()
        cp = rcopy(uall.at[rows(xp, c)], uall.at[rows(xp, c)], s_f.at[c], r_f.at[c], {"ep": part})
        cp.start()
        fs.append(cp)

    for c in range(NCH - 1):
        forward(c)
    for cp in ps:
        cp.wait()
    gates(part)
    forward(NCH - 1)
    gates(xp)
    for cp in fs:
        cp.wait()
    gates(diag)
    for cp in xs:
        cp.wait_send()
    for f in range(steps):
        for cp in weight_copies(layer, 0, f, f, hbm, (pg, pu, pd), psem):
            cp.wait()


def dispatch(layer, os_, x, ids, wr, wo, wg, wu, wd):
    n, qdim = os_.shape
    model = wo.shape[1]
    n_loc, ff = wg.shape[1], wg.shape[3]
    steps = ff // FT
    dma = pltpu.SemaphoreType.DMA
    out_shape = [jax.ShapeDtypeStruct((n, model), BF16), jax.ShapeDtypeStruct((4 * n, model), BF16),
                 jax.ShapeDtypeStruct((8, 4 * n), F32), jax.ShapeDtypeStruct((4 * n, 8), F32)]
    scratch = []
    sems = [dma((steps, 3))] + [dma((NCH,))] * 6
    if layer == 0:
        out_shape.append(jax.ShapeDtypeStruct((4, 8, n), jnp.int32))
        scratch.append(VMEM((8, n), jnp.int32))
        sems += [dma((3,)), dma((3,))]
    n_small = len(out_shape)
    out_shape += [VMEM((steps, model, FT), BF16), VMEM((steps, model, FT), BF16), VMEM((steps, FT, model), BF16)]
    return pl.pallas_call(
        functools.partial(dispatch_kernel, layer, steps, n_loc),
        out_shape=out_shape,
        in_specs=[vspec()] * 5 + [anyspec()] * 3,
        out_specs=[vspec()] * n_small + [vspec()] * 3,
        scratch_shapes=scratch + sems,
        compiler_params=pltpu.CompilerParams(collective_id=2 * layer, has_side_effects=True, vmem_limit_bytes=LIM_D),
        name=f"dispatch{layer}",
    )(os_, x, ids, wr, wo, wg, wu, wd)


def expert_kernel(layer, u_ref, rrow_ref, mcol_ref, pg, pu, pd, wg_hbm, wu_hbm, wd_hbm, y_ref, wg, wu, wd, xe, yacc, sems):
    n = u_ref.shape[0]
    steps = pg.shape[0]
    n_loc = wg_hbm.shape[1]
    hbm = (wg_hbm, wu_hbm, wd_hbm)
    own = (wg, wu, wd)

    for e in range(1, n_loc):
        def issue(f, _, e=e):
            for c in weight_copies(layer, e, f, (e - 1) * steps + f, hbm, own, sems):
                c.start()
            return 0
        lax.fori_loop(0, steps, issue, 0)

    for e in range(n_loc):
        rank_row = rrow_ref[e:e + 1, :]
        count = jnp.sum((rank_row >= 0).astype(F32)).astype(jnp.int32)
        lo = 0
        for m in SIZES:
            @pl.when((count <= m) & ((count > lo) | (lo == 0)))
            def _(m=m, e=e):
                sel = (rank_row == lax.broadcasted_iota(jnp.int32, (m, n), 0).astype(F32)).astype(F32).astype(BF16)
                xe[pl.ds(0, m), :] = dot(sel, u_ref[...]).astype(BF16)
                yacc[pl.ds(0, m), :] = jnp.zeros((m, yacc.shape[1]), F32)

                def step(f, _):
                    if e == 0:
                        w1, w3, w2 = pg, pu, pd
                        slot = f
                    else:
                        w1, w3, w2 = own
                        slot = (e - 1) * steps + f
                        for c in weight_copies(layer, e, f, slot, hbm, own, sems):
                            c.wait()
                    inner = []
                    for j in range(FT // 256):
                        at = pl.ds(j * 256, 256)
                        gate = dot(xe[pl.ds(0, m), :], w1[slot, :, at])
                        up = dot(xe[pl.ds(0, m), :], w3[slot, :, at])
                        inner.append((gate * jax.nn.sigmoid(gate) * up).astype(BF16))
                    yacc[pl.ds(0, m), :] += dot(jnp.concatenate(inner, axis=1), w2[slot])
                    return 0

                lax.fori_loop(0, steps, step, 0)
                y_ref[pl.ds(e * n, m), :] = yacc[pl.ds(0, m), :].astype(BF16)
                if m < n:
                    y_ref[pl.ds(e * n + m, n - m), :] = jnp.zeros((n - m, y_ref.shape[1]), BF16)
            lo = m


def experts(layer, u_all, rrow, mcol, pre, wg, wu, wd):
    n, model = u_all.shape
    steps = pre[0].shape[0]
    n_loc = wg.shape[1]
    slots = steps * (n_loc - 1)
    return pl.pallas_call(
        functools.partial(expert_kernel, layer),
        out_shape=jax.ShapeDtypeStruct((n_loc * n, model), BF16),
        in_specs=[vspec()] * 6 + [anyspec()] * 3,
        out_specs=vspec(),
        scratch_shapes=[VMEM((slots, model, FT), BF16), VMEM((slots, model, FT), BF16), VMEM((slots, FT, model), BF16),
                        VMEM((n, model), BF16), VMEM((n, model), F32), pltpu.SemaphoreType.DMA((slots, 3))],
        compiler_params=pltpu.CompilerParams(vmem_limit_bytes=LIM_E),
        name=f"experts{layer}",
    )(u_all, rrow, mcol, *pre, wg, wu, wd)


def combine_kernel(last, layer, y_ref, mcol_ref, a_ref, *refs):
    if last:
        out_ref, p_d, p_x, p_p, p_me, own, mid, far, *sems = refs
        s_o, r_o, s_m, r_m, s_f, r_f, s_y, r_y = sems
    else:
        (cos_ref, sin_ref, wq_hbm, wk_hbm, wv_hbm, out_ref, qs, kn, vn,
         p_d, p_x, p_p, p_me, own, mid, far, wq, wk, wv, *sems) = refs
        s_o, r_o, s_m, r_m, s_f, r_f, wsem = sems
    n = a_ref.shape[0]
    ch = n // CCH
    nn = mcol_ref.shape[0]
    me, part, xp, diag = peers()
    devs = [{"ep": part}, {"ep": xp}]
    if last:
        pool = lax.axis_index("pool")
        devs.append({"pool": 1 - pool})
    else:
        w_copies = [pltpu.make_async_copy(src.at[layer + 1], dst, wsem.at[i])
                    for i, (src, dst) in enumerate(((wq_hbm, wq), (wk_hbm, wk), (wv_hbm, wv)))]
        for c in w_copies:
            c.start()

    def partial(ep):
        col = mcol_ref[pl.ds(pl.multiple_of(ep * n, n), n), :]
        slot = lax.broadcasted_iota(jnp.int32, (n, nn), 1).astype(F32)
        total = None
        for e in range(y_ref.shape[0] // nn):
            sel = (col[:, e:e + 1] == slot).astype(F32).astype(BF16)
            t = dot(sel, y_ref[e * nn:(e + 1) * nn, :]) * col[:, 2 + e:3 + e]
            total = t if total is None else total + t
        return total

    arrive = barrier(devs)
    p_d[...] = partial(diag)
    arrive()
    depth = 4 if last else CCH
    mids, fars, ys = [], [], []
    for c in range(CCH):
        r = pl.ds(c * ch, ch)
        cp = rcopy(p_d.at[r], mid.at[r], s_m.at[c], r_m.at[c], devs[0])
        cp.start()
        mids.append(cp)
    p_x[...] = partial(xp)

    def send(c):
        r = pl.ds(c * ch, ch)
        mids[c].wait_recv()
        p_x[r, :] = p_x[r, :] + mid[r, :]
        if c >= depth:
            fars[c - depth].wait_send()
        cp = rcopy(p_x.at[r], far.at[r], s_f.at[c], r_f.at[c], devs[1])
        cp.start()
        fars.append(cp)

    def receive(c):
        r = pl.ds(c * ch, ch)
        fars[c].wait_recv()
        res = (p_me[r, :] + far[r, :]).astype(BF16)
        if last:
            o = pl.ds(pl.multiple_of(pool * n + c * ch, ch), ch)
            out_ref[o, :] = res
            cp = rcopy(out_ref.at[o], out_ref.at[o], s_y.at[c], r_y.at[c], devs[2])
            cp.start()
            ys.append(cp)
        else:
            out_ref[r, :] = res
            if c % (CCH // 2) == CCH // 2 - 1:
                r2 = pl.ds(c * ch + ch - n // 2, n // 2)
                h = rms_bf16(out_ref[r2, :].astype(F32))
                project(h, cos_ref[r2, :], sin_ref[r2, :], wq, wk, wv, qs, kn, vn, r2)

    for c in range(depth):
        send(c)
    p_p[...] = partial(part)
    own_cp = rcopy(p_p, own, s_o, r_o, devs[0])
    own_cp.start()
    p_me[...] = partial(me)
    own_cp.wait()
    p_me[...] = a_ref[...].astype(F32) + (p_me[...] + own[...])
    if not last:
        for c in w_copies:
            c.wait()
    for c in range(depth, CCH):
        send(c)
        receive(c - depth)
    for c in range(CCH - depth, CCH):
        receive(c)
    for c in range(CCH):
        mids[c].wait_send()
    for c in range(CCH - depth, CCH):
        fars[c].wait_send()
    for cp in ys:
        cp.wait()


def combine(layer, last, y, mcol, a, nxt=None):
    n, model = a.shape
    dma = pltpu.SemaphoreType.DMA
    sems = [dma, dma, dma((CCH,)), dma((CCH,)), dma((CCH,)), dma((CCH,))]
    args = [y, mcol, a]
    specs = [vspec()] * 3
    scratch = [VMEM((n, model), F32) for _ in range(7)]
    if last:
        sems += [dma((CCH,)), dma((CCH,))]
        out_shape = jax.ShapeDtypeStruct((2 * n, model), BF16)
        out_specs = vspec()
    else:
        cos, sin, wq, wk, wv = nxt
        args += [cos, sin, wq, wk, wv]
        specs += [vspec()] * 2 + [anyspec()] * 3
        sems += [dma((3,))]
        scratch += [VMEM(w.shape[1:], BF16) for w in (wq, wk, wv)]
        out_shape = [jax.ShapeDtypeStruct((n, model), BF16)] + [jax.ShapeDtypeStruct((n, w.shape[2]), BF16) for w in (wq, wk, wv)]
        out_specs = [vspec()] * 4
    return pl.pallas_call(
        functools.partial(combine_kernel, last, layer),
        out_shape=out_shape,
        in_specs=specs,
        out_specs=out_specs,
        scratch_shapes=scratch + sems,
        compiler_params=pltpu.CompilerParams(collective_id=2 * layer + 1, has_side_effects=True, vmem_limit_bytes=LIM_C),
        name=f"combine{layer}",
    )(*args)


def solution(mesh):
    def body(hidden, k_cache, v_cache, lengths, expert_ids, w_query, w_key, w_value, w_out, w_router, w_gate, w_up, w_down):
        n_layers, _, seq, kvh, hd = k_cache.shape
        n_tok = hidden.shape[0] // 2
        kc = k_cache.reshape(n_layers, -1, seq * kvh, hd)
        vc = v_cache.reshape(n_layers, -1, seq * kvh, hd)
        ids = expert_ids.transpose(0, 2, 1)
        wr = w_router.transpose(0, 2, 1)
        tab = jnp.asarray(rope_table(seq, hd))
        w_query, w_key, w_value, w_out, w_gate, w_up, w_down, kc, vc, tab, hidden_h, lens_h = (
            pltpu.with_memory_space_constraint(v, pltpu.HBM) for v in (w_query, w_key, w_value, w_out, w_gate, w_up, w_down, kc, vc, tab, hidden, lengths))
        state = hidden
        qkv = None
        for layer in range(n_layers):
            last = layer == n_layers - 1
            if layer == 0:
                att, wo, cos, sin = attention(layer, n_tok, lens_h, w_out, kc, vc, proj=(hidden_h, tab, w_query, w_key, w_value))
            else:
                att, wo = attention(layer, n_tok, lengths, w_out, kc, vc, qkv=qkv)
            outs = dispatch(layer, att, state, ids, wr, wo, w_gate, w_up, w_down)
            a, u_all, rrow, mcol = outs[:4]
            if layer == 0:
                ids = outs[4]
            y = experts(layer, u_all, rrow, mcol, outs[-3:], w_gate, w_up, w_down)
            if last:
                return combine(layer, True, y, mcol, a)
            state, *qkv = combine(layer, False, y, mcol, a, nxt=(cos, sin, w_query, w_key, w_value))

    rows_spec = ("dp", "ep")
    in_specs = (P(rows_spec, None), P(None, rows_spec), P(None, rows_spec), P(rows_spec), P(None, rows_spec, None), P(), P(), P(), P(), P(), P(None, "ep"), P(None, "ep"), P(None, "ep"))
    return jax.shard_map(body, mesh=mesh, in_specs=in_specs, out_specs=P(rows_spec, None), check_vma=False)
```

```python
import functools

import numpy as np

import jax
import jax.numpy as jnp
from jax import lax
from jax.experimental import pallas as pl
from jax.experimental.pallas import tpu as pltpu
from jax.sharding import PartitionSpec as P

MESH = pl.DeviceIdType.MESH
EPSILON = 1e-6
ROPE_BASE = 10000.0
VMEM = pltpu.VMEM
F32 = jnp.float32
BF16 = jnp.bfloat16

TOKG = 16
TILE = 1024
FT = 512
NSLOT = 3
CCH = 8
LIM_A = 50 * 1024 * 1024
LIM_B = 50 * 1024 * 1024
LIM_D = 8 * 1024 * 1024
LIM_E = 27 * 1024 * 1024
LIM_C = 16 * 1024 * 1024
SIZES = (128, 400, 512)


def vspec():
    return pl.BlockSpec(memory_space=VMEM)


def anyspec():
    return pl.BlockSpec(memory_space=pltpu.HBM)


def sspec():
    return pl.BlockSpec(memory_space=pltpu.SMEM)


def dot(a, b):
    return jnp.dot(a, b, preferred_element_type=F32)


def rms_bf16(v):
    return (v * lax.rsqrt(jnp.mean(v * v, axis=-1, keepdims=True) + EPSILON)).astype(BF16)


def rope_table(seq, hd):
    half = hd // 2
    freqs = np.power(np.float32(ROPE_BASE), (np.float32(-2.0) * np.arange(half, dtype=np.float32) / np.float32(hd)))
    angle = np.arange(seq + 1, dtype=np.float32)[:, None] * freqs.astype(np.float32)[None, :]
    wide = angle.astype(np.float64)
    return np.concatenate([np.cos(wide), np.sin(wide)], axis=1).astype(np.float32)


def rope(vec, cos, sin):
    return vec * cos + pltpu.roll(vec, 64, 1) * sin


def project(h, cos, sin, wq, wk, wv, qs, kn, vn, rows):
    q = dot(h, wq[...])
    k = dot(h, wk[...])
    v = dot(h, wv[...])
    for j in range(q.shape[1] // 128):
        qs[rows, j * 128:(j + 1) * 128] = rope(q[:, j * 128:(j + 1) * 128], cos, sin).astype(BF16)
    for j in range(k.shape[1] // 128):
        kn[rows, j * 128:(j + 1) * 128] = rope(k[:, j * 128:(j + 1) * 128], cos, sin).astype(BF16)
    vn[rows, :] = v.astype(BF16)


def attn_kernel(layer, n_tok, first_layer, lens_in, *refs):
    if first_layer:
        (x_hbm, tab_hbm, wq_hbm, wk_hbm, wv_hbm, wo_hbm, kc, vc, os_, wo, cos_ref, sin_ref,
         x_ref, tab_ref, wq, wk, wv, qs, kn, vn, wsem, kbuf, vbuf, sbuf, mst, men, lens_ref, lsem, ksem, vsem, osem) = refs
    else:
        qs, kn, vn, wo_hbm, kc, vc, os_, wo, kbuf, vbuf, sbuf, mst, men, ksem, vsem, osem = refs
        lens_ref = lens_in
    t0 = lax.axis_index("pool") * n_tok
    if first_layer:
        lens_cp = pltpu.make_async_copy(lens_in, lens_ref, lsem)
        lens_cp.start()
    heads = qs.shape[1] // 128
    n_groups = n_tok // TOKG
    hpk = heads // 2
    cols = heads * TOKG

    def padded(ln):
        return pl.multiple_of(lax.shift_left(lax.shift_right_logical(ln + 7, 3), 4), 16)

    def start_group(g):
        slot = lax.rem(g, NSLOT)
        off = 0
        for i in range(TOKG):
            tok = t0 + g * TOKG + i
            ln = lens_ref[tok]
            n = padded(ln)
            off = pl.multiple_of(off, 16)
            pltpu.make_async_copy(kc.at[layer, tok, pl.ds(0, n), :], kbuf.at[slot, pl.ds(off, n), :], ksem.at[slot]).start()
            pltpu.make_async_copy(vc.at[layer, tok, pl.ds(0, n), :], vbuf.at[slot, pl.ds(off, n), :], vsem.at[slot]).start()
            mst[slot, i:i + 1, :] = jnp.full((1, 128), off, jnp.int32)
            men[slot, i:i + 1, :] = jnp.full((1, 128), off + 2 * ln, jnp.int32)
            off = off + n
        return jnp.asarray(off, jnp.int32)

    if first_layer:
        w_copies = [pltpu.make_async_copy(src.at[layer], dst, wsem.at[i])
                    for i, (src, dst) in enumerate(((wq_hbm, wq), (wk_hbm, wk), (wv_hbm, wv)))]
        x_cp = pltpu.make_async_copy(x_hbm.at[pl.ds(pl.multiple_of(t0, n_tok), n_tok), :], x_ref, wsem.at[3])
        tab_cp = pltpu.make_async_copy(tab_hbm, tab_ref, wsem.at[4])
        x_cp.start()
        tab_cp.start()
        for c in w_copies:
            c.start()
    if first_layer:
        lens_cp.wait()
    totals0 = tuple(start_group(jnp.int32(g)) for g in range(NSLOT - 1))
    wo_cp = pltpu.make_async_copy(wo_hbm.at[layer], wo, osem)
    wo_cp.start()
    if first_layer:
        x_cp.wait()
        tab_cp.wait()
        h = rms_bf16(x_ref[...].astype(F32))

        def pick(i, _):
            cos_ref[pl.ds(i, 1), :] = tab_ref[pl.ds(lens_ref[t0 + i], 1), :]
            return 0
        lax.fori_loop(0, n_tok, pick, 0, unroll=8)
        both = cos_ref[...]
        swapped = pltpu.roll(both, 64, 1)
        low = lax.broadcasted_iota(jnp.int32, both.shape, 1) < 64
        cos = jnp.where(low, both, swapped)
        sin = jnp.where(low, -swapped, both)
        cos_ref[...] = cos
        sin_ref[...] = sin
        for c in w_copies:
            c.wait()
        project(h, cos, sin, wq, wk, wv, qs, kn, vn, pl.ds(0, n_tok))
    scale = 128.0 ** -0.5 * 1.4426950408889634

    lane = lax.broadcasted_iota(jnp.int32, (cols, 128), 1)
    kv = (lax.broadcasted_iota(jnp.int32, (cols, 128), 0) >= (hpk * TOKG)).astype(jnp.int32)
    mine = (lane & 1) == kv

    def heads_of(ref, g):
        row = ref[pl.ds(pl.multiple_of(g * TOKG, TOKG), TOKG), :]
        per = heads // (ref.shape[1] // 128)
        return jnp.concatenate([row[:, (j // per) * 128:(j // per + 1) * 128] for j in range(heads)], axis=0)

    def step(g, totals):
        total = pl.multiple_of(totals[0], 16)
        slot = lax.rem(g, NSLOT)
        last = lax.cond(g + NSLOT - 1 < n_groups, lambda: start_group(g + NSLOT - 1), lambda: jnp.int32(0))
        q2 = heads_of(qs, g)
        s_new = jnp.sum(q2.astype(F32) * heads_of(kn, g).astype(F32), axis=1, keepdims=True)
        start = jnp.where(mine, jnp.concatenate([mst[slot]] * heads, axis=0) - lane, 1 << 30)
        end = jnp.concatenate([men[slot]] * heads, axis=0) - lane
        n = lax.shift_right_logical(total + TILE // 2 - 1, TILE.bit_length() - 1)
        m = n + jnp.where(total > n * TILE, 1, 0)
        vbuf[slot, pl.ds(total, TILE), :] = jnp.zeros((TILE, 128), BF16)
        pltpu.make_async_copy(kbuf.at[slot, pl.ds(0, total), :], kbuf.at[slot, pl.ds(0, total), :], ksem.at[slot]).wait()

        def first(i, macc, rows=TILE):
            base = pl.multiple_of(i * TILE, TILE)
            for j in range(rows // 256):
                at = pl.multiple_of(base + j * 256, 256)
                s = lax.dot_general(q2, kbuf[slot, pl.ds(at, 256), :], (((1,), (1,)), ((), ())), preferred_element_type=F32)
                for p in range(2):
                    off = at + p * 128
                    part = jnp.where((start <= off) & (end > off), s[:, p * 128:(p + 1) * 128], -jnp.inf)
                    sbuf[:, pl.ds(pl.multiple_of(off, 128), 128)] = part
                    macc = jnp.maximum(macc, part)
            return macc

        macc = lax.fori_loop(0, n, first, jnp.full((cols, 128), -jnp.inf, F32))
        macc = lax.fori_loop(n, m, functools.partial(first, rows=TILE // 2), macc)
        peak = jnp.maximum(jnp.max(macc, axis=1, keepdims=True), s_new)
        w_new = jnp.exp2((s_new - peak) * scale)
        peakb = jnp.broadcast_to(peak, (cols, 128))
        pltpu.make_async_copy(vbuf.at[slot, pl.ds(0, total), :], vbuf.at[slot, pl.ds(0, total), :], vsem.at[slot]).wait()

        def second(i, carry, rows=TILE):
            lacc, acc = carry
            base = pl.multiple_of(i * TILE, TILE)
            parts = []
            for j in range(rows // 128):
                p = jnp.exp2((sbuf[:, pl.ds(pl.multiple_of(base + j * 128, 128), 128)] - peakb) * scale)
                lacc = lacc + p
                parts.append(p.astype(BF16))
            acc = acc + dot(jnp.concatenate(parts, axis=1), vbuf[slot, pl.ds(base, rows), :])
            return lacc, acc

        zero = jnp.zeros((cols, 128), F32)
        lacc, acc = lax.fori_loop(0, n, second, (zero, zero))
        lacc, acc = lax.fori_loop(n, m, functools.partial(second, rows=TILE // 2), (lacc, acc))
        den = jnp.sum(lacc, axis=1, keepdims=True) + w_new
        o = ((acc + w_new.astype(BF16).astype(F32) * heads_of(vn, g).astype(F32)) / den).astype(BF16)
        g0 = pl.multiple_of(g * TOKG, TOKG)
        for j in range(heads):
            os_[pl.ds(g0, TOKG), j * 128:(j + 1) * 128] = o[j * TOKG:(j + 1) * TOKG, :]
        return totals[1:] + (last,)

    lax.fori_loop(0, n_groups, step, totals0)
    wo_cp.wait()


def attention(layer, n_tok, lens, w_out, kc, vc, proj=None, qkv=None):
    dma = pltpu.SemaphoreType.DMA
    first_layer = proj is not None
    out_shape = []
    if first_layer:
        x, tab, wq, wk, wv = proj
        model, qdim, kvdim = wq.shape[1], wq.shape[2], wk.shape[2]
        args = [lens, x, tab, wq, wk, wv, w_out, kc, vc]
        specs = [anyspec()] * 9
        out_shape = [VMEM((n_tok, qdim), BF16), VMEM(w_out.shape[1:], BF16)] + [jax.ShapeDtypeStruct((n_tok, 128), F32)] * 2
        scratch = [VMEM((n_tok, model), BF16), VMEM(tab.shape, F32), VMEM((model, qdim), BF16), VMEM((model, kvdim), BF16), VMEM((model, kvdim), BF16),
                   VMEM((n_tok, qdim), BF16), VMEM((n_tok, kvdim), BF16), VMEM((n_tok, kvdim), BF16), dma((5,))]
    else:
        qdim = qkv[0].shape[1]
        args = [lens, *qkv, w_out, kc, vc]
        specs = [sspec()] + [vspec()] * 3 + [anyspec()] * 3
        out_shape = [VMEM((n_tok, qdim), BF16), VMEM(w_out.shape[1:], BF16)]
        scratch = []
    max_rows = TOKG * kc.shape[2]
    cols = (qdim // 128) * TOKG
    scratch += [VMEM((NSLOT, max_rows + TILE, 128), BF16), VMEM((NSLOT, max_rows + TILE, 128), BF16), VMEM((cols, max_rows), F32),
                VMEM((NSLOT, TOKG, 128), jnp.int32), VMEM((NSLOT, TOKG, 128), jnp.int32), *([pltpu.SMEM(lens.shape, jnp.int32), dma] if first_layer else []), dma((NSLOT,)), dma((NSLOT,)), dma]
    return pl.pallas_call(
        functools.partial(attn_kernel, layer, n_tok, first_layer),
        out_shape=out_shape,
        in_specs=specs,
        out_specs=[vspec()] * len(out_shape),
        scratch_shapes=scratch,
        compiler_params=pltpu.CompilerParams(vmem_limit_bytes=LIM_A if first_layer else LIM_B),
        name=f"attention{layer}",
    )(*args)


NCH = 8


def peers():
    me = lax.axis_index("ep")
    core = me % 2
    x = me // 2
    return me, x * 2 + (1 - core), (1 - x) * 2 + core, (1 - x) * 2 + (1 - core)


def barrier(devices):
    sem = pltpu.get_barrier_semaphore()
    for d in devices:
        pl.semaphore_signal(sem, inc=1, device_id=d, device_id_type=MESH)
    return lambda: pl.semaphore_wait(sem, len(devices))


def rcopy(src, dst, ssem, rsem, dev):
    return pltpu.make_async_remote_copy(src_ref=src, dst_ref=dst, send_sem=ssem, recv_sem=rsem, device_id=dev, device_id_type=MESH)


def weight_copies(layer, e, f, slot, hbm, buf, sems):
    wg_hbm, wu_hbm, wd_hbm = hbm
    cols = pl.ds(f * FT, FT) if isinstance(f, int) else pl.ds(pl.multiple_of(f * FT, FT), FT)
    return (pltpu.make_async_copy(wg_hbm.at[layer, e, :, cols], buf[0].at[slot], sems.at[slot, 0]),
            pltpu.make_async_copy(wu_hbm.at[layer, e, :, cols], buf[1].at[slot], sems.at[slot, 1]),
            pltpu.make_async_copy(wd_hbm.at[layer, e, cols, :], buf[2].at[slot], sems.at[slot, 2]))


def dispatch_kernel(layer, steps, n_loc, os_ref, x_ref, ids_ref, wr_ref, wo, wg_hbm, wu_hbm, wd_hbm, *refs):
    first_layer = layer == 0
    if first_layer:
        a_ref, uall, rrow, mcol, idsall, pg, pu, pd, idsbuf, *sems = refs
        psem, s_p, r_p, s_x, r_x, s_f, r_f, s_i, r_i = sems
    else:
        a_ref, uall, rrow, mcol, pg, pu, pd, *sems = refs
        psem, s_p, r_p, s_x, r_x, s_f, r_f = sems
        idsall = ids_ref
    n = os_ref.shape[0]
    ch = n // NCH
    pool = lax.axis_index("pool")
    me, part, xp, diag = peers()
    devs = [{"ep": part}, {"ep": xp}]
    arrive = barrier(devs)

    def rows(ep, c):
        return pl.ds(pl.multiple_of(ep * n + c * ch, ch), ch)

    ics = []
    if first_layer:
        t0 = pl.multiple_of(pool * n, n)
        idsbuf[...] = jnp.zeros(idsbuf.shape, jnp.int32)
        for l in range(ids_ref.shape[0]):
            idsbuf[2 * l:2 * l + 2, :] = ids_ref[l, :, pl.ds(t0, n)]
        idsall[me] = idsbuf[...]
    xs, ps = [], []
    half = n // 2
    for hf in range(2):
        r = pl.ds(hf * half, half)
        if first_layer:
            xr = x_ref[pl.ds(pl.multiple_of(pool * n + hf * half, half), half), :]
        else:
            xr = x_ref[r, :]
        a = (xr.astype(F32) + dot(os_ref[r, :], wo[...])).astype(BF16)
        a_ref[r, :] = a
        uall[pl.ds(pl.multiple_of(me * n + hf * half, half), half), :] = rms_bf16(a.astype(F32))
        if hf == 0:
            arrive()
            if first_layer:
                for i, d in enumerate(devs):
                    cp = rcopy(idsbuf, idsall.at[me], s_i.at[i], r_i.at[i], d)
                    cp.start()
                    ics.append(cp)
        for c in range(hf * NCH // 2, (hf + 1) * NCH // 2):
            cp = rcopy(uall.at[rows(me, c)], uall.at[rows(me, c)], s_x.at[c], r_x.at[c], {"ep": xp})
            cp.start()
            xs.append(cp)
            cp = rcopy(uall.at[rows(me, c)], uall.at[rows(me, c)], s_p.at[c], r_p.at[c], {"ep": part})
            cp.start()
            ps.append(cp)
    hbm = (wg_hbm, wu_hbm, wd_hbm)

    def prefetch(f, _):
        for cp in weight_copies(layer, 0, f, f, hbm, (pg, pu, pd), psem):
            cp.start()
        return 0

    lax.fori_loop(0, steps, prefetch, 0)
    if first_layer:
        ics[1].wait_recv()
        cp = rcopy(idsall.at[xp], idsall.at[xp], s_i.at[2], r_i.at[2], devs[0])
        cp.start()
        cp.wait()
        ics[0].wait()
        ics[1].wait_send()

    tokens = 4 * n
    e0 = me * n_loc
    ids_row = [jnp.concatenate([idsall[b, 2 * layer + k:2 * layer + k + 1, :] for b in range(4)], axis=1) for k in range(2)]
    row8 = lax.broadcasted_iota(jnp.int32, (8, tokens), 0)
    hit = ((ids_row[0] == row8 + e0) | (ids_row[1] == row8 + e0)) & (row8 < n_loc)
    hit_f = hit.astype(F32)
    tri = (lax.broadcasted_iota(jnp.int32, (tokens, tokens), 0) < lax.broadcasted_iota(jnp.int32, (tokens, tokens), 1)).astype(F32).astype(BF16)
    rank = jnp.where(hit_f > 0, dot(hit_f.astype(BF16), tri), -1.0)
    rrow[...] = rank
    idf = jnp.where(row8 == 2, jnp.broadcast_to(ids_row[0].astype(F32), (8, tokens)),
                    jnp.where(row8 == 3, jnp.broadcast_to(ids_row[1].astype(F32), (8, tokens)), rank))
    mcol[...] = jnp.transpose(idf)

    w = wr_ref[layer]
    w1 = w.astype(BF16).astype(F32)
    w2 = (w - w1).astype(BF16).astype(F32)
    w3 = w - w1 - w2
    wr = jnp.concatenate([w1, w2, w3, jnp.zeros((104, w.shape[1]), F32)], axis=0).astype(BF16)
    e0f = e0.astype(F32)

    def gates(ep):
        r = pl.ds(pl.multiple_of(ep * n, n), n)
        lg = lax.dot_general(uall[r, :], wr, (((1,), (1,)), ((), ())), preferred_element_type=F32)
        lg = lg + pltpu.roll(lg, 120, 1) + pltpu.roll(lg, 112, 1)
        lane = lax.broadcasted_iota(jnp.int32, (n, 128), 1).astype(F32)
        col = mcol[r, :]
        id0, id1 = col[:, 2:3], col[:, 3:4]
        l0 = jnp.sum(jnp.where(lane == id0, lg, 0.0), axis=1, keepdims=True)
        l1 = jnp.sum(jnp.where(lane == id1, lg, 0.0), axis=1, keepdims=True)
        top = jnp.maximum(l0, l1)
        x0 = jnp.exp(l0 - top)
        x1 = jnp.exp(l1 - top)
        den = x0 + x1
        lane8 = lax.broadcasted_iota(jnp.int32, (n, 8), 1)
        expert = (lane8 - 2).astype(F32) + e0f
        g = jnp.where(id0 == expert, x0 / den, 0.0) + jnp.where(id1 == expert, x1 / den, 0.0)
        mcol[r, :] = jnp.where(lane8 < 2, col, g)

    gates(me)
    fs = []

    def forward(c):
        xs[c].wait_recv()
        cp = rcopy(uall.at[rows(xp, c)], uall.at[rows(xp, c)], s_f.at[c], r_f.at[c], {"ep": part})
        cp.start()
        fs.append(cp)

    for c in range(NCH - 1):
        forward(c)
    for cp in ps:
        cp.wait()
    gates(part)
    forward(NCH - 1)
    gates(xp)
    for cp in fs:
        cp.wait()
    gates(diag)
    for cp in xs:
        cp.wait_send()
    for f in range(steps):
        for cp in weight_copies(layer, 0, f, f, hbm, (pg, pu, pd), psem):
            cp.wait()


def dispatch(layer, os_, x, ids, wr, wo, wg, wu, wd):
    n, qdim = os_.shape
    model = wo.shape[1]
    n_loc, ff = wg.shape[1], wg.shape[3]
    steps = ff // FT
    dma = pltpu.SemaphoreType.DMA
    out_shape = [jax.ShapeDtypeStruct((n, model), BF16), jax.ShapeDtypeStruct((4 * n, model), BF16),
                 jax.ShapeDtypeStruct((8, 4 * n), F32), jax.ShapeDtypeStruct((4 * n, 8), F32)]
    scratch = []
    sems = [dma((steps, 3))] + [dma((NCH,))] * 6
    if layer == 0:
        out_shape.append(jax.ShapeDtypeStruct((4, 8, n), jnp.int32))
        scratch.append(VMEM((8, n), jnp.int32))
        sems += [dma((3,)), dma((3,))]
    n_small = len(out_shape)
    out_shape += [VMEM((steps, model, FT), BF16), VMEM((steps, model, FT), BF16), VMEM((steps, FT, model), BF16)]
    return pl.pallas_call(
        functools.partial(dispatch_kernel, layer, steps, n_loc),
        out_shape=out_shape,
        in_specs=[vspec()] * 5 + [anyspec()] * 3,
        out_specs=[vspec()] * n_small + [vspec()] * 3,
        scratch_shapes=scratch + sems,
        compiler_params=pltpu.CompilerParams(collective_id=2 * layer, has_side_effects=True, vmem_limit_bytes=LIM_D),
        name=f"dispatch{layer}",
    )(os_, x, ids, wr, wo, wg, wu, wd)


def expert_kernel(layer, u_ref, rrow_ref, mcol_ref, pg, pu, pd, wg_hbm, wu_hbm, wd_hbm, y_ref, wg, wu, wd, xe, yacc, sems):
    n = u_ref.shape[0]
    steps = pg.shape[0]
    n_loc = wg_hbm.shape[1]
    hbm = (wg_hbm, wu_hbm, wd_hbm)
    own = (wg, wu, wd)

    for e in range(1, n_loc):
        def issue(f, _, e=e):
            for c in weight_copies(layer, e, f, (e - 1) * steps + f, hbm, own, sems):
                c.start()
            return 0
        lax.fori_loop(0, steps, issue, 0)

    for e in range(n_loc):
        rank_row = rrow_ref[e:e + 1, :]
        count = jnp.sum((rank_row >= 0).astype(F32)).astype(jnp.int32)
        lo = 0
        for m in SIZES:
            @pl.when((count <= m) & ((count > lo) | (lo == 0)))
            def _(m=m, e=e):
                sel = (rank_row == lax.broadcasted_iota(jnp.int32, (m, n), 0).astype(F32)).astype(F32).astype(BF16)
                xe[pl.ds(0, m), :] = dot(sel, u_ref[...]).astype(BF16)
                yacc[pl.ds(0, m), :] = jnp.zeros((m, yacc.shape[1]), F32)

                def step(f, _):
                    if e == 0:
                        w1, w3, w2 = pg, pu, pd
                        slot = f
                    else:
                        w1, w3, w2 = own
                        slot = (e - 1) * steps + f
                        for c in weight_copies(layer, e, f, slot, hbm, own, sems):
                            c.wait()
                    inner = []
                    for j in range(FT // 256):
                        at = pl.ds(j * 256, 256)
                        gate = dot(xe[pl.ds(0, m), :], w1[slot, :, at])
                        up = dot(xe[pl.ds(0, m), :], w3[slot, :, at])
                        inner.append((gate * jax.nn.sigmoid(gate) * up).astype(BF16))
                    yacc[pl.ds(0, m), :] += dot(jnp.concatenate(inner, axis=1), w2[slot])
                    return 0

                lax.fori_loop(0, steps, step, 0)
                y_ref[pl.ds(e * n, m), :] = yacc[pl.ds(0, m), :].astype(BF16)
                if m < n:
                    y_ref[pl.ds(e * n + m, n - m), :] = jnp.zeros((n - m, y_ref.shape[1]), BF16)
            lo = m


def experts(layer, u_all, rrow, mcol, pre, wg, wu, wd):
    n, model = u_all.shape
    steps = pre[0].shape[0]
    n_loc = wg.shape[1]
    slots = steps * (n_loc - 1)
    return pl.pallas_call(
        functools.partial(expert_kernel, layer),
        out_shape=jax.ShapeDtypeStruct((n_loc * n, model), BF16),
        in_specs=[vspec()] * 6 + [anyspec()] * 3,
        out_specs=vspec(),
        scratch_shapes=[VMEM((slots, model, FT), BF16), VMEM((slots, model, FT), BF16), VMEM((slots, FT, model), BF16),
                        VMEM((n, model), BF16), VMEM((n, model), F32), pltpu.SemaphoreType.DMA((slots, 3))],
        compiler_params=pltpu.CompilerParams(vmem_limit_bytes=LIM_E),
        name=f"experts{layer}",
    )(u_all, rrow, mcol, *pre, wg, wu, wd)


def combine_kernel(last, layer, y_ref, mcol_ref, a_ref, *refs):
    if last:
        out_ref, p_d, p_x, p_p, p_me, own, mid, far, *sems = refs
        s_o, r_o, s_m, r_m, s_f, r_f, s_y, r_y = sems
    else:
        (cos_ref, sin_ref, wq_hbm, wk_hbm, wv_hbm, out_ref, qs, kn, vn,
         p_d, p_x, p_p, p_me, own, mid, far, wq, wk, wv, *sems) = refs
        s_o, r_o, s_m, r_m, s_f, r_f, wsem = sems
    n = a_ref.shape[0]
    ch = n // CCH
    nn = mcol_ref.shape[0]
    me, part, xp, diag = peers()
    devs = [{"ep": part}, {"ep": xp}]
    if last:
        pool = lax.axis_index("pool")
        devs.append({"pool": 1 - pool})
    else:
        w_copies = [pltpu.make_async_copy(src.at[layer + 1], dst, wsem.at[i])
                    for i, (src, dst) in enumerate(((wq_hbm, wq), (wk_hbm, wk), (wv_hbm, wv)))]
        for c in w_copies:
            c.start()

    def partial(ep):
        col = mcol_ref[pl.ds(pl.multiple_of(ep * n, n), n), :]
        slot = lax.broadcasted_iota(jnp.int32, (n, nn), 1).astype(F32)
        total = None
        for e in range(y_ref.shape[0] // nn):
            sel = (col[:, e:e + 1] == slot).astype(F32).astype(BF16)
            t = dot(sel, y_ref[e * nn:(e + 1) * nn, :]) * col[:, 2 + e:3 + e]
            total = t if total is None else total + t
        return total

    arrive = barrier(devs)
    p_d[...] = partial(diag)
    arrive()
    depth = 4 if last else CCH
    mids, fars, ys = [], [], []
    for c in range(CCH):
        r = pl.ds(c * ch, ch)
        cp = rcopy(p_d.at[r], mid.at[r], s_m.at[c], r_m.at[c], devs[0])
        cp.start()
        mids.append(cp)
    p_x[...] = partial(xp)

    def send(c):
        r = pl.ds(c * ch, ch)
        mids[c].wait_recv()
        p_x[r, :] = p_x[r, :] + mid[r, :]
        if c >= depth:
            fars[c - depth].wait_send()
        cp = rcopy(p_x.at[r], far.at[r], s_f.at[c], r_f.at[c], devs[1])
        cp.start()
        fars.append(cp)

    def receive(c):
        r = pl.ds(c * ch, ch)
        fars[c].wait_recv()
        res = (p_me[r, :] + far[r, :]).astype(BF16)
        if last:
            o = pl.ds(pl.multiple_of(pool * n + c * ch, ch), ch)
            out_ref[o, :] = res
            cp = rcopy(out_ref.at[o], out_ref.at[o], s_y.at[c], r_y.at[c], devs[2])
            cp.start()
            ys.append(cp)
        else:
            out_ref[r, :] = res
            if c % (CCH // 2) == CCH // 2 - 1:
                r2 = pl.ds(c * ch + ch - n // 2, n // 2)
                h = rms_bf16(out_ref[r2, :].astype(F32))
                project(h, cos_ref[r2, :], sin_ref[r2, :], wq, wk, wv, qs, kn, vn, r2)

    for c in range(depth):
        send(c)
    p_p[...] = partial(part)
    own_cp = rcopy(p_p, own, s_o, r_o, devs[0])
    own_cp.start()
    p_me[...] = partial(me)
    own_cp.wait()
    p_me[...] = a_ref[...].astype(F32) + (p_me[...] + own[...])
    if not last:
        for c in w_copies:
            c.wait()
    for c in range(depth, CCH):
        send(c)
        receive(c - depth)
    for c in range(CCH - depth, CCH):
        receive(c)
    for c in range(CCH):
        mids[c].wait_send()
    for c in range(CCH - depth, CCH):
        fars[c].wait_send()
    for cp in ys:
        cp.wait()


def combine(layer, last, y, mcol, a, nxt=None):
    n, model = a.shape
    dma = pltpu.SemaphoreType.DMA
    sems = [dma, dma, dma((CCH,)), dma((CCH,)), dma((CCH,)), dma((CCH,))]
    args = [y, mcol, a]
    specs = [vspec()] * 3
    scratch = [VMEM((n, model), F32) for _ in range(7)]
    if last:
        sems += [dma((CCH,)), dma((CCH,))]
        out_shape = jax.ShapeDtypeStruct((2 * n, model), BF16)
        out_specs = vspec()
    else:
        cos, sin, wq, wk, wv = nxt
        args += [cos, sin, wq, wk, wv]
        specs += [vspec()] * 2 + [anyspec()] * 3
        sems += [dma((3,))]
        scratch += [VMEM(w.shape[1:], BF16) for w in (wq, wk, wv)]
        out_shape = [jax.ShapeDtypeStruct((n, model), BF16)] + [jax.ShapeDtypeStruct((n, w.shape[2]), BF16) for w in (wq, wk, wv)]
        out_specs = [vspec()] * 4
    return pl.pallas_call(
        functools.partial(combine_kernel, last, layer),
        out_shape=out_shape,
        in_specs=specs,
        out_specs=out_specs,
        scratch_shapes=scratch + sems,
        compiler_params=pltpu.CompilerParams(collective_id=2 * layer + 1, has_side_effects=True, vmem_limit_bytes=LIM_C),
        name=f"combine{layer}",
    )(*args)


def solution(mesh):
    def body(hidden, k_cache, v_cache, lengths, expert_ids, w_query, w_key, w_value, w_out, w_router, w_gate, w_up, w_down):
        n_layers, _, seq, kvh, hd = k_cache.shape
        n_tok = hidden.shape[0] // 2
        kc = k_cache.reshape(n_layers, -1, seq * kvh, hd)
        vc = v_cache.reshape(n_layers, -1, seq * kvh, hd)
        ids = expert_ids.transpose(0, 2, 1)
        wr = w_router.transpose(0, 2, 1)
        tab = jnp.asarray(rope_table(seq, hd))
        w_query, w_key, w_value, w_out, w_gate, w_up, w_down, kc, vc, tab, hidden_h, lens_h = (
            pltpu.with_memory_space_constraint(v, pltpu.HBM) for v in (w_query, w_key, w_value, w_out, w_gate, w_up, w_down, kc, vc, tab, hidden, lengths))
        state = hidden
        qkv = None
        for layer in range(n_layers):
            last = layer == n_layers - 1
            if layer == 0:
                att, wo, cos, sin = attention(layer, n_tok, lens_h, w_out, kc, vc, proj=(hidden_h, tab, w_query, w_key, w_value))
            else:
                att, wo = attention(layer, n_tok, lengths, w_out, kc, vc, qkv=qkv)
            outs = dispatch(layer, att, state, ids, wr, wo, w_gate, w_up, w_down)
            a, u_all, rrow, mcol = outs[:4]
            if layer == 0:
                ids = outs[4]
            y = experts(layer, u_all, rrow, mcol, outs[-3:], w_gate, w_up, w_down)
            if last:
                return combine(layer, True, y, mcol, a)
            state, *qkv = combine(layer, False, y, mcol, a, nxt=(cos, sin, w_query, w_key, w_value))

    rows_spec = ("dp", "ep")
    in_specs = (P(rows_spec, None), P(None, rows_spec), P(None, rows_spec), P(rows_spec), P(None, rows_spec, None), P(), P(), P(), P(), P(), P(None, "ep"), P(None, "ep"), P(None, "ep"))
    return jax.shard_map(body, mesh=mesh, in_specs=in_specs, out_specs=P(rows_spec, None), check_vma=False)
```
